8 devices in a mesh: data: 2 (over z, y), graph: 4 (over x, core).
Axes of the slice: x: 2, y: 2, z: 1, core: 2. Of those that a mesh axis runs over, the one named last changes fastest.
Arguments:
- x_feat: bfloat16 [8192, 200], P(('data', 'graph')), parts along dimension 0
- dst_local: int32 [131072], P(('data', 'graph')), parts along dimension 0
- src_slot: int32 [131072], P(('data', 'graph')), parts along dimension 0
- edge_w: float32 [131072], P(('data', 'graph')), parts along dimension 0
- send_idx: int32 [2048], P(('data', 'graph')), parts along dimension 0
- hub_ids: int32 [32], P('data'), parts along dimension 0
- w_first: bfloat16 [200, 512], replicated
- b_first: float32 [512], replicated
- w_second: bfloat16 [512, 107], replicated
- grad_out: float32 [8192, 107], P(('data', 'graph')), parts along dimension 0
Outputs:
- output 1: float32 [8192, 200], P(('data', 'graph')), parts along dimension 0
- output 2: float32 [400, 512], P('data'), parts along dimension 0
- output 3: float32 [1024, 107], P('data'), parts along dimension 0
- output 4: float32 [1024], P('data'), parts along dimension 0
- output 5: float32 [214], P('data'), parts along dimension 0
There are 2 independent parts. The reference program is written for one: setup_inputs(seed, part) draws one part's arguments, and reference() takes and returns one part's arrays. A program takes and returns all parts, laid end to end along the dimension named above; an argument that names none is the same for every part.
All inputs are finite; a program needn't handle non-finite values.
Results may differ from the reference program's by a relative error of at most 0.001.
Values are sent between devices in bfloat16 or wider.
A program may use at most 1 GiB of HBM per device.

```python
import jax
import jax.numpy as jnp
from jax import lax

GROUP_SIZE = 4
NODES_DEV = 1024
FEAT_IN = 200
FEAT_HID = 512
FEAT_OUT = 107
EDGE_DEG = 16
SEND_ROWS = 64
NUM_HUBS = 16
HUB_DST_PCT = 15
HUB_SRC_PCT = 15
HALO_SRC_PCT = 35

VERTICES = GROUP_SIZE * NODES_DEV
EDGE_CAP = NODES_DEV * EDGE_DEG
HALO_ROWS = GROUP_SIZE * SEND_ROWS


def draw_graph(graph_key):
    key_list = jax.random.split(graph_key, 16)
    edge_shape = (GROUP_SIZE, EDGE_CAP)
    hub_ids = jax.random.permutation(key_list[0], VERTICES)[:NUM_HUBS].astype(jnp.int32)
    shrink = jax.random.randint(key_list[1], (GROUP_SIZE,), 1, 5)
    full_dev = jax.random.randint(key_list[2], (), 0, GROUP_SIZE)
    counts = jnp.where(jnp.arange(GROUP_SIZE) == full_dev, EDGE_CAP, EDGE_CAP // shrink)
    edge_live = jnp.arange(EDGE_CAP)[None, :] < counts[:, None]
    dst_pick = jax.random.randint(key_list[3], edge_shape, 0, 100)
    dst_span = jax.random.randint(key_list[4], edge_shape, 1, NODES_DEV + 1)
    dst_node = jax.random.randint(key_list[5], edge_shape, 0, NODES_DEV) % dst_span
    dst_hub = jax.random.randint(key_list[6], edge_shape, 0, NUM_HUBS)
    dst_local = jnp.where(dst_pick < HUB_DST_PCT, NODES_DEV + dst_hub, dst_node)
    src_pick = jax.random.randint(key_list[7], edge_shape, 0, 100)
    src_span = jax.random.randint(key_list[8], edge_shape, 1, NODES_DEV + 1)
    src_node = jax.random.randint(key_list[9], edge_shape, 0, NODES_DEV) % src_span
    peer_step = jax.random.randint(key_list[10], edge_shape, 1, GROUP_SIZE)
    peer_dev = (jnp.arange(GROUP_SIZE)[:, None] + peer_step) % GROUP_SIZE
    row_span = jax.random.randint(key_list[11], edge_shape, 1, SEND_ROWS + 1)
    halo_row = jax.random.randint(key_list[12], edge_shape, 0, SEND_ROWS) % row_span
    src_hub = jax.random.randint(key_list[13], edge_shape, 0, NUM_HUBS)
    src_slot = jnp.where(
        src_pick < HUB_SRC_PCT,
        NODES_DEV + HALO_ROWS + src_hub,
        jnp.where(src_pick < HUB_SRC_PCT + HALO_SRC_PCT, NODES_DEV + peer_dev * SEND_ROWS + halo_row, src_node),
    )
    send_idx = jax.random.randint(key_list[14], (GROUP_SIZE * GROUP_SIZE * SEND_ROWS,), 0, NODES_DEV)
    dst_local = jnp.where(edge_live, dst_local, 0).reshape(-1).astype(jnp.int32)
    src_slot = jnp.where(edge_live, src_slot, 0).reshape(-1).astype(jnp.int32)
    return dst_local, src_slot, edge_live.reshape(-1), send_idx.astype(jnp.int32), hub_ids


def setup_inputs(seed: int = 0, part: int = 0) -> dict:
    part_key = jax.random.fold_in(jax.random.key(seed), part)
    dst_local, src_slot, edge_live, send_idx, hub_ids = draw_graph(part_key)
    value_keys = jax.random.split(jax.random.fold_in(part_key, 3), 3)
    weight_keys = jax.random.split(jax.random.key(seed + 1), 3)
    x_feat = jax.random.normal(value_keys[0], (VERTICES, FEAT_IN), jnp.float32).astype(jnp.bfloat16)
    edge_scale = jax.random.uniform(value_keys[1], (GROUP_SIZE * EDGE_CAP,), jnp.float32, 0.5, 1.5)
    edge_w = jnp.where(edge_live, edge_scale * EDGE_DEG ** -0.5, 0.0).astype(jnp.float32)
    grad_out = jax.random.normal(value_keys[2], (VERTICES, FEAT_OUT), jnp.float32)
    w_first = (jax.random.normal(weight_keys[0], (FEAT_IN, FEAT_HID), jnp.float32) * FEAT_IN ** -0.5).astype(jnp.bfloat16)
    b_first = 0.5 * jax.random.normal(weight_keys[1], (FEAT_HID,), jnp.float32)
    w_second = (jax.random.normal(weight_keys[2], (FEAT_HID, FEAT_OUT), jnp.float32) * FEAT_HID ** -0.5).astype(jnp.bfloat16)
    return {
        "x_feat": x_feat,
        "dst_local": dst_local,
        "src_slot": src_slot,
        "edge_w": edge_w,
        "send_idx": send_idx,
        "hub_ids": hub_ids,
        "w_first": w_first,
        "b_first": b_first,
        "w_second": w_second,
        "grad_out": grad_out,
    }


def source_ids(src_slot, send_idx, hub_ids):
    slot_ids = src_slot.reshape(GROUP_SIZE, EDGE_CAP)
    device = jnp.arange(GROUP_SIZE)[:, None]
    halo_pos = jnp.clip(slot_ids - NODES_DEV, 0, HALO_ROWS - 1)
    peer_dev = halo_pos // SEND_ROWS
    send_table = send_idx.reshape(GROUP_SIZE, GROUP_SIZE, SEND_ROWS)
    halo_src = peer_dev * NODES_DEV + send_table[peer_dev, device, halo_pos % SEND_ROWS]
    hub_src = hub_ids[jnp.clip(slot_ids - NODES_DEV - HALO_ROWS, 0, NUM_HUBS - 1)]
    return jnp.where(
        slot_ids < NODES_DEV,
        device * NODES_DEV + slot_ids,
        jnp.where(slot_ids < NODES_DEV + HALO_ROWS, halo_src, hub_src),
    )


def aggregate(features, dst_rows, src_ids, edge_rows, hub_ids):
    def one_device(dev_item):
        dst_dev, src_dev, w_dev = dev_item
        gathered = features[src_dev] * w_dev[:, None]
        return jax.ops.segment_sum(gathered, dst_dev, num_segments=NODES_DEV + NUM_HUBS)
    dev_sums = lax.map(one_device, (dst_rows, src_ids, edge_rows))
    local_rows = dev_sums[:, :NODES_DEV].reshape(VERTICES, -1)
    return local_rows.at[hub_ids].add(dev_sums[:, NODES_DEV:].sum(axis=0))


def reference(x_feat, dst_local, src_slot, edge_w, send_idx, hub_ids, w_first, b_first, w_second, grad_out):
    src_ids = source_ids(src_slot, send_idx, hub_ids)
    dst_rows = dst_local.reshape(GROUP_SIZE, EDGE_CAP)
    edge_rows = edge_w.reshape(GROUP_SIZE, EDGE_CAP)

    def layers(x_in, w_in, b_in, w_out):
        z_first = jnp.dot(x_in, w_in, preferred_element_type=jnp.float32).astype(jnp.bfloat16).astype(jnp.float32)
        pre_act = aggregate(z_first, dst_rows, src_ids, edge_rows, hub_ids) + b_in
        act_full = jax.nn.relu(pre_act)
        hidden = act_full + lax.stop_gradient(act_full.astype(jnp.bfloat16).astype(jnp.float32) - act_full)
        z_second = jnp.dot(hidden, w_out, preferred_element_type=jnp.float32).astype(jnp.bfloat16).astype(jnp.float32)
        return aggregate(z_second, dst_rows, src_ids, edge_rows, hub_ids)

    _, pullback = jax.vjp(
        layers,
        x_feat.astype(jnp.float32),
        w_first.astype(jnp.float32),
        b_first,
        w_second.astype(jnp.float32),
    )
    grad_x, grad_w1, grad_b1, grad_w2 = pullback(grad_out)
    return grad_x, grad_w1, grad_w2, grad_b1, grad_out.sum(axis=0)
```

```python
import functools

import jax
import jax.numpy as jnp
from jax import lax
from jax.experimental import pallas as pl
from jax.experimental.pallas import tpu as pltpu
from jax.sharding import PartitionSpec as P

F32, BF16 = jnp.float32, jnp.bfloat16
NODES, SEND, HALO, HUBS = 1024, 64, 256, 16
TABLE = NODES + HALO + HUBS
TILES = 9
COLS = TILES * 128
ROWS = TILES * TABLE
EDGES = 16384
HID, OUT, FIN = 512, 107, 200
ACCS = 4
UNROLL = 4
NT = (((1,), (1,)), ((), ()))


def split3(x):
    hi = x.astype(BF16)
    rest = x - hi.astype(F32)
    mid = rest.astype(BF16)
    return hi, mid, (rest - mid.astype(F32)).astype(BF16)


def dot(a, b):
    return jnp.dot(a, b, preferred_element_type=F32)


def dot_nt(a, b):
    return lax.dot_general(a, b, NT, preferred_element_type=F32)


def build_kernel(hub_ref, dst_ref, src_ref, w_ref, hi_ref, mid_ref, lo_ref, val_ref, row_ref, lane_ref, row_smem, sem, *accs):
    base = lax.axis_index("graph") * NODES
    dst, src = dst_ref[...], src_ref[...]
    new_dst, new_src = dst, src
    for k in range(HUBS):
        local = hub_ref[k] - base
        local = jnp.where((local >= 0) & (local < NODES), local, -1)
        new_dst = jnp.where(dst == local, NODES + k, new_dst)
        new_src = jnp.where(src == local, NODES + HALO + k, new_src)
    row_ref[...] = (new_dst >> 7) * TABLE + new_src
    lane_ref[...] = new_dst & 127
    copy = pltpu.make_async_copy(row_ref, row_smem, sem)
    copy.start()

    def zero(i, carry):
        for acc in accs:
            acc[pl.ds(pl.multiple_of(i * 48, 8), 48), :] = jnp.zeros((48, 128), F32)
        return carry

    lax.fori_loop(0, ROWS // 48, zero, 0)
    iota = lax.broadcasted_iota(jnp.int32, (8, 128), 1)

    def prep(g, carry):
        at = pl.multiple_of(g * 8, 8)
        lanes, weights = lane_ref[pl.ds(at, 8), :], w_ref[pl.ds(at, 8), :]
        for c in range(128):
            hit = jnp.broadcast_to(lanes[:, c:c + 1], (8, 128)) == iota
            val = jnp.where(hit, jnp.broadcast_to(weights[:, c:c + 1], (8, 128)), 0.0)
            val_ref[pl.ds(pl.multiple_of(g * 1024 + c * 8, 8), 8), :] = val
        return carry

    lax.fori_loop(0, 16, prep, 0)
    copy.wait()

    def scatter(t, carry):
        per_group = 128 // UNROLL
        group = t // per_group
        col = (t - group * per_group) * UNROLL
        vbase = pl.multiple_of(t * UNROLL * 8, 8 * UNROLL)
        n = 0
        for c in range(UNROLL):
            for s in range(8):
                acc = accs[n % ACCS]
                n += 1
                r = row_smem[group * 8 + s, col + c]
                acc[pl.ds(r, 1), :] = acc[pl.ds(r, 1), :] + val_ref[pl.ds(vbase + c * 8 + s, 1), :]
        return carry

    lax.fori_loop(0, EDGES // (8 * UNROLL), scatter, 0)

    def finish(i, carry):
        at = pl.multiple_of(i * 48, 16)
        for t in range(TILES):
            part = pl.ds(pl.multiple_of(t * TABLE + i * 48, 8), 48)
            total = accs[0][part, :]
            for acc in accs[1:]:
                total = total + acc[part, :]
            for piece, ref in zip(split3(total), (hi_ref, mid_ref, lo_ref)):
                ref[pl.ds(at, 48), t * 128:(t + 1) * 128] = piece
        return carry

    lax.fori_loop(0, TABLE // 48, finish, 0)


def build(hub_ids, dst, src, w):
    piece = jax.ShapeDtypeStruct((TABLE, COLS), BF16)
    square = lambda a: a.reshape(128, 128)
    vmem = pl.BlockSpec(memory_space=pltpu.VMEM)
    return pl.pallas_call(
        build_kernel,
        out_shape=(piece,) * 3,
        in_specs=[pl.BlockSpec(memory_space=pltpu.SMEM)] + [vmem] * 3,
        out_specs=(vmem,) * 3,
        scratch_shapes=[
            pltpu.VMEM((EDGES, 128), F32),
            pltpu.VMEM((128, 128), jnp.int32),
            pltpu.VMEM((128, 128), jnp.int32),
            pltpu.SMEM((128, 128), jnp.int32),
            pltpu.SemaphoreType.DMA,
        ] + [pltpu.VMEM((ROWS, 128), F32)] * ACCS,
        compiler_params=pltpu.CompilerParams(vmem_limit_bytes=48 << 20),
        name="build",
    )(hub_ids, square(dst), square(src), square(w))


def step_kernel(
    hi_ref, mid_ref, lo_ref, x_ref, w1_ref, b1_ref, w2_ref, dh_ref, send_ref, hub_ref,
    dx_ref, dw1_ref, dw2_ref, db1_ref, db2_ref,
    row_s, pt_s, xs, xr, hs, hr, z_s, yt_s, d2_s, g2_s, g2h_s, rb, sb, ys, yr, dy_s, g1_s, sd, rd, ret_s, dz1_s,
    xt_s, a2, half2, got2, tot2, a1, half1, got1, tot1, send_sem, recv_sem,
):
    me = lax.axis_index("graph")
    sibling = me + 1 - 2 * lax.rem(me, 2)
    across = lax.rem(me + 2, 4)
    core = lax.rem(me, 2)
    mesh_id = pl.DeviceIdType.MESH
    peers = [lax.rem(me + d, 4) for d in (1, 2, 3)]
    barrier = pltpu.get_barrier_semaphore()
    for q in peers:
        pl.semaphore_signal(barrier, inc=1, device_id={"graph": q}, device_id_type=mesh_id)
    pl.semaphore_wait(barrier, 3)
    used = [0]

    def remote(src, dst, q):
        i = used[0]
        used[0] += 1
        copy = pltpu.make_async_remote_copy(
            src_ref=src, dst_ref=dst, send_sem=send_sem.at[i], recv_sem=recv_sem.at[i],
            device_id={"graph": q}, device_id_type=mesh_id)
        copy.start()
        return copy

    pieces = (hi_ref, mid_ref, lo_ref)
    row_s[...] = jnp.full((1, 384), -1.0, F32)
    row_s[:, :HALO] = send_ref[...].astype(F32)
    hub_local = hub_ref[...] - me * NODES
    row_s[:, HALO:HALO + HUBS] = jnp.where((hub_local >= 0) & (hub_local < NODES), hub_local, -1).astype(F32)
    row = row_s[...]
    column = jnp.transpose(jnp.broadcast_to(row, (128, 384)))
    lane = lax.broadcasted_iota(jnp.int32, (272, 128), 1).astype(F32)
    picks = jnp.concatenate(
        [jnp.where(column[:272] == lane + float(j * 128), 1.0, 0.0).astype(BF16) for j in range(8)], axis=1)
    sub = lax.broadcasted_iota(jnp.int32, (NODES, 384), 0).astype(F32)
    pt_s[...] = jnp.where(sub == row, 1.0, 0.0).astype(BF16)
    x = x_ref[...]
    sent = dot(picks, x).astype(BF16)
    hub_col = column[HALO:HALO + HUBS]
    alias = [jnp.where((hub_col == row[:, j * 128:(j + 1) * 128]) & (hub_col >= 0.0), 1.0, 0.0) for j in range(2)]
    for q in range(4):
        xs[q, :SEND, :] = sent[q * SEND:(q + 1) * SEND]
        xs[q, SEND:SEND + HUBS, :] = sent[HALO:]
        part = alias[q // 2][:, (q % 2) * SEND:(q % 2 + 1) * SEND]
        xs[q, SEND + HUBS:, :SEND] = part.astype(BF16)
        xs[q, SEND + HUBS:, SEND:] = jnp.zeros((HUBS, FIN - SEND), BF16)
    d2_s[...] = jnp.zeros((COLS, 384), BF16)
    dh = dh_ref[...]
    for j, piece in enumerate(split3(dh)):
        d2_s[:NODES, j * 128:j * 128 + OUT] = piece
    hub_pick = picks[HALO:]
    hub_dh = dot(hub_pick, d2_s[:NODES, :])
    hs[...] = (hub_dh[:, :128] + hub_dh[:, 128:256]) + hub_dh[:, 256:]
    xr[me] = jnp.zeros((96, FIN), BF16)
    hr[me] = hs[...]
    round_a = []
    for q in peers:
        round_a.append(remote(xs.at[q], xr.at[me], q))
        round_a.append(remote(hs, hr.at[me], q))
    db2_ref[...] = jnp.sum(dh, axis=0, keepdims=True)

    def reduce_group(own, half, got, total):
        remote(own.at[1 - core], got.at[0], sibling).wait()
        half[...] = own[core] + got[0]
        remote(half, got.at[1], across).wait()
        total[core] = half[...] + got[1]
        remote(total.at[core], total.at[core], sibling).wait()

    xt_s[:FIN, :] = jnp.transpose(jnp.concatenate([x, jnp.zeros((NODES, 56), BF16)], axis=1).astype(F32))[:FIN].astype(BF16)
    w1t = jnp.transpose(jnp.concatenate([w1_ref[...], jnp.zeros((56, HID), BF16)], axis=0).astype(F32)).astype(BF16)[:, :FIN]
    z_s[:, :NODES] = dot_nt(w1t, x).astype(BF16)

    def forward_own(at):
        z = z_s[:, :NODES]
        acc = dot(z, hi_ref[:NODES, at])
        acc = acc + dot(z, mid_ref[:NODES, at])
        yt_s[:, at] = acc + dot(z, lo_ref[:NODES, at])

    def over_columns(body):
        def turn(n, carry):
            body(pl.ds(pl.multiple_of(n * 256, 256), 256))
            return carry

        lax.fori_loop(0, 4, turn, 0)

    over_columns(forward_own)
    forward_own(pl.ds(NODES, 128))

    def wait_all(copies):
        for copy in copies:
            copy.wait()

    wait_all(round_a)
    halo_x = jnp.concatenate([xr[q, :SEND, :] for q in range(4)], axis=0)
    own_hub_x = sent[HALO:].astype(F32)
    hub_x = own_hub_x
    for q in range(4):
        hub_x = hub_x + xr[q, SEND:SEND + HUBS, :].astype(F32)
    z_s[:, NODES:NODES + HALO] = dot_nt(w1t, halo_x).astype(BF16)
    z_hub = dot_nt(w1t, hub_x.astype(BF16)).astype(BF16)

    def forward_far(at):
        z = z_s[:, NODES:NODES + HALO]
        acc = yt_s[:, at]
        for ref in pieces:
            acc = acc + dot(z, ref[NODES:NODES + HALO, at])
        for ref in pieces:
            acc = acc + dot(z_hub, ref[NODES + HALO:, at])
        yt_s[:, at] = acc

    forward_far(pl.ds(NODES, 128))
    ys[...] = jnp.transpose(yt_s[:, NODES:])[:HUBS]
    yr[me] = ys[...]
    round_y = [remote(ys, yr.at[me], q) for q in peers]
    over_columns(forward_far)

    hub_dh = (hr[0] + hr[1]) + (hr[2] + hr[3])
    for j, piece in enumerate(split3(hub_dh)):
        d2_s[NODES:NODES + HUBS, j * 128:(j + 1) * 128] = piece

    def grad2(rows):
        a = dot(hi_ref[rows, :], d2_s[:, :256])
        b = dot(mid_ref[rows, :], d2_s[:, :256])
        c = dot(hi_ref[rows, :], d2_s[:, 256:]) + dot(lo_ref[rows, :], d2_s[:, :128])
        return ((c + b[:, 128:]) + (a[:, 128:] + b[:, :128])) + a[:, :128]

    g2h_s[...] = grad2(pl.ds(NODES, HALO + HUBS))
    far = g2h_s[:HALO, :]
    alias_row = jnp.concatenate([xr[q, SEND + HUBS:, :SEND] for q in range(4)], axis=1)
    hub_g2 = g2h_s[HALO:, :]
    for piece in split3(far):
        hub_g2 = hub_g2 + dot(alias_row, piece)
    for q in range(4):
        sb[q, :SEND, :] = far[q * SEND:(q + 1) * SEND]
        sb[q, SEND:, :] = hub_g2
    rb[me] = sb[me]
    round_b = [remote(sb.at[q], rb.at[me], q) for q in peers]

    def grad2_own(m, carry):
        at = pl.ds(pl.multiple_of(m * 256, 256), 256)
        g2_s[at, :] = grad2(at)
        return carry

    lax.fori_loop(0, 4, grad2_own, 0)
    wait_all(round_y)
    wait_all(round_b)

    hub_full = (rb[0, SEND:, :] + rb[1, SEND:, :]) + (rb[2, SEND:, :] + rb[3, SEND:, :])
    hub_dz2 = hub_full.astype(BF16)
    keep = lax.broadcasted_iota(jnp.int32, (4, SEND, 128), 0) != me
    back = jnp.where(keep, rb[:, :SEND, :], 0.0).reshape(HALO, 128)
    own = g2_s[...]
    halo_pick = pt_s[:, :HALO]
    hub_put = pt_s[:, HALO:HALO + HUBS]
    for piece in split3(back):
        own = own + dot(halo_pick, piece)
    is_hub = dot(hub_put, jnp.ones((HUBS, 128), BF16)) > 0.5
    dz2 = jnp.where(is_hub, dot(hub_put, hub_dz2), own).astype(BF16)

    y_hub = (yr[0] + yr[1]) + (yr[2] + yr[3])
    b1 = b1_ref[...]
    b1_col = jnp.transpose(jnp.broadcast_to(b1, (128, HID)))
    hub_sel = picks[HALO:]
    for piece in split3(jnp.transpose(jnp.concatenate([y_hub, jnp.zeros((112, HID), F32)], axis=0))):
        yt_s[:, :NODES] += dot(piece[:, :HUBS], hub_sel)
    pre = yt_s[:, :NODES] + jnp.concatenate([b1_col] * 8, axis=1)
    hidden_t = jnp.maximum(pre, 0.0).astype(BF16)
    live = jnp.transpose(jnp.where(pre > 0.0, 1.0, 0.0))
    dw2 = dot(hidden_t, dz2)
    db2 = jnp.concatenate([db2_ref[...], jnp.zeros((1, 128 - OUT), F32)], axis=1)
    for h in range(2):
        a2[h, :256, :] = dw2[h * 256:(h + 1) * 256]
        a2[h, 256:, :] = jnp.broadcast_to(db2, (8, 128))
    reduce_group(a2, half2, got2, tot2)
    w2 = w2_ref[...]
    grad_h = dot_nt(dz2[:, :OUT], w2)
    dy = jnp.where(live > 0.5, grad_h, 0.0)
    hub_dy = jnp.where(y_hub + b1 > 0.0, dot_nt(hub_dz2[:, :OUT], w2), 0.0)
    db1 = jnp.sum(dy, axis=0, keepdims=True)
    for j, piece in enumerate(split3(dy)):
        dy_s[j, :NODES, :] = piece
    for j, piece in enumerate(split3(hub_dy)):
        dy_s[j, NODES:NODES + HUBS, :] = piece
        dy_s[j, NODES + HUBS:, :] = jnp.zeros((112, HID), BF16)

    def grad1(rows):
        acc = dot(lo_ref[rows, :], dy_s[0])
        acc = acc + dot(mid_ref[rows, :], dy_s[1])
        acc = acc + dot(hi_ref[rows, :], dy_s[2])
        acc = acc + dot(mid_ref[rows, :], dy_s[0])
        acc = acc + dot(hi_ref[rows, :], dy_s[1])
        return acc + dot(hi_ref[rows, :], dy_s[0])

    ret_s[...] = grad1(pl.ds(NODES, HALO + HUBS))
    for q in range(4):
        sd[q, :SEND, :] = ret_s[q * SEND:(q + 1) * SEND, :]
        sd[q, SEND:, :] = ret_s[HALO:, :]
    rd[me] = sd[me]
    round_d = [remote(sd.at[q], rd.at[me], q) for q in peers]

    for m in range(2):
        g1_s[m * 512:(m + 1) * 512, :] = grad1(pl.ds(m * 512, 512))
    wait_all(round_d)
    back = jnp.where(lax.broadcasted_iota(jnp.int32, (4, SEND, HID), 0) != me, rd[:, :SEND, :], 0.0).reshape(HALO, HID)
    hub_back = (rd[0, SEND:, :] + rd[1, SEND:, :]) + (rd[2, SEND:, :] + rd[3, SEND:, :])
    dz1 = g1_s[...]
    for piece in split3(back):
        dz1 = dz1 + dot(halo_pick, piece)
    for piece in split3(hub_back):
        dz1 = dz1 + dot(hub_put, piece)
    dz1_s[...] = dz1.astype(BF16)
    dw1 = dot(xt_s[:FIN, :], dz1_s[...])

    dx_ref[...] = dot_nt(dz1_s[...], w1_ref[...])
    for h in range(2):
        a1[h, :FIN, :] = dw1[:, h * 256:(h + 1) * 256]
        a1[h, FIN:, :] = jnp.broadcast_to(db1[:, h * 256:(h + 1) * 256], (8, 256))
    reduce_group(a1, half1, got1, tot1)
    for h in range(2):
        dw1_ref[:, h * 256:(h + 1) * 256] = tot1[h, :FIN, :]
        db1_ref[:, h * 256:(h + 1) * 256] = tot1[h, FIN:FIN + 1, :]
    for h in range(2):
        dw2_ref[h * 256:(h + 1) * 256, :] = tot2[h, :256, :OUT]
    db2_ref[...] = tot2[0, 256:257, :OUT]


def step(hi, mid, lo, x, w1, b1, w2, dh, send, hubs):
    vmem = pl.BlockSpec(memory_space=pltpu.VMEM)
    out = lambda *shape: jax.ShapeDtypeStruct(shape, F32)
    f32 = lambda *shape: pltpu.VMEM(shape, F32)
    b16 = lambda *shape: pltpu.VMEM(shape, BF16)
    return pl.pallas_call(
        step_kernel,
        out_shape=(out(NODES, FIN), out(FIN, HID), out(HID, OUT), out(1, HID), out(1, OUT)),
        in_specs=[vmem] * 10,
        out_specs=(vmem,) * 5,
        scratch_shapes=[
            f32(1, 384), b16(NODES, 384), b16(4, 96, FIN), b16(4, 96, FIN), f32(HUBS, 128), f32(4, HUBS, 128),
            b16(HID, NODES + HALO), f32(HID, COLS), b16(COLS, 384), f32(NODES, 128), f32(HALO + HUBS, 128),
            f32(4, SEND + HUBS, 128), f32(4, SEND + HUBS, 128), f32(HUBS, HID), f32(4, HUBS, HID),
            b16(3, COLS, HID), f32(NODES, HID), f32(4, SEND + HUBS, HID), f32(4, SEND + HUBS, HID),
            f32(HALO + HUBS, HID), b16(NODES, HID), b16(FIN + 8, NODES),
            f32(2, 264, 128), f32(264, 128), f32(2, 264, 128), f32(2, 264, 128),
            f32(2, 208, 256), f32(208, 256), f32(2, 208, 256), f32(2, 208, 256),
            pltpu.SemaphoreType.DMA((24,)), pltpu.SemaphoreType.DMA((24,)),
        ],
        compiler_params=pltpu.CompilerParams(collective_id=0, has_side_effects=True, vmem_limit_bytes=48 << 20),
        name="step",
    )(hi, mid, lo, x, w1, b1, w2, dh, send, hubs)


def solution(mesh):
    vertex_spec = P(("data", "graph"))
    vertex_rows = P(("data", "graph"), None)
    part_spec = P("data")
    part_rows = P("data", None)
    replicated = P()

    def device_step(x, dst, src, w, send, hub_ids, w_first, b_first, w_second, dy_out):
        hi, mid, lo = build(hub_ids, dst, src, w)
        dx, dw1, dw2, db1, db2 = step(
            hi, mid, lo, x, w_first, b_first.reshape(1, HID), w_second, dy_out, send.reshape(1, HALO), hub_ids.reshape(1, HUBS))
        return dx, dw1, dw2, db1.reshape(HID), db2.reshape(OUT)

    return jax.shard_map(
        device_step,
        mesh=mesh,
        in_specs=(vertex_rows, vertex_spec, vertex_spec, vertex_spec, vertex_spec, part_spec, replicated, replicated, replicated, vertex_rows),
        out_specs=(vertex_rows, part_rows, part_rows, part_spec, part_spec),
        check_vma=False,
    )
```

```python
import functools

import jax
import jax.numpy as jnp
from jax import lax
from jax.experimental import pallas as pl
from jax.experimental.pallas import tpu as pltpu
from jax.sharding import PartitionSpec as P

F32, BF16 = jnp.float32, jnp.bfloat16
NODES, SEND, HALO, HUBS = 1024, 64, 256, 16
TABLE = NODES + HALO + HUBS
TILES = 9
COLS = TILES * 128
ROWS = TILES * TABLE
EDGES = 16384
HID, OUT, FIN = 512, 107, 200
ACCS = 4
UNROLL = 4
NT = (((1,), (1,)), ((), ()))


def split3(x):
    hi = x.astype(BF16)
    rest = x - hi.astype(F32)
    mid = rest.astype(BF16)
    return hi, mid, (rest - mid.astype(F32)).astype(BF16)


def dot(a, b):
    return jnp.dot(a, b, preferred_element_type=F32)


def dot_nt(a, b):
    return lax.dot_general(a, b, NT, preferred_element_type=F32)


def build_kernel(hub_ref, dst_ref, src_ref, w_ref, hi_ref, mid_ref, lo_ref, val_ref, row_ref, lane_ref, row_smem, sem, *accs):
    base = lax.axis_index("graph") * NODES
    dst, src = dst_ref[...], src_ref[...]
    new_dst, new_src = dst, src
    for k in range(HUBS):
        local = hub_ref[k] - base
        local = jnp.where((local >= 0) & (local < NODES), local, -1)
        new_dst = jnp.where(dst == local, NODES + k, new_dst)
        new_src = jnp.where(src == local, NODES + HALO + k, new_src)
    row_ref[...] = (new_dst >> 7) * TABLE + new_src
    lane_ref[...] = new_dst & 127
    copy = pltpu.make_async_copy(row_ref, row_smem, sem)
    copy.start()

    def zero(i, carry):
        for acc in accs:
            acc[pl.ds(pl.multiple_of(i * 48, 8), 48), :] = jnp.zeros((48, 128), F32)
        return carry

    lax.fori_loop(0, ROWS // 48, zero, 0)
    iota = lax.broadcasted_iota(jnp.int32, (8, 128), 1)

    def prep(g, carry):
        at = pl.multiple_of(g * 8, 8)
        lanes, weights = lane_ref[pl.ds(at, 8), :], w_ref[pl.ds(at, 8), :]
        for c in range(128):
            hit = jnp.broadcast_to(lanes[:, c:c + 1], (8, 128)) == iota
            val = jnp.where(hit, jnp.broadcast_to(weights[:, c:c + 1], (8, 128)), 0.0)
            val_ref[pl.ds(pl.multiple_of(g * 1024 + c * 8, 8), 8), :] = val
        return carry

    lax.fori_loop(0, 16, prep, 0)
    copy.wait()

    def scatter(t, carry):
        per_group = 128 // UNROLL
        group = t // per_group
        col = (t - group * per_group) * UNROLL
        vbase = pl.multiple_of(t * UNROLL * 8, 8 * UNROLL)
        n = 0
        for c in range(UNROLL):
            for s in range(8):
                acc = accs[n % ACCS]
                n += 1
                r = row_smem[group * 8 + s, col + c]
                acc[pl.ds(r, 1), :] = acc[pl.ds(r, 1), :] + val_ref[pl.ds(vbase + c * 8 + s, 1), :]
        return carry

    lax.fori_loop(0, EDGES // (8 * UNROLL), scatter, 0)

    def finish(i, carry):
        at = pl.multiple_of(i * 48, 16)
        for t in range(TILES):
            part = pl.ds(pl.multiple_of(t * TABLE + i * 48, 8), 48)
            total = accs[0][part, :]
            for acc in accs[1:]:
                total = total + acc[part, :]
            for piece, ref in zip(split3(total), (hi_ref, mid_ref, lo_ref)):
                ref[pl.ds(at, 48), t * 128:(t + 1) * 128] = piece
        return carry

    lax.fori_loop(0, TABLE // 48, finish, 0)


def build(hub_ids, dst, src, w):
    piece = jax.ShapeDtypeStruct((TABLE, COLS), BF16)
    square = lambda a: a.reshape(128, 128)
    vmem = pl.BlockSpec(memory_space=pltpu.VMEM)
    return pl.pallas_call(
        build_kernel,
        out_shape=(piece,) * 3,
        in_specs=[pl.BlockSpec(memory_space=pltpu.SMEM)] + [vmem] * 3,
        out_specs=(vmem,) * 3,
        scratch_shapes=[
            pltpu.VMEM((EDGES, 128), F32),
            pltpu.VMEM((128, 128), jnp.int32),
            pltpu.VMEM((128, 128), jnp.int32),
            pltpu.SMEM((128, 128), jnp.int32),
            pltpu.SemaphoreType.DMA,
        ] + [pltpu.VMEM((ROWS, 128), F32)] * ACCS,
        compiler_params=pltpu.CompilerParams(vmem_limit_bytes=48 << 20),
        name="build",
    )(hub_ids, square(dst), square(src), square(w))


def step_kernel(
    hi_ref, mid_ref, lo_ref, xt_ref, w1_ref, b1_ref, w2t_ref, dht_ref, send_ref, hub_ref,
    dxt_ref, dw1_ref, dw2t_ref, db1_ref, db2_ref,
    row_s, pt_s, xs, xr, hs, hr, z_s, yt_s, d2_s, g2_s, g2h_s, rb, sb, ys, yr, dy_s, g1_s, sd, rd, ret_s, dz1_s,
    a2, half2, got2, tot2, a1, half1, got1, tot1, send_sem, recv_sem,
):
    me = lax.axis_index("graph")
    sibling = me + 1 - 2 * lax.rem(me, 2)
    across = lax.rem(me + 2, 4)
    core = lax.rem(me, 2)
    mesh_id = pl.DeviceIdType.MESH
    peers = [lax.rem(me + d, 4) for d in (1, 2, 3)]
    barrier = pltpu.get_barrier_semaphore()
    for q in peers:
        pl.semaphore_signal(barrier, inc=1, device_id={"graph": q}, device_id_type=mesh_id)
    pl.semaphore_wait(barrier, 3)
    used = [0]

    def remote(src, dst, q):
        i = used[0]
        used[0] += 1
        copy = pltpu.make_async_remote_copy(
            src_ref=src, dst_ref=dst, send_sem=send_sem.at[i], recv_sem=recv_sem.at[i],
            device_id={"graph": q}, device_id_type=mesh_id)
        copy.start()
        return copy

    pieces = (hi_ref, mid_ref, lo_ref)
    row_s[...] = jnp.full((1, 384), -1.0, F32)
    row_s[:, :HALO] = send_ref[...].astype(F32)
    hub_local = hub_ref[...] - me * NODES
    row_s[:, HALO:HALO + HUBS] = jnp.where((hub_local >= 0) & (hub_local < NODES), hub_local, -1).astype(F32)
    row = row_s[...]
    column = jnp.transpose(jnp.broadcast_to(row, (128, 384)))
    lane = lax.broadcasted_iota(jnp.int32, (272, 128), 1).astype(F32)
    picks = jnp.concatenate(
        [jnp.where(column[:272] == lane + float(j * 128), 1.0, 0.0).astype(BF16) for j in range(8)], axis=1)
    sub = lax.broadcasted_iota(jnp.int32, (NODES, 384), 0).astype(F32)
    pt_s[...] = jnp.where(sub == row, 1.0, 0.0).astype(BF16)
    xt = xt_ref[...]
    sent = dot_nt(picks, xt).astype(BF16)
    hub_col = column[HALO:HALO + HUBS]
    alias = [jnp.where((hub_col == row[:, j * 128:(j + 1) * 128]) & (hub_col >= 0.0), 1.0, 0.0) for j in range(2)]
    for q in range(4):
        xs[q, :SEND, :] = sent[q * SEND:(q + 1) * SEND]
        xs[q, SEND:SEND + HUBS, :] = sent[HALO:]
        part = alias[q // 2][:, (q % 2) * SEND:(q % 2 + 1) * SEND]
        xs[q, SEND + HUBS:, :SEND] = part.astype(BF16)
        xs[q, SEND + HUBS:, SEND:] = jnp.zeros((HUBS, FIN - SEND), BF16)
    d2_s[...] = jnp.zeros((COLS, 384), BF16)
    dht = dht_ref[...]
    dh = jnp.transpose(jnp.concatenate([dht, jnp.zeros((128 - OUT, NODES), F32)], axis=0))
    for j, piece in enumerate(split3(dh)):
        d2_s[:NODES, j * 128:(j + 1) * 128] = piece
    hub_pick = picks[HALO:]
    hub_dh = dot(hub_pick, d2_s[:NODES, :])
    hs[...] = (hub_dh[:, :128] + hub_dh[:, 128:256]) + hub_dh[:, 256:]
    xr[me] = jnp.zeros((96, FIN), BF16)
    hr[me] = hs[...]
    round_a = []
    for q in peers:
        round_a.append(remote(xs.at[q], xr.at[me], q))
        round_a.append(remote(hs, hr.at[me], q))
    db2 = jnp.sum(dh, axis=0, keepdims=True)

    def reduce_group(own, half, got, total):
        remote(own.at[1 - core], got.at[0], sibling).wait()
        half[...] = own[core] + got[0]
        remote(half, got.at[1], across).wait()
        total[core] = half[...] + got[1]
        remote(total.at[core], total.at[core], sibling).wait()

    w1t = jnp.transpose(jnp.concatenate([w1_ref[...], jnp.zeros((56, HID), BF16)], axis=0).astype(F32)).astype(BF16)[:, :FIN]
    z_s[:, :NODES] = dot(w1t, xt).astype(BF16)

    def forward_own(at):
        z = z_s[:, :NODES]
        acc = dot(z, hi_ref[:NODES, at])
        acc = acc + dot(z, mid_ref[:NODES, at])
        yt_s[:, at] = acc + dot(z, lo_ref[:NODES, at])

    def over_columns(body):
        def turn(n, carry):
            body(pl.ds(pl.multiple_of(n * 256, 256), 256))
            return carry

        lax.fori_loop(0, 4, turn, 0)

    over_columns(forward_own)
    forward_own(pl.ds(NODES, 128))

    def wait_all(copies):
        for copy in copies:
            copy.wait()

    wait_all(round_a)
    halo_x = jnp.concatenate([xr[q, :SEND, :] for q in range(4)], axis=0)
    own_hub_x = sent[HALO:].astype(F32)
    hub_x = own_hub_x
    for q in range(4):
        hub_x = hub_x + xr[q, SEND:SEND + HUBS, :].astype(F32)
    z_s[:, NODES:NODES + HALO] = dot_nt(w1t, halo_x).astype(BF16)
    z_hub = dot_nt(w1t, hub_x.astype(BF16)).astype(BF16)

    def forward_far(at):
        z = z_s[:, NODES:NODES + HALO]
        acc = yt_s[:, at]
        for ref in pieces:
            acc = acc + dot(z, ref[NODES:NODES + HALO, at])
        for ref in pieces:
            acc = acc + dot(z_hub, ref[NODES + HALO:, at])
        yt_s[:, at] = acc

    forward_far(pl.ds(NODES, 128))
    ys[...] = jnp.transpose(yt_s[:, NODES:])[:HUBS]
    yr[me] = ys[...]
    round_y = [remote(ys, yr.at[me], q) for q in peers]
    over_columns(forward_far)

    hub_dh = (hr[0] + hr[1]) + (hr[2] + hr[3])
    for j, piece in enumerate(split3(hub_dh)):
        d2_s[NODES:NODES + HUBS, j * 128:(j + 1) * 128] = piece

    def grad2(rows):
        a = dot(hi_ref[rows, :], d2_s[:, :256])
        b = dot(mid_ref[rows, :], d2_s[:, :256])
        c = dot(hi_ref[rows, :], d2_s[:, 256:]) + dot(lo_ref[rows, :], d2_s[:, :128])
        return ((c + b[:, 128:]) + (a[:, 128:] + b[:, :128])) + a[:, :128]

    g2h_s[...] = grad2(pl.ds(NODES, HALO + HUBS))
    far = g2h_s[:HALO, :]
    alias_row = jnp.concatenate([xr[q, SEND + HUBS:, :SEND] for q in range(4)], axis=1)
    hub_g2 = g2h_s[HALO:, :]
    for piece in split3(far):
        hub_g2 = hub_g2 + dot(alias_row, piece)
    for q in range(4):
        sb[q, :SEND, :] = far[q * SEND:(q + 1) * SEND]
        sb[q, SEND:, :] = hub_g2
    rb[me] = sb[me]
    round_b = [remote(sb.at[q], rb.at[me], q) for q in peers]

    def grad2_own(m, carry):
        at = pl.ds(pl.multiple_of(m * 256, 256), 256)
        g2_s[at, :] = grad2(at)
        return carry

    lax.fori_loop(0, 4, grad2_own, 0)
    wait_all(round_y)
    wait_all(round_b)

    hub_full = (rb[0, SEND:, :] + rb[1, SEND:, :]) + (rb[2, SEND:, :] + rb[3, SEND:, :])
    hub_dz2 = hub_full.astype(BF16)
    keep = lax.broadcasted_iota(jnp.int32, (4, SEND, 128), 0) != me
    back = jnp.where(keep, rb[:, :SEND, :], 0.0).reshape(HALO, 128)
    own = g2_s[...]
    halo_pick = pt_s[:, :HALO]
    hub_put = pt_s[:, HALO:HALO + HUBS]
    for piece in split3(back):
        own = own + dot(halo_pick, piece)
    is_hub = dot(hub_put, jnp.ones((HUBS, 128), BF16)) > 0.5
    dz2 = jnp.where(is_hub, dot(hub_put, hub_dz2), own).astype(BF16)

    y_hub = (yr[0] + yr[1]) + (yr[2] + yr[3])
    b1 = b1_ref[...]
    b1_col = jnp.transpose(jnp.broadcast_to(b1, (128, HID)))
    hub_sel = picks[HALO:]
    for piece in split3(jnp.transpose(jnp.concatenate([y_hub, jnp.zeros((112, HID), F32)], axis=0))):
        yt_s[:, :NODES] += dot(piece[:, :HUBS], hub_sel)
    pre = yt_s[:, :NODES] + jnp.concatenate([b1_col] * 8, axis=1)
    hidden_t = jnp.maximum(pre, 0.0).astype(BF16)
    live = jnp.transpose(jnp.where(pre > 0.0, 1.0, 0.0))
    dw2t = jnp.transpose(dot(hidden_t, dz2))
    for h in range(2):
        a2[h, :112, :] = dw2t[:112, h * 256:(h + 1) * 256]
        a2[h, 112:, :128] = jnp.broadcast_to(db2, (8, 128))
        a2[h, 112:, 128:] = jnp.zeros((8, 128), F32)
    reduce_group(a2, half2, got2, tot2)
    w2t = w2t_ref[...]
    grad_h = dot(dz2[:, :OUT], w2t)
    dy = jnp.where(live > 0.5, grad_h, 0.0)
    hub_dy = jnp.where(y_hub + b1 > 0.0, dot(hub_dz2[:, :OUT], w2t), 0.0)
    db1 = jnp.sum(dy, axis=0, keepdims=True)
    for j, piece in enumerate(split3(dy)):
        dy_s[j, :NODES, :] = piece
    for j, piece in enumerate(split3(hub_dy)):
        dy_s[j, NODES:NODES + HUBS, :] = piece
        dy_s[j, NODES + HUBS:, :] = jnp.zeros((112, HID), BF16)

    def grad1(rows):
        acc = dot(lo_ref[rows, :], dy_s[0])
        acc = acc + dot(mid_ref[rows, :], dy_s[1])
        acc = acc + dot(hi_ref[rows, :], dy_s[2])
        acc = acc + dot(mid_ref[rows, :], dy_s[0])
        acc = acc + dot(hi_ref[rows, :], dy_s[1])
        return acc + dot(hi_ref[rows, :], dy_s[0])

    ret_s[...] = grad1(pl.ds(NODES, HALO + HUBS))
    for q in range(4):
        sd[q, :SEND, :] = ret_s[q * SEND:(q + 1) * SEND, :]
        sd[q, SEND:, :] = ret_s[HALO:, :]
    rd[me] = sd[me]
    round_d = [remote(sd.at[q], rd.at[me], q) for q in peers]

    for m in range(2):
        g1_s[m * 512:(m + 1) * 512, :] = grad1(pl.ds(m * 512, 512))
    wait_all(round_d)
    back = jnp.where(lax.broadcasted_iota(jnp.int32, (4, SEND, HID), 0) != me, rd[:, :SEND, :], 0.0).reshape(HALO, HID)
    hub_back = (rd[0, SEND:, :] + rd[1, SEND:, :]) + (rd[2, SEND:, :] + rd[3, SEND:, :])
    dz1 = g1_s[...]
    for piece in split3(back):
        dz1 = dz1 + dot(halo_pick, piece)
    for piece in split3(hub_back):
        dz1 = dz1 + dot(hub_put, piece)
    dz1_s[...] = dz1.astype(BF16)
    dw1 = dot(xt_ref[...], dz1_s[...])

    dxt_ref[...] = dot_nt(w1_ref[...], dz1_s[...])
    for h in range(2):
        a1[h, :FIN, :] = dw1[:, h * 256:(h + 1) * 256]
        a1[h, FIN:, :] = jnp.broadcast_to(db1[:, h * 256:(h + 1) * 256], (8, 256))
    reduce_group(a1, half1, got1, tot1)
    for h in range(2):
        dw1_ref[:, h * 256:(h + 1) * 256] = tot1[h, :FIN, :]
        db1_ref[:, h * 256:(h + 1) * 256] = tot1[h, FIN:FIN + 1, :]
    for h in range(2):
        dw2t_ref[:, h * 256:(h + 1) * 256] = tot2[h, :OUT, :]
    db2_ref[...] = tot2[0, 112:113, :OUT]


def step(hi, mid, lo, x, w1, b1, w2, dh, send, hubs):
    vmem = pl.BlockSpec(memory_space=pltpu.VMEM)
    out = lambda *shape: jax.ShapeDtypeStruct(shape, F32)
    f32 = lambda *shape: pltpu.VMEM(shape, F32)
    b16 = lambda *shape: pltpu.VMEM(shape, BF16)
    return pl.pallas_call(
        step_kernel,
        out_shape=(out(FIN, NODES), out(FIN, HID), out(OUT, HID), out(1, HID), out(1, OUT)),
        in_specs=[vmem] * 10,
        out_specs=(vmem,) * 5,
        scratch_shapes=[
            f32(1, 384), b16(NODES, 384), b16(4, 96, FIN), b16(4, 96, FIN), f32(HUBS, 128), f32(4, HUBS, 128),
            b16(HID, NODES + HALO), f32(HID, COLS), b16(COLS, 384), f32(NODES, 128), f32(HALO + HUBS, 128),
            f32(4, SEND + HUBS, 128), f32(4, SEND + HUBS, 128), f32(HUBS, HID), f32(4, HUBS, HID),
            b16(3, COLS, HID), f32(NODES, HID), f32(4, SEND + HUBS, HID), f32(4, SEND + HUBS, HID),
            f32(HALO + HUBS, HID), b16(NODES, HID),
            f32(2, 120, 256), f32(120, 256), f32(2, 120, 256), f32(2, 120, 256),
            f32(2, 208, 256), f32(208, 256), f32(2, 208, 256), f32(2, 208, 256),
            pltpu.SemaphoreType.DMA((24,)), pltpu.SemaphoreType.DMA((24,)),
        ],
        compiler_params=pltpu.CompilerParams(collective_id=0, has_side_effects=True, vmem_limit_bytes=48 << 20),
        name="step",
    )(hi, mid, lo, x, w1, b1, w2, dh, send, hubs)


def solution(mesh):
    vertex_spec = P(("data", "graph"))
    vertex_rows = P(("data", "graph"), None)
    part_spec = P("data")
    part_rows = P("data", None)
    replicated = P()

    def device_step(x, dst, src, w, send, hub_ids, w_first, b_first, w_second, dy_out):
        hi, mid, lo = build(hub_ids, dst, src, w)
        dx, dw1, dw2, db1, db2 = step(
            hi, mid, lo, x.T, w_first, b_first.reshape(1, HID), w_second.T, dy_out.T, send.reshape(1, HALO), hub_ids.reshape(1, HUBS))
        return dx.T, dw1, dw2.T, db1.reshape(HID), db2.reshape(OUT)

    return jax.shard_map(
        device_step,
        mesh=mesh,
        in_specs=(vertex_rows, vertex_spec, vertex_spec, vertex_spec, vertex_spec, part_spec, replicated, replicated, replicated, vertex_rows),
        out_specs=(vertex_rows, part_rows, part_rows, part_spec, part_spec),
        check_vma=False,
    )
```

```python
import functools

import jax
import jax.numpy as jnp
from jax import lax
from jax.experimental import pallas as pl
from jax.experimental.pallas import tpu as pltpu
from jax.sharding import PartitionSpec as P

F32, BF16 = jnp.float32, jnp.bfloat16
NODES, SEND, HALO, HUBS = 1024, 64, 256, 16
TABLE = NODES + HALO + HUBS
TILES = 9
COLS = TILES * 128
ROWS = TILES * TABLE
EDGES = 16384
HID, OUT, FIN = 512, 107, 200

ACCS = 4
GROUP = 2
CHUNK = 32
PARTS = 128 // CHUNK
NT = (((1,), (1,)), ((), ()))


def split3(x):
    hi = x.astype(BF16)
    rest = x - hi.astype(F32)
    mid = rest.astype(BF16)
    return hi, mid, (rest - mid.astype(F32)).astype(BF16)


def dot(a, b):
    return jnp.dot(a, b, preferred_element_type=F32)


def dot_nt(a, b):
    return lax.dot_general(a, b, NT, preferred_element_type=F32)


def build_kernel(hub_ref, dst_ref, src_ref, w_ref, hi_ref, mid_ref, lo_ref, row_ref, lane_ref, perm_ref, val_a, val_b, sem, *rest):
    row_smem, accs = rest[:8], rest[8:]
    base = lax.axis_index("graph") * NODES
    dst, src = dst_ref[...], src_ref[...]
    new_dst, new_src = dst, src
    for k in range(HUBS):
        local = hub_ref[k] - base
        local = jnp.where((local >= 0) & (local < NODES), local, -1)
        new_dst = jnp.where(dst == local, NODES + k, new_dst)
        new_src = jnp.where(src == local, NODES + HALO + k, new_src)
    row_ref[...] = (new_dst >> 7) * TABLE + new_src
    lane_ref[...] = new_dst & 127
    copies = []
    for s in range(8):
        perm_ref[s] = row_ref[pl.ds(s, 16, stride=8), :]
    for s in range(8):
        copies.append(pltpu.make_async_copy(perm_ref.at[s], row_smem[s], sem.at[s]))
        copies[-1].start()

    def zero(i, carry):
        for acc in accs:
            acc[pl.ds(pl.multiple_of(i * 48, 8), 48), :] = jnp.zeros((48, 128), F32)
        return carry

    lax.fori_loop(0, ROWS // 48, zero, 0)
    iota = lax.broadcasted_iota(jnp.int32, (8, 128), 1)

    def wide(block, c):
        return jnp.broadcast_to(block[:, c:c + 1], (8, 128))

    def prep(n, val_ref):
        g, k = n // PARTS, n % PARTS
        at = pl.ds(pl.multiple_of(g * 8, 8), 8)
        shift = lax.rem(128 - k * CHUNK, 128)
        lanes, weights, rows = (pltpu.roll(ref[at, :], shift, 1) for ref in (lane_ref, w_ref, row_ref))
        same = [jnp.where(rows == pltpu.roll(rows, d, 1), 1.0, 0.0) for d in range(1, GROUP)]
        for c in range(0, CHUNK, GROUP):
            vals = []
            for i in range(GROUP):
                vals.append(jnp.where(wide(lanes, c + i) == iota, wide(weights, c + i), 0.0))
            for i in range(GROUP):
                total = vals[i]
                for j in range(i):
                    total = total + wide(same[i - j - 1], c + i) * vals[j]
                val_ref[(c + i) * 8:(c + i + 1) * 8, :] = total

    def scatter(n, val_ref):
        g, col = n // PARTS, (n % PARTS) * CHUNK
        for c in range(0, CHUNK, GROUP):
            for s in range(8):
                acc = accs[s % ACCS]
                rows = [row_smem[s][g, col + c + i] for i in range(GROUP)]
                sums = [acc[pl.ds(rows[i], 1), :] + val_ref[(c + i) * 8 + s:(c + i) * 8 + s + 1, :] for i in range(GROUP)]
                for r, total in zip(rows, sums):
                    acc[pl.ds(r, 1), :] = total

    prep(0, val_a)
    for copy in copies:
        copy.wait()
    last = 16 * PARTS - 1

    def turn(h, carry):
        prep(2 * h + 1, val_b)
        scatter(2 * h, val_a)
        prep(jnp.minimum(2 * h + 2, last), val_a)
        scatter(2 * h + 1, val_b)
        return carry

    lax.fori_loop(0, 8 * PARTS, turn, 0)

    def finish(i, carry):
        at = pl.multiple_of(i * 48, 16)
        for t in range(TILES):
            part = pl.ds(pl.multiple_of(t * TABLE + i * 48, 8), 48)
            total = accs[0][part, :]
            for acc in accs[1:]:
                total = total + acc[part, :]
            for piece, ref in zip(split3(total), (hi_ref, mid_ref, lo_ref)):
                ref[pl.ds(at, 48), t * 128:(t + 1) * 128] = piece
        return carry

    lax.fori_loop(0, TABLE // 48, finish, 0)


def build(hub_ids, dst, src, w):
    piece = jax.ShapeDtypeStruct((TABLE, COLS), BF16)
    square = lambda a: a.reshape(128, 128)
    vmem = pl.BlockSpec(memory_space=pltpu.VMEM)
    return pl.pallas_call(
        build_kernel,
        out_shape=(piece,) * 3,
        in_specs=[pl.BlockSpec(memory_space=pltpu.SMEM)] + [vmem] * 3,
        out_specs=(vmem,) * 3,
        scratch_shapes=[
            pltpu.VMEM((128, 128), jnp.int32),
            pltpu.VMEM((128, 128), jnp.int32),
            pltpu.VMEM((8, 16, 128), jnp.int32),
            pltpu.VMEM((1024, 128), F32),
            pltpu.VMEM((1024, 128), F32),
            pltpu.SemaphoreType.DMA((8,)),
        ] + [pltpu.SMEM((16, 128), jnp.int32)] * 8 + [pltpu.VMEM((ROWS, 128), F32)] * ACCS,
        compiler_params=pltpu.CompilerParams(vmem_limit_bytes=48 << 20),
        name="build",
    )(hub_ids, square(dst), square(src), square(w))


def step_kernel(
    hi_ref, mid_ref, lo_ref, xt_ref, w1_ref, b1_ref, w2t_ref, dht_ref, send_ref, hub_ref,
    dxt_ref, dw1_ref, dw2t_ref, db1_ref, db2_ref,
    row_s, pt_s, xs, xr, hs, hr, z_s, yt_s, d2_s, g2_s, g2h_s, rb, sb, ys, yr, dy_s, g1_s, sd, rd, ret_s, dz1_s,
    a2, half2, got2, tot2, a1, half1, got1, tot1, send_sem, recv_sem,
):
    me = lax.axis_index("graph")
    sibling = me + 1 - 2 * lax.rem(me, 2)
    across = lax.rem(me + 2, 4)
    core = lax.rem(me, 2)
    mesh_id = pl.DeviceIdType.MESH
    peers = [lax.rem(me + d, 4) for d in (1, 2, 3)]
    barrier = pltpu.get_barrier_semaphore()
    for q in peers:
        pl.semaphore_signal(barrier, inc=1, device_id={"graph": q}, device_id_type=mesh_id)
    pl.semaphore_wait(barrier, 3)
    used = [0]

    def remote(src, dst, q):
        i = used[0]
        used[0] += 1
        copy = pltpu.make_async_remote_copy(
            src_ref=src, dst_ref=dst, send_sem=send_sem.at[i], recv_sem=recv_sem.at[i],
            device_id={"graph": q}, device_id_type=mesh_id)
        copy.start()
        return copy

    pieces = (hi_ref, mid_ref, lo_ref)
    row_s[...] = jnp.full((1, 384), -1.0, F32)
    row_s[:, :HALO] = send_ref[...].astype(F32)
    hub_local = hub_ref[...] - me * NODES
    row_s[:, HALO:HALO + HUBS] = jnp.where((hub_local >= 0) & (hub_local < NODES), hub_local, -1).astype(F32)
    row = row_s[...]
    column = jnp.transpose(jnp.broadcast_to(row, (128, 384)))
    lane = lax.broadcasted_iota(jnp.int32, (272, 128), 1).astype(F32)
    picks = jnp.concatenate(
        [jnp.where(column[:272] == lane + float(j * 128), 1.0, 0.0).astype(BF16) for j in range(8)], axis=1)
    sub = lax.broadcasted_iota(jnp.int32, (NODES, 384), 0).astype(F32)
    pt_s[...] = jnp.where(sub == row, 1.0, 0.0).astype(BF16)
    xt = xt_ref[...]
    sent = dot_nt(picks, xt).astype(BF16)
    hub_col = column[HALO:HALO + HUBS]
    alias = [jnp.where((hub_col == row[:, j * 128:(j + 1) * 128]) & (hub_col >= 0.0), 1.0, 0.0) for j in range(2)]
    for q in range(4):
        xs[q, :SEND, :] = sent[q * SEND:(q + 1) * SEND]
        xs[q, SEND:SEND + HUBS, :] = sent[HALO:]
        part = alias[q // 2][:, (q % 2) * SEND:(q % 2 + 1) * SEND]
        xs[q, SEND + HUBS:, :SEND] = part.astype(BF16)
        xs[q, SEND + HUBS:, SEND:] = jnp.zeros((HUBS, FIN - SEND), BF16)
    d2_s[...] = jnp.zeros((COLS, 384), BF16)
    dht = dht_ref[...]
    dh = jnp.transpose(jnp.concatenate([dht, jnp.zeros((128 - OUT, NODES), F32)], axis=0))
    for j, piece in enumerate(split3(dh)):
        d2_s[:NODES, j * 128:(j + 1) * 128] = piece
    hub_pick = picks[HALO:]
    hub_dh = dot(hub_pick, d2_s[:NODES, :])
    hs[...] = (hub_dh[:, :128] + hub_dh[:, 128:256]) + hub_dh[:, 256:]
    xr[me] = jnp.zeros((96, FIN), BF16)
    hr[me] = hs[...]
    round_a = []
    for q in peers:
        round_a.append(remote(xs.at[q], xr.at[me], q))
        round_a.append(remote(hs, hr.at[me], q))
    db2 = jnp.sum(dh, axis=0, keepdims=True)

    def reduce_group(own, half, got, total):
        remote(own.at[1 - core], got.at[0], sibling).wait()
        half[...] = own[core] + got[0]
        remote(half, got.at[1], across).wait()
        total[core] = half[...] + got[1]
        remote(total.at[core], total.at[core], sibling).wait()

    w1t = jnp.transpose(jnp.concatenate([w1_ref[...], jnp.zeros((56, HID), BF16)], axis=0).astype(F32)).astype(BF16)[:, :FIN]
    z_s[:, :NODES] = dot(w1t, xt).astype(BF16)

    def forward_own(at):
        z = z_s[:, :NODES]
        acc = dot(z, hi_ref[:NODES, at])
        acc = acc + dot(z, mid_ref[:NODES, at])
        yt_s[:, at] = acc + dot(z, lo_ref[:NODES, at])

    def over_columns(body):
        def turn(n, carry):
            body(pl.ds(pl.multiple_of(n * 256, 256), 256))
            return carry

        lax.fori_loop(0, 4, turn, 0)

    over_columns(forward_own)
    forward_own(pl.ds(NODES, 128))

    def wait_all(copies):
        for copy in copies:
            copy.wait()

    wait_all(round_a)
    halo_x = jnp.concatenate([xr[q, :SEND, :] for q in range(4)], axis=0)
    own_hub_x = sent[HALO:].astype(F32)
    hub_x = own_hub_x
    for q in range(4):
        hub_x = hub_x + xr[q, SEND:SEND + HUBS, :].astype(F32)
    z_s[:, NODES:NODES + HALO] = dot_nt(w1t, halo_x).astype(BF16)
    z_hub = dot_nt(w1t, hub_x.astype(BF16)).astype(BF16)

    def forward_far(at):
        z = z_s[:, NODES:NODES + HALO]
        acc = yt_s[:, at]
        for ref in pieces:
            acc = acc + dot(z, ref[NODES:NODES + HALO, at])
        for ref in pieces:
            acc = acc + dot(z_hub, ref[NODES + HALO:, at])
        yt_s[:, at] = acc

    forward_far(pl.ds(NODES, 128))
    ys[...] = jnp.transpose(yt_s[:, NODES:])[:HUBS]
    yr[me] = ys[...]
    round_y = [remote(ys, yr.at[me], q) for q in peers]
    over_columns(forward_far)

    hub_dh = (hr[0] + hr[1]) + (hr[2] + hr[3])
    for j, piece in enumerate(split3(hub_dh)):
        d2_s[NODES:NODES + HUBS, j * 128:(j + 1) * 128] = piece

    def grad2(rows):
        a = dot(hi_ref[rows, :], d2_s[:, :256])
        b = dot(mid_ref[rows, :], d2_s[:, :256])
        c = dot(hi_ref[rows, :], d2_s[:, 256:]) + dot(lo_ref[rows, :], d2_s[:, :128])
        return ((c + b[:, 128:]) + (a[:, 128:] + b[:, :128])) + a[:, :128]

    g2h_s[...] = grad2(pl.ds(NODES, HALO + HUBS))
    far = g2h_s[:HALO, :]
    alias_row = jnp.concatenate([xr[q, SEND + HUBS:, :SEND] for q in range(4)], axis=1)
    hub_g2 = g2h_s[HALO:, :]
    for piece in split3(far):
        hub_g2 = hub_g2 + dot(alias_row, piece)
    for q in range(4):
        sb[q, :SEND, :] = far[q * SEND:(q + 1) * SEND]
        sb[q, SEND:, :] = hub_g2
    rb[me] = sb[me]
    round_b = [remote(sb.at[q], rb.at[me], q) for q in peers]

    def grad2_own(m, carry):
        at = pl.ds(pl.multiple_of(m * 256, 256), 256)
        g2_s[at, :] = grad2(at)
        return carry

    lax.fori_loop(0, 4, grad2_own, 0)
    wait_all(round_y)
    wait_all(round_b)

    hub_full = (rb[0, SEND:, :] + rb[1, SEND:, :]) + (rb[2, SEND:, :] + rb[3, SEND:, :])
    hub_dz2 = hub_full.astype(BF16)
    keep = lax.broadcasted_iota(jnp.int32, (4, SEND, 128), 0) != me
    back = jnp.where(keep, rb[:, :SEND, :], 0.0).reshape(HALO, 128)
    own = g2_s[...]
    halo_pick = pt_s[:, :HALO]
    hub_put = pt_s[:, HALO:HALO + HUBS]
    for piece in split3(back):
        own = own + dot(halo_pick, piece)
    is_hub = dot(hub_put, jnp.ones((HUBS, 128), BF16)) > 0.5
    dz2 = jnp.where(is_hub, dot(hub_put, hub_dz2), own).astype(BF16)

    y_hub = (yr[0] + yr[1]) + (yr[2] + yr[3])
    b1 = b1_ref[...]
    b1_col = jnp.transpose(jnp.broadcast_to(b1, (128, HID)))
    hub_sel = picks[HALO:]
    for piece in split3(jnp.transpose(jnp.concatenate([y_hub, jnp.zeros((112, HID), F32)], axis=0))):
        yt_s[:, :NODES] += dot(piece[:, :HUBS], hub_sel)
    pre = yt_s[:, :NODES] + jnp.concatenate([b1_col] * 8, axis=1)
    hidden_t = jnp.maximum(pre, 0.0).astype(BF16)
    live = jnp.transpose(jnp.where(pre > 0.0, 1.0, 0.0))
    dw2t = jnp.transpose(dot(hidden_t, dz2))
    for h in range(2):
        a2[h, :112, :] = dw2t[:112, h * 256:(h + 1) * 256]
        a2[h, 112:, :128] = jnp.broadcast_to(db2, (8, 128))
        a2[h, 112:, 128:] = jnp.zeros((8, 128), F32)
    reduce_group(a2, half2, got2, tot2)
    w2t = w2t_ref[...]
    grad_h = dot(dz2[:, :OUT], w2t)
    dy = jnp.where(live > 0.5, grad_h, 0.0)
    hub_dy = jnp.where(y_hub + b1 > 0.0, dot(hub_dz2[:, :OUT], w2t), 0.0)
    db1 = jnp.sum(dy, axis=0, keepdims=True)
    for j, piece in enumerate(split3(dy)):
        dy_s[j, :NODES, :] = piece
    for j, piece in enumerate(split3(hub_dy)):
        dy_s[j, NODES:NODES + HUBS, :] = piece
        dy_s[j, NODES + HUBS:, :] = jnp.zeros((112, HID), BF16)

    def grad1(rows):
        acc = dot(lo_ref[rows, :], dy_s[0])
        acc = acc + dot(mid_ref[rows, :], dy_s[1])
        acc = acc + dot(hi_ref[rows, :], dy_s[2])
        acc = acc + dot(mid_ref[rows, :], dy_s[0])
        acc = acc + dot(hi_ref[rows, :], dy_s[1])
        return acc + dot(hi_ref[rows, :], dy_s[0])

    ret_s[...] = grad1(pl.ds(NODES, HALO + HUBS))
    for q in range(4):
        sd[q, :SEND, :] = ret_s[q * SEND:(q + 1) * SEND, :]
        sd[q, SEND:, :] = ret_s[HALO:, :]
    rd[me] = sd[me]
    round_d = [remote(sd.at[q], rd.at[me], q) for q in peers]

    for m in range(2):
        g1_s[m * 512:(m + 1) * 512, :] = grad1(pl.ds(m * 512, 512))
    wait_all(round_d)
    back = jnp.where(lax.broadcasted_iota(jnp.int32, (4, SEND, HID), 0) != me, rd[:, :SEND, :], 0.0).reshape(HALO, HID)
    hub_back = (rd[0, SEND:, :] + rd[1, SEND:, :]) + (rd[2, SEND:, :] + rd[3, SEND:, :])
    dz1 = g1_s[...]
    for piece in split3(back):
        dz1 = dz1 + dot(halo_pick, piece)
    for piece in split3(hub_back):
        dz1 = dz1 + dot(hub_put, piece)
    dz1_s[...] = dz1.astype(BF16)
    dw1 = dot(xt_ref[...], dz1_s[...])

    dxt_ref[...] = dot_nt(w1_ref[...], dz1_s[...])
    for h in range(2):
        a1[h, :FIN, :] = dw1[:, h * 256:(h + 1) * 256]
        a1[h, FIN:, :] = jnp.broadcast_to(db1[:, h * 256:(h + 1) * 256], (8, 256))
    reduce_group(a1, half1, got1, tot1)
    for h in range(2):
        dw1_ref[:, h * 256:(h + 1) * 256] = tot1[h, :FIN, :]
        db1_ref[:, h * 256:(h + 1) * 256] = tot1[h, FIN:FIN + 1, :]
    for h in range(2):
        dw2t_ref[:, h * 256:(h + 1) * 256] = tot2[h, :OUT, :]
    db2_ref[...] = tot2[0, 112:113, :OUT]


def step(hi, mid, lo, x, w1, b1, w2, dh, send, hubs):
    vmem = pl.BlockSpec(memory_space=pltpu.VMEM)
    out = lambda *shape: jax.ShapeDtypeStruct(shape, F32)
    f32 = lambda *shape: pltpu.VMEM(shape, F32)
    b16 = lambda *shape: pltpu.VMEM(shape, BF16)
    return pl.pallas_call(
        step_kernel,
        out_shape=(out(FIN, NODES), out(FIN, HID), out(OUT, HID), out(1, HID), out(1, OUT)),
        in_specs=[vmem] * 10,
        out_specs=(vmem,) * 5,
        scratch_shapes=[
            f32(1, 384), b16(NODES, 384), b16(4, 96, FIN), b16(4, 96, FIN), f32(HUBS, 128), f32(4, HUBS, 128),
            b16(HID, NODES + HALO), f32(HID, COLS), b16(COLS, 384), f32(NODES, 128), f32(HALO + HUBS, 128),
            f32(4, SEND + HUBS, 128), f32(4, SEND + HUBS, 128), f32(HUBS, HID), f32(4, HUBS, HID),
            b16(3, COLS, HID), f32(NODES, HID), f32(4, SEND + HUBS, HID), f32(4, SEND + HUBS, HID),
            f32(HALO + HUBS, HID), b16(NODES, HID),
            f32(2, 120, 256), f32(120, 256), f32(2, 120, 256), f32(2, 120, 256),
            f32(2, 208, 256), f32(208, 256), f32(2, 208, 256), f32(2, 208, 256),
            pltpu.SemaphoreType.DMA((24,)), pltpu.SemaphoreType.DMA((24,)),
        ],
        compiler_params=pltpu.CompilerParams(collective_id=0, has_side_effects=True, vmem_limit_bytes=48 << 20),
        name="step",
    )(hi, mid, lo, x, w1, b1, w2, dh, send, hubs)


def solution(mesh):
    vertex_spec = P(("data", "graph"))
    vertex_rows = P(("data", "graph"), None)
    part_spec = P("data")
    part_rows = P("data", None)
    replicated = P()

    def device_step(x, dst, src, w, send, hub_ids, w_first, b_first, w_second, dy_out):
        hi, mid, lo = build(hub_ids, dst, src, w)
        dx, dw1, dw2, db1, db2 = step(
            hi, mid, lo, x.T, w_first, b_first.reshape(1, HID), w_second.T, dy_out.T, send.reshape(1, HALO), hub_ids.reshape(1, HUBS))
        return dx.T, dw1, dw2.T, db1.reshape(HID), db2.reshape(OUT)

    return jax.shard_map(
        device_step,
        mesh=mesh,
        in_specs=(vertex_rows, vertex_spec, vertex_spec, vertex_spec, vertex_spec, part_spec, replicated, replicated, replicated, vertex_rows),
        out_specs=(vertex_rows, part_rows, part_rows, part_spec, part_spec),
        check_vma=False,
    )
```

```python
import functools

import jax
import jax.numpy as jnp
from jax import lax
from jax.experimental import pallas as pl
from jax.experimental.pallas import tpu as pltpu
from jax.sharding import PartitionSpec as P

F32, BF16 = jnp.float32, jnp.bfloat16
NODES, SEND, HALO, HUBS = 1024, 64, 256, 16
TABLE = NODES + HALO + HUBS
TILES = 9
COLS = TILES * 128
ROWS = TILES * TABLE
EDGES = 16384
HID, OUT, FIN = 512, 107, 200

ACCS = 4
GROUP = 2
CHUNK = 32
PARTS = 128 // CHUNK
BUILD_VMEM = 27 << 20
STEP_VMEM = 34 << 20
NT = (((1,), (1,)), ((), ()))


def split3(x):
    hi = x.astype(BF16)
    rest = x - hi.astype(F32)
    mid = rest.astype(BF16)
    return hi, mid, (rest - mid.astype(F32)).astype(BF16)


def dot(a, b):
    return jnp.dot(a, b, preferred_element_type=F32)


def dot_nt(a, b):
    return lax.dot_general(a, b, NT, preferred_element_type=F32)


def build_kernel(hub_hbm, dst_hbm, src_hbm, w_hbm, hi_ref, mid_ref, lo_ref, hub_ref, dst_ref, src_ref, w_ref, row_ref, lane_ref, perm_ref, val_a, val_b, sem, *rest):
    row_smem, accs = rest[:8], rest[8:]
    loads = []
    for i, (a, b) in enumerate(((hub_hbm, hub_ref), (dst_hbm, dst_ref), (src_hbm, src_ref), (w_hbm, w_ref))):
        loads.append(pltpu.make_async_copy(a, b, sem.at[8 + i]))
        loads[-1].start()

    def zero(i, carry):
        for acc in accs:
            acc[pl.ds(pl.multiple_of(i * 48, 8), 48), :] = jnp.zeros((48, 128), F32)
        return carry

    lax.fori_loop(0, ROWS // 48, zero, 0)
    for load in loads:
        load.wait()
    base = lax.axis_index("graph") * NODES
    dst, src = dst_ref[...], src_ref[...]
    new_dst, new_src = dst, src
    for k in range(HUBS):
        local = hub_ref[k] - base
        local = jnp.where((local >= 0) & (local < NODES), local, -1)
        new_dst = jnp.where(dst == local, NODES + k, new_dst)
        new_src = jnp.where(src == local, NODES + HALO + k, new_src)
    row_ref[...] = (new_dst >> 7) * TABLE + new_src
    lane_ref[...] = new_dst & 127
    copies = []
    for s in range(8):
        perm_ref[s] = row_ref[pl.ds(s, 16, stride=8), :]
    for s in range(8):
        copies.append(pltpu.make_async_copy(perm_ref.at[s], row_smem[s], sem.at[s]))
        copies[-1].start()

    iota = lax.broadcasted_iota(jnp.int32, (8, 128), 1)

    def wide(block, c):
        return jnp.broadcast_to(block[:, c:c + 1], (8, 128))

    def prep(n, val_ref):
        g, k = n // PARTS, n % PARTS
        at = pl.ds(pl.multiple_of(g * 8, 8), 8)
        shift = lax.rem(128 - k * CHUNK, 128)
        lanes, weights, rows = (pltpu.roll(ref[at, :], shift, 1) for ref in (lane_ref, w_ref, row_ref))
        same = [jnp.where(rows == pltpu.roll(rows, d, 1), 1.0, 0.0) for d in range(1, GROUP)]
        for c in range(0, CHUNK, GROUP):
            vals = []
            for i in range(GROUP):
                vals.append(jnp.where(wide(lanes, c + i) == iota, wide(weights, c + i), 0.0))
            for i in range(GROUP):
                total = vals[i]
                for j in range(i):
                    total = total + wide(same[i - j - 1], c + i) * vals[j]
                val_ref[(c + i) * 8:(c + i + 1) * 8, :] = total

    def scatter(n, val_ref):
        g, col = n // PARTS, (n % PARTS) * CHUNK
        for c in range(0, CHUNK, GROUP):
            for s in range(8):
                acc = accs[s % ACCS]
                rows = [row_smem[s][g, col + c + i] for i in range(GROUP)]
                sums = [acc[pl.ds(rows[i], 1), :] + val_ref[(c + i) * 8 + s:(c + i) * 8 + s + 1, :] for i in range(GROUP)]
                for r, total in zip(rows, sums):
                    acc[pl.ds(r, 1), :] = total

    prep(0, val_a)
    for copy in copies:
        copy.wait()
    last = 16 * PARTS - 1

    def turn(h, carry):
        prep(2 * h + 1, val_b)
        scatter(2 * h, val_a)
        prep(jnp.minimum(2 * h + 2, last), val_a)
        scatter(2 * h + 1, val_b)
        return carry

    lax.fori_loop(0, 8 * PARTS, turn, 0)

    def finish(i, carry):
        at = pl.multiple_of(i * 48, 16)
        for t in range(TILES):
            part = pl.ds(pl.multiple_of(t * TABLE + i * 48, 8), 48)
            total = accs[0][part, :]
            for acc in accs[1:]:
                total = total + acc[part, :]
            for piece, ref in zip(split3(total), (hi_ref, mid_ref, lo_ref)):
                ref[pl.ds(at, 48), t * 128:(t + 1) * 128] = piece
        return carry

    lax.fori_loop(0, TABLE // 48, finish, 0)


def build(hub_ids, dst, src, w):
    piece = jax.ShapeDtypeStruct((TABLE, COLS), BF16)
    square = lambda a: a.reshape(128, 128)
    table = pltpu.VMEM((128, 128), jnp.int32)
    return pl.pallas_call(
        build_kernel,
        out_shape=(piece,) * 3,
        in_specs=[pl.BlockSpec(memory_space=pltpu.HBM)] * 4,
        out_specs=(pl.BlockSpec(memory_space=pltpu.VMEM),) * 3,
        scratch_shapes=[
            pltpu.SMEM((HUBS,), jnp.int32), table, table, pltpu.VMEM((128, 128), F32), table, table,
            pltpu.VMEM((8, 16, 128), jnp.int32), pltpu.VMEM((CHUNK * 8, 128), F32), pltpu.VMEM((CHUNK * 8, 128), F32),
            pltpu.SemaphoreType.DMA((12,)),
        ] + [pltpu.SMEM((16, 128), jnp.int32)] * 8 + [pltpu.VMEM((ROWS, 128), F32)] * ACCS,
        compiler_params=pltpu.CompilerParams(vmem_limit_bytes=BUILD_VMEM),
        name="build",
    )(hub_ids, square(dst), square(src), square(w))


def step_kernel(
    hi_ref, mid_ref, lo_ref, xt_hbm, w1_hbm, b1_hbm, w2t_hbm, dht_hbm, send_hbm, hub_hbm,
    dxt_ref, dw1_ref, dw2t_ref, db1_ref, db2_ref,
    xt_ref, w1_ref, b1_ref, w2t_ref, dht_ref, send_ref, hub_ref,
    row_s, pt_s, xs, xr, hs, hr, z_s, yt_s, d2_s, dhub_s, g2_s, g2h_s, rb, sb, ys, yr, dy_s, g1_s, sd, rd, dz1_s,
    a2, half2, got2, tot2, a1, half1, got1, tot1, load_sem, send_sem, recv_sem,
):
    me = lax.axis_index("graph")
    sibling = me + 1 - 2 * lax.rem(me, 2)
    across = lax.rem(me + 2, 4)
    core = lax.rem(me, 2)
    mesh_id = pl.DeviceIdType.MESH
    peers = [lax.rem(me + d, 4) for d in (1, 2, 3)]
    loads = []
    for i, (a, b) in enumerate((
            (send_hbm, send_ref), (hub_hbm, hub_ref), (xt_hbm, xt_ref), (dht_hbm, dht_ref), (w1_hbm, w1_ref), (b1_hbm, b1_ref),
            (w2t_hbm, w2t_ref))):
        loads.append(pltpu.make_async_copy(a, b, load_sem.at[i]))
        loads[-1].start()
    barrier = pltpu.get_barrier_semaphore()
    for q in peers:
        pl.semaphore_signal(barrier, inc=1, device_id={"graph": q}, device_id_type=mesh_id)
    for load in loads:
        load.wait()
    pl.semaphore_wait(barrier, 3)
    used = [0]

    def remote(src, dst, q):
        i = used[0]
        used[0] += 1
        copy = pltpu.make_async_remote_copy(
            src_ref=src, dst_ref=dst, send_sem=send_sem.at[i], recv_sem=recv_sem.at[i],
            device_id={"graph": q}, device_id_type=mesh_id)
        copy.start()
        return copy

    def wait_all(copies):
        for copy in copies:
            copy.wait()

    pieces = (hi_ref, mid_ref, lo_ref)
    row_s[...] = jnp.full((1, 384), -1.0, F32)
    row_s[:, :HALO] = send_ref[...].astype(F32)
    hub_local = hub_ref[...] - me * NODES
    row_s[:, HALO:HALO + HUBS] = jnp.where((hub_local >= 0) & (hub_local < NODES), hub_local, -1).astype(F32)
    row = row_s[...]
    column = jnp.transpose(jnp.broadcast_to(row, (128, 384)))
    lane = lax.broadcasted_iota(jnp.int32, (272, 128), 1).astype(F32)
    picks = jnp.concatenate(
        [jnp.where(column[:272] == lane + float(j * 128), 1.0, 0.0).astype(BF16) for j in range(8)], axis=1)
    xt = xt_ref[...]
    sent = dot_nt(picks, xt).astype(BF16)
    hub_col = column[HALO:HALO + HUBS]
    alias = [jnp.where((hub_col == row[:, j * 128:(j + 1) * 128]) & (hub_col >= 0.0), 1.0, 0.0) for j in range(2)]
    for q in range(4):
        xs[q, :SEND, :] = sent[q * SEND:(q + 1) * SEND]
        xs[q, SEND:SEND + HUBS, :] = sent[HALO:]
        part = alias[q // 2][:, (q % 2) * SEND:(q % 2 + 1) * SEND]
        xs[q, SEND + HUBS:, :SEND] = part.astype(BF16)
        xs[q, SEND + HUBS:, SEND:] = jnp.zeros((HUBS, FIN - SEND), BF16)
    xr[me] = jnp.zeros((96, FIN), BF16)
    dht = dht_ref[...]
    dh = jnp.transpose(jnp.concatenate([dht, jnp.zeros((128 - OUT, NODES), F32)], axis=0))
    for j, piece in enumerate(split3(dh)):
        d2_s[:, j * 128:(j + 1) * 128] = piece
    round_a = [remote(xs.at[q], xr.at[me], q) for q in peers]
    hub_dh = dot(picks[HALO:], d2_s[...])
    hs[...] = (hub_dh[:, :128] + hub_dh[:, 128:256]) + hub_dh[:, 256:]
    hr[me] = hs[...]
    db2 = jnp.sum(dh, axis=0, keepdims=True)
    round_a += [remote(hs, hr.at[me], q) for q in peers]
    sub = lax.broadcasted_iota(jnp.int32, (NODES, 384), 0).astype(F32)
    pt_s[...] = jnp.where(sub == row, 1.0, 0.0).astype(BF16)

    def grad2(rows, cols, right):
        a = dot(hi_ref[rows, cols], right[:, :256])
        b = dot(mid_ref[rows, cols], right[:, :256])
        c = dot(hi_ref[rows, cols], right[:, 256:]) + dot(lo_ref[rows, cols], right[:, :128])
        return ((c + b[:, 128:]) + (a[:, 128:] + b[:, :128])) + a[:, :128]

    own_cols, hub_cols = pl.ds(0, NODES), pl.ds(NODES, 128)
    far_rows = pl.ds(NODES, HALO + HUBS)
    g2h_s[...] = grad2(far_rows, own_cols, d2_s)

    def grad2_own(m, carry):
        at = pl.ds(pl.multiple_of(m * 256, 256), 256)
        g2_s[at, :] = grad2(at, own_cols, d2_s)
        return carry

    lax.fori_loop(0, 4, grad2_own, 0)
    w1t = jnp.transpose(jnp.concatenate([w1_ref[...], jnp.zeros((56, HID), BF16)], axis=0).astype(F32)).astype(BF16)[:, :FIN]
    z_s[:, :NODES] = dot(w1t, xt).astype(BF16)

    def forward_own(at):
        z = z_s[:, :NODES]
        acc = dot(z, hi_ref[:NODES, at])
        acc = acc + dot(z, mid_ref[:NODES, at])
        yt_s[:, at] = acc + dot(z, lo_ref[:NODES, at])

    def over_columns(body):
        def turn(n, carry):
            body(pl.ds(pl.multiple_of(n * 256, 256), 256))
            return carry

        lax.fori_loop(0, 4, turn, 0)

    forward_own(hub_cols)
    wait_all(round_a)

    halo_x = jnp.concatenate([xr[q, :SEND, :] for q in range(4)], axis=0)
    hub_x = sent[HALO:].astype(F32)
    for q in range(4):
        hub_x = hub_x + xr[q, SEND:SEND + HUBS, :].astype(F32)
    z_s[:, NODES:] = dot_nt(w1t, halo_x).astype(BF16)
    z_hub = dot_nt(w1t, hub_x.astype(BF16)).astype(BF16)

    def forward_far(at):
        z = z_s[:, NODES:]
        acc = yt_s[:, at]
        for ref in pieces:
            acc = acc + dot(z, ref[NODES:NODES + HALO, at])
        for ref in pieces:
            acc = acc + dot(z_hub, ref[NODES + HALO:, at])
        yt_s[:, at] = acc

    forward_far(hub_cols)
    ys[...] = jnp.transpose(yt_s[:, NODES:])[:HUBS]
    yr[me] = ys[...]
    hub_dh = (hr[0] + hr[1]) + (hr[2] + hr[3])
    for j, piece in enumerate(split3(hub_dh)):
        dhub_s[:HUBS, j * 128:(j + 1) * 128] = piece
    dhub_s[HUBS:, :] = jnp.zeros((128 - HUBS, 384), BF16)
    round_b = [remote(ys, yr.at[me], q) for q in peers]
    g2h_s[...] += grad2(far_rows, hub_cols, dhub_s)
    far = g2h_s[:HALO, :]
    alias_row = jnp.concatenate([xr[q, SEND + HUBS:, :SEND] for q in range(4)], axis=1)
    hub_g2 = g2h_s[HALO:, :]
    for piece in split3(far):
        hub_g2 = hub_g2 + dot(alias_row, piece)
    for q in range(4):
        sb[q, :SEND, :] = far[q * SEND:(q + 1) * SEND]
        sb[q, SEND:, :] = hub_g2
    rb[me] = sb[me]
    round_b += [remote(sb.at[q], rb.at[me], q) for q in peers]

    over_columns(forward_own)
    over_columns(forward_far)

    def grad2_hub(m, carry):
        at = pl.ds(pl.multiple_of(m * 256, 256), 256)
        g2_s[at, :] += grad2(at, hub_cols, dhub_s)
        return carry

    lax.fori_loop(0, 4, grad2_hub, 0)
    wait_all(round_b)

    hub_dz2 = ((rb[0, SEND:, :] + rb[1, SEND:, :]) + (rb[2, SEND:, :] + rb[3, SEND:, :])).astype(BF16)
    keep = lax.broadcasted_iota(jnp.int32, (4, SEND, 128), 0) != me
    back = jnp.where(keep, rb[:, :SEND, :], 0.0).reshape(HALO, 128)
    own = g2_s[...]
    halo_pick = pt_s[:, :HALO]
    hub_put = pt_s[:, HALO:HALO + HUBS]
    for piece in split3(back):
        own = own + dot(halo_pick, piece)
    is_hub = dot(hub_put, jnp.ones((HUBS, 128), BF16)) > 0.5
    dz2 = jnp.where(is_hub, dot(hub_put, hub_dz2), own).astype(BF16)

    y_hub = (yr[0] + yr[1]) + (yr[2] + yr[3])
    b1 = b1_ref[...]
    b1_col = jnp.transpose(jnp.broadcast_to(b1, (128, HID)))
    for piece in split3(jnp.transpose(jnp.concatenate([y_hub, jnp.zeros((112, HID), F32)], axis=0))):
        yt_s[:, :NODES] += dot(piece[:, :HUBS], picks[HALO:])
    pre = yt_s[:, :NODES] + jnp.concatenate([b1_col] * 8, axis=1)
    yt_s[:, :NODES] = pre
    live = jnp.transpose(jnp.where(pre > 0.0, 1.0, 0.0))
    w2t = w2t_ref[...]
    dy = jnp.where(live > 0.5, dot(dz2[:, :OUT], w2t), 0.0)
    hub_dy = jnp.where(y_hub + b1 > 0.0, dot(hub_dz2[:, :OUT], w2t), 0.0)
    db1 = jnp.sum(dy, axis=0, keepdims=True)
    for j, piece in enumerate(split3(dy)):
        dy_s[j, :NODES, :] = piece
    for j, piece in enumerate(split3(hub_dy)):
        dy_s[j, NODES:NODES + HUBS, :] = piece
        dy_s[j, NODES + HUBS:, :] = jnp.zeros((112, HID), BF16)

    class GroupSum:
        def __init__(self, own, half, got, total):
            self.own, self.half, self.got, self.total = own, half, got, total
            self.copy = remote(own.at[1 - core], got.at[0], sibling)

        def across(self):
            self.copy.wait()
            self.half[...] = self.own[core] + self.got[0]
            self.copy = remote(self.half, self.got.at[1], across)

        def back(self):
            self.copy.wait()
            self.total[core] = self.half[...] + self.got[1]
            self.copy = remote(self.total.at[core], self.total.at[core], sibling)

        def done(self):
            self.copy.wait()

    def grad1(rows, cols):
        acc = dot(lo_ref[rows, :], dy_s[0, :, cols])
        acc = acc + dot(mid_ref[rows, :], dy_s[1, :, cols])
        acc = acc + dot(hi_ref[rows, :], dy_s[2, :, cols])
        acc = acc + dot(mid_ref[rows, :], dy_s[0, :, cols])
        acc = acc + dot(hi_ref[rows, :], dy_s[1, :, cols])
        return acc + dot(hi_ref[rows, :], dy_s[0, :, cols])

    halves = (pl.ds(0, 256), pl.ds(256, 256))
    round_d = []
    for h, cols in enumerate(halves):
        ret = grad1(far_rows, cols)
        for q in range(4):
            sd[h, q, :SEND, :] = ret[q * SEND:(q + 1) * SEND]
            sd[h, q, SEND:, :] = ret[HALO:]
        rd[h, me] = sd[h, me]
        round_d.append([remote(sd.at[h, q], rd.at[h, me], q) for q in peers])

    dw2t = jnp.transpose(dot(jnp.maximum(yt_s[:, :NODES], 0.0).astype(BF16), dz2))
    for h in range(2):
        a2[h, :112, :] = dw2t[:112, h * 256:(h + 1) * 256]
        a2[h, 112:, :128] = jnp.broadcast_to(db2, (8, 128))
        a2[h, 112:, 128:] = jnp.zeros((8, 128), F32)

    def grad1_own(h, m):
        rows = pl.ds(m * 512, 512)
        g1_s[rows, halves[h]] = grad1(rows, halves[h])

    def finish(h):
        wait_all(round_d[h])
        cols = halves[h]
        keep = lax.broadcasted_iota(jnp.int32, (4, SEND, 256), 0) != me
        back = jnp.where(keep, rd[h, :, :SEND, :], 0.0).reshape(HALO, 256)
        hub_back = (rd[h, 0, SEND:, :] + rd[h, 1, SEND:, :]) + (rd[h, 2, SEND:, :] + rd[h, 3, SEND:, :])
        dz1 = g1_s[:, cols]
        for piece in split3(back):
            dz1 = dz1 + dot(halo_pick, piece)
        for piece in split3(hub_back):
            dz1 = dz1 + dot(hub_put, piece)
        dz1 = dz1.astype(BF16)
        dz1_s[:, cols] = dz1
        dw1 = dot(xt_ref[...], dz1)
        for i in range(2):
            at = slice(i * 128, (i + 1) * 128)
            a1[h, i, :FIN, :] = dw1[:, at]
            a1[h, i, FIN:, :] = jnp.broadcast_to(db1[:, h * 256 + i * 128:h * 256 + (i + 1) * 128], (8, 128))
        return GroupSum(a1.at[h], half1.at[h], got1.at[h], tot1.at[h])

    sum2 = GroupSum(a2, half2, got2, tot2)
    grad1_own(0, 0)
    sum2.across()
    grad1_own(0, 1)
    sum1 = [finish(0)]
    grad1_own(1, 0)
    sum1[0].across()
    sum2.back()
    grad1_own(1, 1)
    sum1.append(finish(1))
    sum1[0].back()
    sum2.done()
    for h in range(2):
        dw2t_ref[:, h * 256:(h + 1) * 256] = tot2[h, :OUT, :]
    db2_ref[...] = tot2[0, 112:113, :OUT]
    sum1[1].across()
    dxt_ref[...] = dot_nt(w1_ref[...], dz1_s[...])
    sum1[1].back()
    sum1[0].done()

    def put(h):
        for i in range(2):
            at = slice(h * 256 + i * 128, h * 256 + (i + 1) * 128)
            dw1_ref[:, at] = tot1[h, i, :FIN, :]
            db1_ref[:, at] = tot1[h, i, FIN:FIN + 1, :]

    put(0)
    sum1[1].done()
    put(1)


def step(hi, mid, lo, xt, w1, b1, w2t, dht, send, hubs):
    vmem = pl.BlockSpec(memory_space=pltpu.VMEM)
    out = lambda *shape: jax.ShapeDtypeStruct(shape, F32)
    f32 = lambda *shape: pltpu.VMEM(shape, F32)
    b16 = lambda *shape: pltpu.VMEM(shape, BF16)
    return pl.pallas_call(
        step_kernel,
        out_shape=(out(FIN, NODES), out(FIN, HID), out(OUT, HID), out(1, HID), out(1, OUT)),
        in_specs=[vmem] * 3 + [pl.BlockSpec(memory_space=pltpu.HBM)] * 7,
        out_specs=(vmem,) * 5,
        scratch_shapes=[
            b16(FIN, NODES), b16(FIN, HID), f32(1, HID), b16(OUT, HID), f32(OUT, NODES),
            pltpu.VMEM((1, HALO), jnp.int32), pltpu.VMEM((1, HUBS), jnp.int32),
            f32(1, 384), b16(NODES, 384), b16(4, 96, FIN), b16(4, 96, FIN), f32(HUBS, 128), f32(4, HUBS, 128),
            b16(HID, NODES + HALO), f32(HID, COLS), b16(NODES, 384), b16(128, 384), f32(NODES, 128), f32(HALO + HUBS, 128),
            f32(4, SEND + HUBS, 128), f32(4, SEND + HUBS, 128), f32(HUBS, HID), f32(4, HUBS, HID),
            b16(3, COLS, HID), f32(NODES, HID), f32(2, 4, SEND + HUBS, 256), f32(2, 4, SEND + HUBS, 256), b16(NODES, HID),
            f32(2, 120, 256), f32(120, 256), f32(2, 120, 256), f32(2, 120, 256),
            f32(2, 2, 208, 128), f32(2, 208, 128), f32(2, 2, 208, 128), f32(2, 2, 208, 128),
            pltpu.SemaphoreType.DMA((7,)), pltpu.SemaphoreType.DMA((28,)), pltpu.SemaphoreType.DMA((28,)),
        ],
        compiler_params=pltpu.CompilerParams(collective_id=0, has_side_effects=True, vmem_limit_bytes=STEP_VMEM),
        name="step",
    )(hi, mid, lo, xt, w1, b1, w2t, dht, send, hubs)


def emit_kernel(*refs):
    ins, outs, sem = refs[:5], refs[5:10], refs[10]
    copies = [pltpu.make_async_copy(a, b, sem.at[i]) for i, (a, b) in enumerate(zip(ins, outs))]
    for copy in copies:
        copy.start()
    for copy in copies:
        copy.wait()


def emit(*arrays):
    return pl.pallas_call(
        emit_kernel,
        out_shape=tuple(jax.ShapeDtypeStruct(a.shape, a.dtype) for a in arrays),
        in_specs=[pl.BlockSpec(memory_space=pltpu.VMEM)] * 5,
        out_specs=(pl.BlockSpec(memory_space=pltpu.HBM),) * 5,
        scratch_shapes=[pltpu.SemaphoreType.DMA((5,))],
        compiler_params=pltpu.CompilerParams(vmem_limit_bytes=4 << 20),
        name="emit",
    )(*arrays)


def solution(mesh):
    vertex_spec = P(("data", "graph"))
    vertex_rows = P(("data", "graph"), None)
    part_spec = P("data")
    part_rows = P("data", None)
    replicated = P()

    def device_step(x, dst, src, w, send, hub_ids, w_first, b_first, w_second, dy_out):
        hi, mid, lo = build(hub_ids, dst, src, w)
        dx, dw1, dw2, db1, db2 = emit(*step(
            hi, mid, lo, x.T, w_first, b_first.reshape(1, HID), w_second.T, dy_out.T, send.reshape(1, HALO), hub_ids.reshape(1, HUBS)))
        return dx.T, dw1, dw2.T, db1.reshape(HID), db2.reshape(OUT)

    return jax.shard_map(
        device_step,
        mesh=mesh,
        in_specs=(vertex_rows, vertex_spec, vertex_spec, vertex_spec, vertex_spec, part_spec, replicated, replicated, replicated, vertex_rows),
        out_specs=(vertex_rows, part_rows, part_rows, part_spec, part_spec),
        check_vma=False,
    )
```

```python
import functools

import jax
import jax.numpy as jnp
from jax import lax
from jax.experimental import pallas as pl
from jax.experimental.pallas import tpu as pltpu
from jax.sharding import PartitionSpec as P

F32, BF16 = jnp.float32, jnp.bfloat16
NODES, SEND, HALO, HUBS = 1024, 64, 256, 16
TABLE = NODES + HALO + HUBS
TILES = 9
COLS = TILES * 128
ROWS = TILES * TABLE
EDGES = 16384
HID, OUT, FIN = 512, 107, 200

ACCS = 4
GROUP = 2
CHUNK = 32
PARTS = 128 // CHUNK
BUILD_VMEM = 27 << 20
STEP_VMEM = 34 << 20
NT = (((1,), (1,)), ((), ()))


def split3(x):
    hi = x.astype(BF16)
    rest = x - hi.astype(F32)
    mid = rest.astype(BF16)
    return hi, mid, (rest - mid.astype(F32)).astype(BF16)


def in_hbm(a):
    return pltpu.with_memory_space_constraint(a, pltpu.HBM)


def dot(a, b):
    return jnp.dot(a, b, preferred_element_type=F32)


def dot_nt(a, b):
    return lax.dot_general(a, b, NT, preferred_element_type=F32)


def build_kernel(hub_hbm, dst_hbm, src_hbm, w_hbm, hi_ref, mid_ref, lo_ref, hub_ref, dst_ref, src_ref, w_ref, row_ref, lane_ref, perm_ref, val_a, val_b, sem, *rest):
    row_smem, accs = rest[:8], rest[8:]
    loads = []
    for i, (a, b) in enumerate(((hub_hbm, hub_ref), (dst_hbm, dst_ref), (src_hbm, src_ref), (w_hbm, w_ref))):
        loads.append(pltpu.make_async_copy(a, b, sem.at[8 + i]))
        loads[-1].start()

    def zero(i, carry):
        for acc in accs:
            acc[pl.ds(pl.multiple_of(i * 48, 8), 48), :] = jnp.zeros((48, 128), F32)
        return carry

    lax.fori_loop(0, ROWS // 48, zero, 0)
    for load in loads:
        load.wait()
    base = lax.axis_index("graph") * NODES
    dst, src = dst_ref[...], src_ref[...]
    new_dst, new_src = dst, src
    for k in range(HUBS):
        local = hub_ref[k] - base
        local = jnp.where((local >= 0) & (local < NODES), local, -1)
        new_dst = jnp.where(dst == local, NODES + k, new_dst)
        new_src = jnp.where(src == local, NODES + HALO + k, new_src)
    row_ref[...] = (new_dst >> 7) * TABLE + new_src
    lane_ref[...] = new_dst & 127
    copies = []
    for s in range(8):
        perm_ref[s] = row_ref[pl.ds(s, 16, stride=8), :]
    for s in range(8):
        copies.append(pltpu.make_async_copy(perm_ref.at[s], row_smem[s], sem.at[s]))
        copies[-1].start()

    iota = lax.broadcasted_iota(jnp.int32, (8, 128), 1)

    def wide(block, c):
        return jnp.broadcast_to(block[:, c:c + 1], (8, 128))

    def prep(n, val_ref):
        g, k = n // PARTS, n % PARTS
        at = pl.ds(pl.multiple_of(g * 8, 8), 8)
        shift = lax.rem(128 - k * CHUNK, 128)
        lanes, weights, rows = (pltpu.roll(ref[at, :], shift, 1) for ref in (lane_ref, w_ref, row_ref))
        same = [jnp.where(rows == pltpu.roll(rows, d, 1), 1.0, 0.0) for d in range(1, GROUP)]
        for c in range(0, CHUNK, GROUP):
            vals = []
            for i in range(GROUP):
                vals.append(jnp.where(wide(lanes, c + i) == iota, wide(weights, c + i), 0.0))
            for i in range(GROUP):
                total = vals[i]
                for j in range(i):
                    total = total + wide(same[i - j - 1], c + i) * vals[j]
                val_ref[(c + i) * 8:(c + i + 1) * 8, :] = total

    def scatter(n, val_ref):
        g, col = n // PARTS, (n % PARTS) * CHUNK
        for c in range(0, CHUNK, GROUP):
            for s in range(8):
                acc = accs[s % ACCS]
                rows = [row_smem[s][g, col + c + i] for i in range(GROUP)]
                sums = [acc[pl.ds(rows[i], 1), :] + val_ref[(c + i) * 8 + s:(c + i) * 8 + s + 1, :] for i in range(GROUP)]
                for r, total in zip(rows, sums):
                    acc[pl.ds(r, 1), :] = total

    prep(0, val_a)
    for copy in copies:
        copy.wait()
    last = 16 * PARTS - 1

    def turn(h, carry):
        prep(2 * h + 1, val_b)
        scatter(2 * h, val_a)
        prep(jnp.minimum(2 * h + 2, last), val_a)
        scatter(2 * h + 1, val_b)
        return carry

    lax.fori_loop(0, 8 * PARTS, turn, 0)

    def finish(i, carry):
        at = pl.multiple_of(i * 48, 16)
        for t in range(TILES):
            part = pl.ds(pl.multiple_of(t * TABLE + i * 48, 8), 48)
            total = accs[0][part, :]
            for acc in accs[1:]:
                total = total + acc[part, :]
            for piece, ref in zip(split3(total), (hi_ref, mid_ref, lo_ref)):
                ref[pl.ds(at, 48), t * 128:(t + 1) * 128] = piece
        return carry

    lax.fori_loop(0, TABLE // 48, finish, 0)


def build(hub_ids, dst, src, w):
    piece = jax.ShapeDtypeStruct((TABLE, COLS), BF16)
    square = lambda a: a.reshape(128, 128)
    table = pltpu.VMEM((128, 128), jnp.int32)
    return pl.pallas_call(
        build_kernel,
        out_shape=(piece,) * 3,
        in_specs=[pl.BlockSpec(memory_space=pltpu.HBM)] * 4,
        out_specs=(pl.BlockSpec(memory_space=pltpu.VMEM),) * 3,
        scratch_shapes=[
            pltpu.SMEM((HUBS,), jnp.int32), table, table, pltpu.VMEM((128, 128), F32), table, table,
            pltpu.VMEM((8, 16, 128), jnp.int32), pltpu.VMEM((CHUNK * 8, 128), F32), pltpu.VMEM((CHUNK * 8, 128), F32),
            pltpu.SemaphoreType.DMA((12,)),
        ] + [pltpu.SMEM((16, 128), jnp.int32)] * 8 + [pltpu.VMEM((ROWS, 128), F32)] * ACCS,
        compiler_params=pltpu.CompilerParams(vmem_limit_bytes=BUILD_VMEM),
        name="build",
    )(*(in_hbm(a) for a in (hub_ids, square(dst), square(src), square(w))))


def step_kernel(
    hi_ref, mid_ref, lo_ref, xt_hbm, w1_hbm, b1_hbm, w2t_hbm, dht_hbm, send_hbm, hub_hbm,
    dxt_ref, dw1_ref, dw2t_ref, db1_ref, db2_ref,
    xt_ref, w1_ref, b1_ref, w2t_ref, dht_ref, send_ref, hub_ref,
    row_s, pt_s, xs, xr, hs, hr, z_s, yt_s, d2_s, dhub_s, g2_s, g2h_s, rb, sb, ys, yr, dy_s, g1_s, sd, rd, dz1_s,
    a2, half2, got2, tot2, a1, half1, got1, tot1, load_sem, send_sem, recv_sem,
):
    me = lax.axis_index("graph")
    sibling = me + 1 - 2 * lax.rem(me, 2)
    across = lax.rem(me + 2, 4)
    core = lax.rem(me, 2)
    mesh_id = pl.DeviceIdType.MESH
    peers = [lax.rem(me + d, 4) for d in (1, 2, 3)]
    loads = []
    for i, (a, b) in enumerate((
            (send_hbm, send_ref), (hub_hbm, hub_ref), (xt_hbm, xt_ref), (dht_hbm, dht_ref), (w1_hbm, w1_ref), (b1_hbm, b1_ref),
            (w2t_hbm, w2t_ref))):
        loads.append(pltpu.make_async_copy(a, b, load_sem.at[i]))
        loads[-1].start()
    barrier = pltpu.get_barrier_semaphore()
    for q in peers:
        pl.semaphore_signal(barrier, inc=1, device_id={"graph": q}, device_id_type=mesh_id)
    for load in loads:
        load.wait()
    pl.semaphore_wait(barrier, 3)
    used = [0]

    def remote(src, dst, q):
        i = used[0]
        used[0] += 1
        copy = pltpu.make_async_remote_copy(
            src_ref=src, dst_ref=dst, send_sem=send_sem.at[i], recv_sem=recv_sem.at[i],
            device_id={"graph": q}, device_id_type=mesh_id)
        copy.start()
        return copy

    def wait_all(copies):
        for copy in copies:
            copy.wait()

    pieces = (hi_ref, mid_ref, lo_ref)
    row_s[...] = jnp.full((1, 384), -1.0, F32)
    row_s[:, :HALO] = send_ref[...].astype(F32)
    hub_local = hub_ref[...] - me * NODES
    row_s[:, HALO:HALO + HUBS] = jnp.where((hub_local >= 0) & (hub_local < NODES), hub_local, -1).astype(F32)
    row = row_s[...]
    column = jnp.transpose(jnp.broadcast_to(row, (128, 384)))
    lane = lax.broadcasted_iota(jnp.int32, (272, 128), 1).astype(F32)
    picks = jnp.concatenate(
        [jnp.where(column[:272] == lane + float(j * 128), 1.0, 0.0).astype(BF16) for j in range(8)], axis=1)
    xt = xt_ref[...]
    sent = dot_nt(picks, xt).astype(BF16)
    hub_col = column[HALO:HALO + HUBS]
    alias = [jnp.where((hub_col == row[:, j * 128:(j + 1) * 128]) & (hub_col >= 0.0), 1.0, 0.0) for j in range(2)]
    for q in range(4):
        xs[q, :SEND, :] = sent[q * SEND:(q + 1) * SEND]
        xs[q, SEND:SEND + HUBS, :] = sent[HALO:]
        part = alias[q // 2][:, (q % 2) * SEND:(q % 2 + 1) * SEND]
        xs[q, SEND + HUBS:, :SEND] = part.astype(BF16)
        xs[q, SEND + HUBS:, SEND:] = jnp.zeros((HUBS, FIN - SEND), BF16)
    xr[me] = jnp.zeros((96, FIN), BF16)
    dht = dht_ref[...]
    dh = jnp.transpose(jnp.concatenate([dht, jnp.zeros((128 - OUT, NODES), F32)], axis=0))
    for j, piece in enumerate(split3(dh)):
        d2_s[:, j * 128:(j + 1) * 128] = piece
    round_a = [remote(xs.at[q], xr.at[me], q) for q in peers]
    hub_dh = dot(picks[HALO:], d2_s[...])
    hs[...] = (hub_dh[:, :128] + hub_dh[:, 128:256]) + hub_dh[:, 256:]
    hr[me] = hs[...]
    db2 = jnp.sum(dh, axis=0, keepdims=True)
    round_a += [remote(hs, hr.at[me], q) for q in peers]
    sub = lax.broadcasted_iota(jnp.int32, (NODES, 384), 0).astype(F32)
    pt_s[...] = jnp.where(sub == row, 1.0, 0.0).astype(BF16)

    def grad2(rows, cols, right):
        a = dot(hi_ref[rows, cols], right[:, :256])
        b = dot(mid_ref[rows, cols], right[:, :256])
        c = dot(hi_ref[rows, cols], right[:, 256:]) + dot(lo_ref[rows, cols], right[:, :128])
        return ((c + b[:, 128:]) + (a[:, 128:] + b[:, :128])) + a[:, :128]

    own_cols, hub_cols = pl.ds(0, NODES), pl.ds(NODES, 128)
    far_rows = pl.ds(NODES, HALO + HUBS)
    g2h_s[...] = grad2(far_rows, own_cols, d2_s)

    def grad2_own(m, carry):
        at = pl.ds(pl.multiple_of(m * 256, 256), 256)
        g2_s[at, :] = grad2(at, own_cols, d2_s)
        return carry

    lax.fori_loop(0, 4, grad2_own, 0)
    w1t = jnp.transpose(jnp.concatenate([w1_ref[...], jnp.zeros((56, HID), BF16)], axis=0).astype(F32)).astype(BF16)[:, :FIN]
    z_s[:, :NODES] = dot(w1t, xt).astype(BF16)

    def forward_own(at):
        z = z_s[:, :NODES]
        acc = dot(z, hi_ref[:NODES, at])
        acc = acc + dot(z, mid_ref[:NODES, at])
        yt_s[:, at] = acc + dot(z, lo_ref[:NODES, at])

    def over_columns(body):
        def turn(n, carry):
            body(pl.ds(pl.multiple_of(n * 256, 256), 256))
            return carry

        lax.fori_loop(0, 4, turn, 0)

    forward_own(hub_cols)
    wait_all(round_a)

    halo_x = jnp.concatenate([xr[q, :SEND, :] for q in range(4)], axis=0)
    hub_x = sent[HALO:].astype(F32)
    for q in range(4):
        hub_x = hub_x + xr[q, SEND:SEND + HUBS, :].astype(F32)
    z_s[:, NODES:] = dot_nt(w1t, halo_x).astype(BF16)
    z_hub = dot_nt(w1t, hub_x.astype(BF16)).astype(BF16)

    def forward_far(at):
        z = z_s[:, NODES:]
        acc = yt_s[:, at]
        for ref in pieces:
            acc = acc + dot(z, ref[NODES:NODES + HALO, at])
        for ref in pieces:
            acc = acc + dot(z_hub, ref[NODES + HALO:, at])
        yt_s[:, at] = acc

    forward_far(hub_cols)
    ys[...] = jnp.transpose(yt_s[:, NODES:])[:HUBS]
    yr[me] = ys[...]
    hub_dh = (hr[0] + hr[1]) + (hr[2] + hr[3])
    for j, piece in enumerate(split3(hub_dh)):
        dhub_s[:HUBS, j * 128:(j + 1) * 128] = piece
    dhub_s[HUBS:, :] = jnp.zeros((128 - HUBS, 384), BF16)
    round_b = [remote(ys, yr.at[me], q) for q in peers]
    g2h_s[...] += grad2(far_rows, hub_cols, dhub_s)
    far = g2h_s[:HALO, :]
    alias_row = jnp.concatenate([xr[q, SEND + HUBS:, :SEND] for q in range(4)], axis=1)
    hub_g2 = g2h_s[HALO:, :]
    for piece in split3(far):
        hub_g2 = hub_g2 + dot(alias_row, piece)
    for q in range(4):
        sb[q, :SEND, :] = far[q * SEND:(q + 1) * SEND]
        sb[q, SEND:, :] = hub_g2
    rb[me] = sb[me]
    round_b += [remote(sb.at[q], rb.at[me], q) for q in peers]

    over_columns(forward_own)
    over_columns(forward_far)

    def grad2_hub(m, carry):
        at = pl.ds(pl.multiple_of(m * 256, 256), 256)
        g2_s[at, :] += grad2(at, hub_cols, dhub_s)
        return carry

    lax.fori_loop(0, 4, grad2_hub, 0)
    wait_all(round_b)

    hub_dz2 = ((rb[0, SEND:, :] + rb[1, SEND:, :]) + (rb[2, SEND:, :] + rb[3, SEND:, :])).astype(BF16)
    keep = lax.broadcasted_iota(jnp.int32, (4, SEND, 128), 0) != me
    back = jnp.where(keep, rb[:, :SEND, :], 0.0).reshape(HALO, 128)
    own = g2_s[...]
    halo_pick = pt_s[:, :HALO]
    hub_put = pt_s[:, HALO:HALO + HUBS]
    for piece in split3(back):
        own = own + dot(halo_pick, piece)
    is_hub = dot(hub_put, jnp.ones((HUBS, 128), BF16)) > 0.5
    dz2 = jnp.where(is_hub, dot(hub_put, hub_dz2), own).astype(BF16)

    y_hub = (yr[0] + yr[1]) + (yr[2] + yr[3])
    b1 = b1_ref[...]
    b1_col = jnp.transpose(jnp.broadcast_to(b1, (128, HID)))
    for piece in split3(jnp.transpose(jnp.concatenate([y_hub, jnp.zeros((112, HID), F32)], axis=0))):
        yt_s[:, :NODES] += dot(piece[:, :HUBS], picks[HALO:])
    pre = yt_s[:, :NODES] + jnp.concatenate([b1_col] * 8, axis=1)
    yt_s[:, :NODES] = pre
    live = jnp.transpose(jnp.where(pre > 0.0, 1.0, 0.0))
    w2t = w2t_ref[...]
    dy = jnp.where(live > 0.5, dot(dz2[:, :OUT], w2t), 0.0)
    hub_dy = jnp.where(y_hub + b1 > 0.0, dot(hub_dz2[:, :OUT], w2t), 0.0)
    db1 = jnp.sum(dy, axis=0, keepdims=True)
    for j, piece in enumerate(split3(dy)):
        dy_s[j, :NODES, :] = piece
    for j, piece in enumerate(split3(hub_dy)):
        dy_s[j, NODES:NODES + HUBS, :] = piece
        dy_s[j, NODES + HUBS:, :] = jnp.zeros((112, HID), BF16)

    class GroupSum:
        def __init__(self, own, half, got, total):
            self.own, self.half, self.got, self.total = own, half, got, total
            self.copy = remote(own.at[1 - core], got.at[0], sibling)

        def across(self):
            self.copy.wait()
            self.half[...] = self.own[core] + self.got[0]
            self.copy = remote(self.half, self.got.at[1], across)

        def back(self):
            self.copy.wait()
            self.total[core] = self.half[...] + self.got[1]
            self.copy = remote(self.total.at[core], self.total.at[core], sibling)

        def done(self):
            self.copy.wait()

    def grad1(rows, cols):
        acc = dot(lo_ref[rows, :], dy_s[0, :, cols])
        acc = acc + dot(mid_ref[rows, :], dy_s[1, :, cols])
        acc = acc + dot(hi_ref[rows, :], dy_s[2, :, cols])
        acc = acc + dot(mid_ref[rows, :], dy_s[0, :, cols])
        acc = acc + dot(hi_ref[rows, :], dy_s[1, :, cols])
        return acc + dot(hi_ref[rows, :], dy_s[0, :, cols])

    halves = (pl.ds(0, 256), pl.ds(256, 256))
    round_d = []
    for h, cols in enumerate(halves):
        ret = grad1(far_rows, cols)
        for q in range(4):
            sd[h, q, :SEND, :] = ret[q * SEND:(q + 1) * SEND]
            sd[h, q, SEND:, :] = ret[HALO:]
        rd[h, me] = sd[h, me]
        round_d.append([remote(sd.at[h, q], rd.at[h, me], q) for q in peers])

    dw2t = jnp.transpose(dot(jnp.maximum(yt_s[:, :NODES], 0.0).astype(BF16), dz2))
    for h in range(2):
        a2[h, :112, :] = dw2t[:112, h * 256:(h + 1) * 256]
        a2[h, 112:, :128] = jnp.broadcast_to(db2, (8, 128))
        a2[h, 112:, 128:] = jnp.zeros((8, 128), F32)

    def grad1_own(h, m):
        rows = pl.ds(m * 512, 512)
        g1_s[rows, halves[h]] = grad1(rows, halves[h])

    def finish(h):
        wait_all(round_d[h])
        cols = halves[h]
        keep = lax.broadcasted_iota(jnp.int32, (4, SEND, 256), 0) != me
        back = jnp.where(keep, rd[h, :, :SEND, :], 0.0).reshape(HALO, 256)
        hub_back = (rd[h, 0, SEND:, :] + rd[h, 1, SEND:, :]) + (rd[h, 2, SEND:, :] + rd[h, 3, SEND:, :])
        dz1 = g1_s[:, cols]
        for piece in split3(back):
            dz1 = dz1 + dot(halo_pick, piece)
        for piece in split3(hub_back):
            dz1 = dz1 + dot(hub_put, piece)
        dz1 = dz1.astype(BF16)
        dz1_s[:, cols] = dz1
        dw1 = dot(xt_ref[...], dz1)
        for i in range(2):
            at = slice(i * 128, (i + 1) * 128)
            a1[h, i, :FIN, :] = dw1[:, at]
            a1[h, i, FIN:, :] = jnp.broadcast_to(db1[:, h * 256 + i * 128:h * 256 + (i + 1) * 128], (8, 128))
        return GroupSum(a1.at[h], half1.at[h], got1.at[h], tot1.at[h])

    sum2 = GroupSum(a2, half2, got2, tot2)
    grad1_own(0, 0)
    sum2.across()
    grad1_own(0, 1)
    sum1 = [finish(0)]
    grad1_own(1, 0)
    sum1[0].across()
    sum2.back()
    grad1_own(1, 1)
    sum1.append(finish(1))
    sum1[0].back()
    sum2.done()
    for h in range(2):
        dw2t_ref[:, h * 256:(h + 1) * 256] = tot2[h, :OUT, :]
    db2_ref[...] = tot2[0, 112:113, :OUT]
    sum1[1].across()
    dxt_ref[...] = dot_nt(w1_ref[...], dz1_s[...])
    sum1[1].back()
    sum1[0].done()

    def put(h):
        for i in range(2):
            at = slice(h * 256 + i * 128, h * 256 + (i + 1) * 128)
            dw1_ref[:, at] = tot1[h, i, :FIN, :]
            db1_ref[:, at] = tot1[h, i, FIN:FIN + 1, :]

    put(0)
    sum1[1].done()
    put(1)


def step(hi, mid, lo, xt, w1, b1, w2t, dht, send, hubs):
    vmem = pl.BlockSpec(memory_space=pltpu.VMEM)
    out = lambda *shape: jax.ShapeDtypeStruct(shape, F32)
    f32 = lambda *shape: pltpu.VMEM(shape, F32)
    b16 = lambda *shape: pltpu.VMEM(shape, BF16)
    return pl.pallas_call(
        step_kernel,
        out_shape=(out(FIN, NODES), out(FIN, HID), out(OUT, HID), out(1, HID), out(1, OUT)),
        in_specs=[vmem] * 3 + [pl.BlockSpec(memory_space=pltpu.HBM)] * 7,
        out_specs=(vmem,) * 5,
        scratch_shapes=[
            b16(FIN, NODES), b16(FIN, HID), f32(1, HID), b16(OUT, HID), f32(OUT, NODES),
            pltpu.VMEM((1, HALO), jnp.int32), pltpu.VMEM((1, HUBS), jnp.int32),
            f32(1, 384), b16(NODES, 384), b16(4, 96, FIN), b16(4, 96, FIN), f32(HUBS, 128), f32(4, HUBS, 128),
            b16(HID, NODES + HALO), f32(HID, COLS), b16(NODES, 384), b16(128, 384), f32(NODES, 128), f32(HALO + HUBS, 128),
            f32(4, SEND + HUBS, 128), f32(4, SEND + HUBS, 128), f32(HUBS, HID), f32(4, HUBS, HID),
            b16(3, COLS, HID), f32(NODES, HID), f32(2, 4, SEND + HUBS, 256), f32(2, 4, SEND + HUBS, 256), b16(NODES, HID),
            f32(2, 120, 256), f32(120, 256), f32(2, 120, 256), f32(2, 120, 256),
            f32(2, 2, 208, 128), f32(2, 208, 128), f32(2, 2, 208, 128), f32(2, 2, 208, 128),
            pltpu.SemaphoreType.DMA((7,)), pltpu.SemaphoreType.DMA((28,)), pltpu.SemaphoreType.DMA((28,)),
        ],
        compiler_params=pltpu.CompilerParams(collective_id=0, has_side_effects=True, vmem_limit_bytes=STEP_VMEM),
        name="step",
    )(hi, mid, lo, *(in_hbm(a) for a in (xt, w1, b1, w2t, dht, send, hubs)))


def emit_kernel(*refs):
    ins, outs, sem = refs[:5], refs[5:10], refs[10]
    copies = [pltpu.make_async_copy(a, b, sem.at[i]) for i, (a, b) in enumerate(zip(ins, outs))]
    for copy in copies:
        copy.start()
    for copy in copies:
        copy.wait()


def emit(*arrays):
    return pl.pallas_call(
        emit_kernel,
        out_shape=tuple(jax.ShapeDtypeStruct(a.shape, a.dtype) for a in arrays),
        in_specs=[pl.BlockSpec(memory_space=pltpu.VMEM)] * 5,
        out_specs=(pl.BlockSpec(memory_space=pltpu.HBM),) * 5,
        scratch_shapes=[pltpu.SemaphoreType.DMA((5,))],
        compiler_params=pltpu.CompilerParams(vmem_limit_bytes=4 << 20),
        name="emit",
    )(*arrays)


def solution(mesh):
    vertex_spec = P(("data", "graph"))
    vertex_rows = P(("data", "graph"), None)
    part_spec = P("data")
    part_rows = P("data", None)
    replicated = P()

    def device_step(x, dst, src, w, send, hub_ids, w_first, b_first, w_second, dy_out):
        hi, mid, lo = build(hub_ids, dst, src, w)
        dx, dw1, dw2, db1, db2 = emit(*step(
            hi, mid, lo, x.T, w_first, b_first.reshape(1, HID), w_second.T, dy_out.T, send.reshape(1, HALO), hub_ids.reshape(1, HUBS)))
        return dx.T, dw1, dw2.T, db1.reshape(HID), db2.reshape(OUT)

    return jax.shard_map(
        device_step,
        mesh=mesh,
        in_specs=(vertex_rows, vertex_spec, vertex_spec, vertex_spec, vertex_spec, part_spec, replicated, replicated, replicated, vertex_rows),
        out_specs=(vertex_rows, part_rows, part_rows, part_spec, part_spec),
        check_vma=False,
    )
```

```python
import functools

import jax
import jax.numpy as jnp
from jax import lax
from jax.experimental import pallas as pl
from jax.experimental.pallas import tpu as pltpu
from jax.sharding import PartitionSpec as P

F32, BF16 = jnp.float32, jnp.bfloat16
NODES, SEND, HALO, HUBS = 1024, 64, 256, 16
TABLE = NODES + HALO + HUBS
TILES = 9
COLS = TILES * 128
ROWS = TILES * TABLE
EDGES = 16384
HID, OUT, FIN = 512, 107, 200

ACCS = 4
GROUP = 2
CHUNK = 32
PARTS = 128 // CHUNK
BUILD_VMEM = 27 << 20
STEP_VMEM = 34 << 20
NT = (((1,), (1,)), ((), ()))


def split3(x):
    hi = x.astype(BF16)
    rest = x - hi.astype(F32)
    mid = rest.astype(BF16)
    return hi, mid, (rest - mid.astype(F32)).astype(BF16)


def in_hbm(a):
    return pltpu.with_memory_space_constraint(a, pltpu.HBM)


def dot(a, b):
    return jnp.dot(a, b, preferred_element_type=F32)


def dot_nt(a, b):
    return lax.dot_general(a, b, NT, preferred_element_type=F32)


def build_kernel(hub_hbm, dst_hbm, src_hbm, w_hbm, hi_ref, mid_ref, lo_ref, side_ref, hub_ref, dst_ref, src_ref, w_ref, row_ref, lane_ref, perm_ref, val_a, val_b, sem, *rest):
    row_smem, accs = rest[:8], rest[8:]
    loads = []
    for i, (a, b) in enumerate(((hub_hbm, hub_ref), (dst_hbm, dst_ref), (src_hbm, src_ref), (w_hbm, w_ref))):
        loads.append(pltpu.make_async_copy(a, b, sem.at[8 + i]))
        loads[-1].start()

    def zero(i, carry):
        for acc in accs:
            acc[pl.ds(pl.multiple_of(i * 48, 8), 48), :] = jnp.zeros((48, 128), F32)
        return carry

    lax.fori_loop(0, ROWS // 48, zero, 0)
    for load in loads:
        load.wait()
    base = lax.axis_index("graph") * NODES
    dst, src = dst_ref[...], src_ref[...]
    new_dst, new_src = dst, src
    for k in range(HUBS):
        local = hub_ref[k] - base
        local = jnp.where((local >= 0) & (local < NODES), local, -1)
        new_dst = jnp.where(dst == local, NODES + k, new_dst)
        new_src = jnp.where(src == local, NODES + HALO + k, new_src)
    row_ref[...] = (new_dst >> 7) * TABLE + new_src
    lane_ref[...] = new_dst & 127
    copies = []
    for s in range(8):
        perm_ref[s] = row_ref[pl.ds(s, 16, stride=8), :]
    for s in range(8):
        copies.append(pltpu.make_async_copy(perm_ref.at[s], row_smem[s], sem.at[s]))
        copies[-1].start()

    iota = lax.broadcasted_iota(jnp.int32, (8, 128), 1)

    def wide(block, c):
        return jnp.broadcast_to(block[:, c:c + 1], (8, 128))

    def prep(n, val_ref):
        g, k = n // PARTS, n % PARTS
        at = pl.ds(pl.multiple_of(g * 8, 8), 8)
        shift = lax.rem(128 - k * CHUNK, 128)
        lanes, weights, rows = (pltpu.roll(ref[at, :], shift, 1) for ref in (lane_ref, w_ref, row_ref))
        same = [jnp.where(rows == pltpu.roll(rows, d, 1), 1.0, 0.0) for d in range(1, GROUP)]
        for c in range(0, CHUNK, GROUP):
            vals = []
            for i in range(GROUP):
                vals.append(jnp.where(wide(lanes, c + i) == iota, wide(weights, c + i), 0.0))
            for i in range(GROUP):
                total = vals[i]
                for j in range(i):
                    total = total + wide(same[i - j - 1], c + i) * vals[j]
                val_ref[(c + i) * 8:(c + i + 1) * 8, :] = total

    def scatter(n, val_ref):
        g, col = n // PARTS, (n % PARTS) * CHUNK
        for c in range(0, CHUNK, GROUP):
            for s in range(8):
                acc = accs[s % ACCS]
                rows = [row_smem[s][g, col + c + i] for i in range(GROUP)]
                sums = [acc[pl.ds(rows[i], 1), :] + val_ref[(c + i) * 8 + s:(c + i) * 8 + s + 1, :] for i in range(GROUP)]
                for r, total in zip(rows, sums):
                    acc[pl.ds(r, 1), :] = total

    prep(0, val_a)
    for copy in copies:
        copy.wait()
    last = 16 * PARTS - 1

    def turn(h, carry):
        prep(2 * h + 1, val_b)
        scatter(2 * h, val_a)
        prep(jnp.minimum(2 * h + 2, last), val_a)
        scatter(2 * h + 1, val_b)
        return carry

    lax.fori_loop(0, 8 * PARTS, turn, 0)

    def finish(i, carry):
        at = pl.multiple_of(i * 48, 16)
        for t in range(TILES):
            part = pl.ds(pl.multiple_of(t * TABLE + i * 48, 8), 48)
            total = accs[0][part, :]
            for acc in accs[1:]:
                total = total + acc[part, :]
            parts = split3(total)
            if t < TILES - 1:
                for piece, ref in zip(parts, (hi_ref, mid_ref, lo_ref)):
                    ref[pl.ds(at, 48), t * 128:(t + 1) * 128] = piece
            else:
                side = parts[0].astype(F32)
                for i, j in enumerate((1, 2, 0, 1, 0)):
                    side = side + pltpu.roll(parts[j].astype(F32), (i + 1) * HUBS, 1)
                side_ref[pl.ds(at, 48), :] = side.astype(BF16)
        return carry

    lax.fori_loop(0, TABLE // 48, finish, 0)


def build(hub_ids, dst, src, w):
    piece = jax.ShapeDtypeStruct((TABLE, NODES), BF16)
    side = jax.ShapeDtypeStruct((TABLE, 128), BF16)
    square = lambda a: a.reshape(128, 128)
    table = pltpu.VMEM((128, 128), jnp.int32)
    return pl.pallas_call(
        build_kernel,
        out_shape=(piece, piece, piece, side),
        in_specs=[pl.BlockSpec(memory_space=pltpu.HBM)] * 4,
        out_specs=(pl.BlockSpec(memory_space=pltpu.VMEM),) * 4,
        scratch_shapes=[
            pltpu.SMEM((HUBS,), jnp.int32), table, table, pltpu.VMEM((128, 128), F32), table, table,
            pltpu.VMEM((8, 16, 128), jnp.int32), pltpu.VMEM((CHUNK * 8, 128), F32), pltpu.VMEM((CHUNK * 8, 128), F32),
            pltpu.SemaphoreType.DMA((12,)),
        ] + [pltpu.SMEM((16, 128), jnp.int32)] * 8 + [pltpu.VMEM((ROWS, 128), F32)] * ACCS,
        compiler_params=pltpu.CompilerParams(vmem_limit_bytes=BUILD_VMEM),
        name="build",
    )(*(in_hbm(a) for a in (hub_ids, square(dst), square(src), square(w))))


def step_kernel(
    hi_ref, mid_ref, lo_ref, side_ref, xt_hbm, w1_hbm, b1_hbm, w2t_hbm, dht_hbm, send_hbm, hub_hbm,
    dxt_ref, dw1_ref, dw2t_ref, db1_ref, db2_ref,
    xt_ref, w1_ref, b1_ref, w2t_ref, dht_ref, send_ref, hub_ref,
    sent_s, pt_s, xs, xr, hs, hr, z_s, yt_s, d2_s, dhub_s, g2_s, g2h_s, rb, sb, ys, yr, dy_s, dyh_s, g1_s, sd, rd, dz1_s,
    a2, half2, got2, tot2, a1, half1, got1, tot1, load_sem, send_sem, recv_sem,
):
    me = lax.axis_index("graph")
    sibling = me + 1 - 2 * lax.rem(me, 2)
    across = lax.rem(me + 2, 4)
    core = lax.rem(me, 2)
    mesh_id = pl.DeviceIdType.MESH
    peers = [lax.rem(me + d, 4) for d in (1, 2, 3)]
    loads = []
    for i, (a, b) in enumerate((
            (send_hbm, send_ref), (hub_hbm, hub_ref), (xt_hbm, xt_ref), (dht_hbm, dht_ref), (w1_hbm, w1_ref), (b1_hbm, b1_ref),
            (w2t_hbm, w2t_ref))):
        loads.append(pltpu.make_async_copy(a, b, load_sem.at[i]))
        loads[-1].start()
    barrier = pltpu.get_barrier_semaphore()
    for q in peers:
        pl.semaphore_signal(barrier, inc=1, device_id={"graph": q}, device_id_type=mesh_id)
    for load in loads:
        load.wait()
    pl.semaphore_wait(barrier, 3)
    used = [0]

    def remote(src, dst, q):
        i = used[0]
        used[0] += 1
        copy = pltpu.make_async_remote_copy(
            src_ref=src, dst_ref=dst, send_sem=send_sem.at[i], recv_sem=recv_sem.at[i],
            device_id={"graph": q}, device_id_type=mesh_id)
        copy.start()
        return copy

    def wait_all(copies):
        for copy in copies:
            copy.wait()

    pieces = (hi_ref, mid_ref, lo_ref)
    hub_local = hub_ref[...] - me * NODES
    hub_row = jnp.where((hub_local >= 0) & (hub_local < NODES), hub_local, -1).astype(F32)
    hub_block = jnp.concatenate([hub_row, jnp.full((1, SEND - HUBS), -1.0, F32)], axis=1)
    send_row = send_ref[...].astype(F32)
    row = jnp.concatenate([jnp.where(me == q, hub_block, send_row[:, q * SEND:(q + 1) * SEND]) for q in range(4)], axis=1)
    row3 = jnp.concatenate([hub_row] * 3 + [jnp.full((1, 128 - 3 * HUBS), -1.0, F32)], axis=1)
    column = jnp.transpose(jnp.broadcast_to(jnp.concatenate([row, row3], axis=1), (128, 384)))
    lane = lax.broadcasted_iota(jnp.int32, (HALO + 3 * HUBS, 128), 1).astype(F32)
    picks = jnp.concatenate(
        [jnp.where(column[:HALO + 3 * HUBS] == lane + float(j * 128), 1.0, 0.0).astype(BF16) for j in range(8)], axis=1)
    xt = xt_ref[...]
    sent_s[...] = dot_nt(picks[:HALO], xt).astype(BF16).reshape(4, SEND, FIN)
    hub_col = column[HALO:HALO + HUBS]
    alias = [jnp.where((hub_col == row[:, j * 128:(j + 1) * 128]) & (hub_col >= 0.0), 1.0, 0.0) for j in range(2)]
    own_hub_x = sent_s[me, :HUBS, :]
    for q in range(4):
        xs[q, :SEND, :] = sent_s[q]
        xs[q, SEND:SEND + HUBS, :] = own_hub_x
        part = alias[q // 2][:, (q % 2) * SEND:(q % 2 + 1) * SEND]
        xs[q, SEND + HUBS:, :SEND] = part.astype(BF16)
        xs[q, SEND + HUBS:, SEND:] = jnp.zeros((HUBS, FIN - SEND), BF16)
    xr[me] = jnp.zeros((96, FIN), BF16)
    dht = dht_ref[...]
    dh = jnp.transpose(jnp.concatenate([dht, jnp.zeros((128 - OUT, NODES), F32)], axis=0))
    for j, piece in enumerate(split3(dh)):
        d2_s[:, j * 128:(j + 1) * 128] = piece
    round_a = [remote(xs.at[q], xr.at[me], q) for q in peers]
    hub_dh = dot(picks[HALO:HALO + HUBS], d2_s[...])
    hs[...] = (hub_dh[:, :128] + hub_dh[:, 128:256]) + hub_dh[:, 256:]
    hr[me] = hs[...]
    db2 = jnp.sum(dh, axis=0, keepdims=True)
    round_a += [remote(hs, hr.at[me], q) for q in peers]
    sub = lax.broadcasted_iota(jnp.int32, (NODES, HALO), 0).astype(F32)
    pt_s[...] = jnp.where(sub == row, 1.0, 0.0).astype(BF16)

    def grad2(rows):
        a = dot(hi_ref[rows, :], d2_s[:, :256])
        b = dot(mid_ref[rows, :], d2_s[:, :256])
        c = dot(hi_ref[rows, :], d2_s[:, 256:]) + dot(lo_ref[rows, :], d2_s[:, :128])
        return ((c + b[:, 128:]) + (a[:, 128:] + b[:, :128])) + a[:, :128]

    far_rows = pl.ds(NODES, HALO + HUBS)
    g2h_s[...] = grad2(far_rows)

    def grad2_own(m, carry):
        at = pl.ds(pl.multiple_of(m * 256, 256), 256)
        g2_s[at, :] = grad2(at)
        return carry

    lax.fori_loop(0, 4, grad2_own, 0)
    w1t = jnp.transpose(jnp.concatenate([w1_ref[...], jnp.zeros((56, HID), BF16)], axis=0).astype(F32)).astype(BF16)[:, :FIN]
    z_s[:, :NODES] = dot(w1t, xt).astype(BF16)

    def forward_own(at):
        z = z_s[:, :NODES]
        acc = dot(z, hi_ref[:NODES, at])
        acc = acc + dot(z, mid_ref[:NODES, at])
        yt_s[:, at] = acc + dot(z, lo_ref[:NODES, at])

    def over_columns(body):
        def turn(n, carry):
            body(pl.ds(pl.multiple_of(n * 256, 256), 256))
            return carry

        lax.fori_loop(0, 4, turn, 0)

    y_side = dot(z_s[:, :NODES], side_ref[:NODES, :])
    wait_all(round_a)

    halo_x = jnp.concatenate([xr[q, :SEND, :] for q in range(4)], axis=0)
    hub_x = sent_s[me, :HUBS, :].astype(F32)
    for q in range(4):
        hub_x = hub_x + xr[q, SEND:SEND + HUBS, :].astype(F32)
    z_s[:, NODES:] = dot_nt(w1t, halo_x).astype(BF16)
    z_hub = dot_nt(w1t, jnp.concatenate([hub_x.astype(BF16)] * 3, axis=0)).astype(BF16)

    def forward_far(at):
        z = z_s[:, NODES:]
        acc = yt_s[:, at]
        for ref in pieces:
            acc = acc + dot(z, ref[NODES:NODES + HALO, at])
        hub_rows = jnp.concatenate([ref[NODES + HALO:, at] for ref in pieces], axis=0)
        yt_s[:, at] = acc + dot(z_hub, hub_rows)

    y_side = y_side + dot(z_s[:, NODES:], side_ref[NODES:NODES + HALO, :])
    y_side = jnp.transpose(y_side + dot(z_hub[:, :HUBS], side_ref[NODES + HALO:, :]))
    ys[...] = (y_side[:HUBS] + y_side[HUBS:2 * HUBS]) + y_side[2 * HUBS:3 * HUBS]
    yr[me] = ys[...]
    hub_dh = (hr[0] + hr[1]) + (hr[2] + hr[3])
    def side_by_side(x):
        hi, mid, lo = split3(x)
        return jnp.concatenate([hi, hi, hi, mid, mid, lo, jnp.zeros((32, x.shape[1]), BF16)], axis=0)

    dhub_s[...] = side_by_side(hub_dh)
    round_b = [remote(ys, yr.at[me], q) for q in peers]
    g2h_s[...] += dot(side_ref[far_rows, :], dhub_s[...])
    far = g2h_s[:HALO, :]
    alias_row = jnp.concatenate([xr[q, SEND + HUBS:, :SEND] for q in range(4)], axis=1)
    hub_g2 = g2h_s[HALO:, :]
    for piece in split3(far):
        hub_g2 = hub_g2 + dot(alias_row, piece)
    is_alias = dot(jnp.transpose(jnp.concatenate([alias_row.astype(F32), jnp.zeros((112, HALO), F32)], axis=0)).astype(BF16),
                   jnp.ones((128, 128), BF16))
    far = jnp.where(is_alias > 0.5, 0.0, far)
    for q in range(4):
        sb[q, :SEND, :] = far[q * SEND:(q + 1) * SEND]
        sb[q, SEND:, :] = hub_g2
    rb[me] = sb[me]
    round_b += [remote(sb.at[q], rb.at[me], q) for q in peers]

    over_columns(forward_own)
    over_columns(forward_far)

    def grad2_hub(m, carry):
        at = pl.ds(pl.multiple_of(m * 256, 256), 256)
        g2_s[at, :] += dot(side_ref[at, :], dhub_s[...])
        return carry

    lax.fori_loop(0, 4, grad2_hub, 0)
    wait_all(round_b)

    def returned(ref):
        hub_sum = (ref[0, SEND:, :] + ref[1, SEND:, :]) + (ref[2, SEND:, :] + ref[3, SEND:, :])
        ref[me, :HUBS, :] = hub_sum
        ref[me, HUBS:SEND, :] = jnp.zeros((SEND - HUBS, hub_sum.shape[1]), F32)
        return ref[:, :SEND, :].reshape(HALO, hub_sum.shape[1]), hub_sum

    back, hub_sum = returned(rb)
    hub_dz2 = hub_sum.astype(BF16)
    own = g2_s[...]
    for piece in split3(back):
        own = own + dot(pt_s[...], piece)
    dz2 = own.astype(BF16)

    y_hub = (yr[0] + yr[1]) + (yr[2] + yr[3])
    b1 = b1_ref[...]
    b1_col = jnp.transpose(jnp.broadcast_to(b1, (128, HID)))
    y_rows = jnp.concatenate([piece.astype(F32) for piece in split3(y_hub)] + [jnp.zeros((128 - 3 * HUBS, HID), F32)], axis=0)
    y_own = dot(jnp.transpose(y_rows).astype(BF16)[:, :3 * HUBS], picks[HALO:])
    pre = (yt_s[...] + y_own) + jnp.concatenate([b1_col] * 8, axis=1)
    yt_s[...] = pre
    live = jnp.transpose(jnp.where(pre > 0.0, 1.0, 0.0))
    w2t = w2t_ref[...]
    dy = jnp.where(live > 0.5, dot(dz2[:, :OUT], w2t), 0.0)
    hub_dy = jnp.where(y_hub + b1 > 0.0, dot(hub_dz2[:, :OUT], w2t), 0.0)
    db1 = jnp.sum(dy, axis=0, keepdims=True)
    for j, piece in enumerate(split3(dy)):
        dy_s[j] = piece
    dyh_s[...] = side_by_side(hub_dy)

    class GroupSum:
        def __init__(self, own, half, got, total):
            self.own, self.half, self.got, self.total = own, half, got, total
            self.copy = remote(own.at[1 - core], got.at[0], sibling)

        def across(self):
            self.copy.wait()
            self.half[...] = self.own[core] + self.got[0]
            self.copy = remote(self.half, self.got.at[1], across)

        def back(self):
            self.copy.wait()
            self.total[core] = self.half[...] + self.got[1]
            self.copy = remote(self.total.at[core], self.total.at[core], sibling)

        def done(self):
            self.copy.wait()

    def grad1(rows, cols):
        acc = dot(lo_ref[rows, :], dy_s[0, :, cols])
        acc = acc + dot(mid_ref[rows, :], dy_s[1, :, cols])
        acc = acc + dot(hi_ref[rows, :], dy_s[2, :, cols])
        acc = acc + dot(mid_ref[rows, :], dy_s[0, :, cols])
        acc = acc + dot(hi_ref[rows, :], dy_s[1, :, cols])
        acc = acc + dot(hi_ref[rows, :], dy_s[0, :, cols])
        return acc + dot(side_ref[rows, :], dyh_s[:, cols])

    halves = (pl.ds(0, 256), pl.ds(256, 256))
    round_d = []
    for h, cols in enumerate(halves):
        ret = grad1(far_rows, cols)
        for q in range(4):
            sd[h, q, :SEND, :] = ret[q * SEND:(q + 1) * SEND]
            sd[h, q, SEND:, :] = ret[HALO:]
        rd[h, me] = sd[h, me]
        round_d.append([remote(sd.at[h, q], rd.at[h, me], q) for q in peers])

    dw2t = jnp.transpose(dot(jnp.maximum(yt_s[...], 0.0).astype(BF16), dz2))
    for h in range(2):
        a2[h, :112, :] = dw2t[:112, h * 256:(h + 1) * 256]
        a2[h, 112:, :128] = jnp.broadcast_to(db2, (8, 128))
        a2[h, 112:, 128:] = jnp.zeros((8, 128), F32)

    def grad1_own(h, m):
        rows = pl.ds(m * 512, 512)
        g1_s[rows, halves[h]] = grad1(rows, halves[h])

    def finish(h):
        wait_all(round_d[h])
        cols = halves[h]
        back, _ = returned(rd.at[h])
        dz1 = g1_s[:, cols]
        for piece in split3(back):
            dz1 = dz1 + dot(pt_s[...], piece)
        dz1 = dz1.astype(BF16)
        dz1_s[:, cols] = dz1
        dw1 = dot(xt_ref[...], dz1)
        for i in range(2):
            at = slice(i * 128, (i + 1) * 128)
            a1[h, i, :FIN, :] = dw1[:, at]
            a1[h, i, FIN:, :] = jnp.broadcast_to(db1[:, h * 256 + i * 128:h * 256 + (i + 1) * 128], (8, 128))
        return GroupSum(a1.at[h], half1.at[h], got1.at[h], tot1.at[h])

    sum2 = GroupSum(a2, half2, got2, tot2)
    grad1_own(0, 0)
    sum2.across()
    grad1_own(0, 1)
    sum1 = [finish(0)]
    grad1_own(1, 0)
    sum1[0].across()
    sum2.back()
    grad1_own(1, 1)
    sum1.append(finish(1))
    sum1[0].back()
    sum2.done()
    for h in range(2):
        dw2t_ref[:, h * 256:(h + 1) * 256] = tot2[h, :OUT, :]
    db2_ref[...] = tot2[0, 112:113, :OUT]
    sum1[1].across()
    dxt_ref[...] = dot_nt(w1_ref[...], dz1_s[...])
    sum1[1].back()
    sum1[0].done()

    def put(h):
        for i in range(2):
            at = slice(h * 256 + i * 128, h * 256 + (i + 1) * 128)
            dw1_ref[:, at] = tot1[h, i, :FIN, :]
            db1_ref[:, at] = tot1[h, i, FIN:FIN + 1, :]

    put(0)
    sum1[1].done()
    put(1)


def step(hi, mid, lo, side, xt, w1, b1, w2t, dht, send, hubs):
    vmem = pl.BlockSpec(memory_space=pltpu.VMEM)
    out = lambda *shape: jax.ShapeDtypeStruct(shape, F32)
    f32 = lambda *shape: pltpu.VMEM(shape, F32)
    b16 = lambda *shape: pltpu.VMEM(shape, BF16)
    return pl.pallas_call(
        step_kernel,
        out_shape=(out(FIN, NODES), out(FIN, HID), out(OUT, HID), out(1, HID), out(1, OUT)),
        in_specs=[vmem] * 4 + [pl.BlockSpec(memory_space=pltpu.HBM)] * 7,
        out_specs=(vmem,) * 5,
        scratch_shapes=[
            b16(FIN, NODES), b16(FIN, HID), f32(1, HID), b16(OUT, HID), f32(OUT, NODES),
            pltpu.VMEM((1, HALO), jnp.int32), pltpu.VMEM((1, HUBS), jnp.int32),
            b16(4, SEND, FIN), b16(NODES, HALO), b16(4, 96, FIN), b16(4, 96, FIN), f32(HUBS, 128), f32(4, HUBS, 128),
            b16(HID, NODES + HALO), f32(HID, NODES), b16(NODES, 384), b16(128, 128), f32(NODES, 128), f32(HALO + HUBS, 128),
            f32(4, SEND + HUBS, 128), f32(4, SEND + HUBS, 128), f32(HUBS, HID), f32(4, HUBS, HID),
            b16(3, NODES, HID), b16(128, HID), f32(NODES, HID), f32(2, 4, SEND + HUBS, 256), f32(2, 4, SEND + HUBS, 256), b16(NODES, HID),
            f32(2, 120, 256), f32(120, 256), f32(2, 120, 256), f32(2, 120, 256),
            f32(2, 2, 208, 128), f32(2, 208, 128), f32(2, 2, 208, 128), f32(2, 2, 208, 128),
            pltpu.SemaphoreType.DMA((7,)), pltpu.SemaphoreType.DMA((28,)), pltpu.SemaphoreType.DMA((28,)),
        ],
        compiler_params=pltpu.CompilerParams(collective_id=0, has_side_effects=True, vmem_limit_bytes=STEP_VMEM),
        name="step",
    )(hi, mid, lo, side, *(in_hbm(a) for a in (xt, w1, b1, w2t, dht, send, hubs)))


def emit_kernel(*refs):
    ins, outs, sem = refs[:5], refs[5:10], refs[10]
    copies = [pltpu.make_async_copy(a, b, sem.at[i]) for i, (a, b) in enumerate(zip(ins, outs))]
    for copy in copies:
        copy.start()
    for copy in copies:
        copy.wait()


def emit(*arrays):
    return pl.pallas_call(
        emit_kernel,
        out_shape=tuple(jax.ShapeDtypeStruct(a.shape, a.dtype) for a in arrays),
        in_specs=[pl.BlockSpec(memory_space=pltpu.VMEM)] * 5,
        out_specs=(pl.BlockSpec(memory_space=pltpu.HBM),) * 5,
        scratch_shapes=[pltpu.SemaphoreType.DMA((5,))],
        compiler_params=pltpu.CompilerParams(vmem_limit_bytes=4 << 20),
        name="emit",
    )(*arrays)


def solution(mesh):
    vertex_spec = P(("data", "graph"))
    vertex_rows = P(("data", "graph"), None)
    part_spec = P("data")
    part_rows = P("data", None)
    replicated = P()

    def device_step(x, dst, src, w, send, hub_ids, w_first, b_first, w_second, dy_out):
        table = build(hub_ids, dst, src, w)
        dx, dw1, dw2, db1, db2 = emit(*step(
            *table, x.T, w_first, b_first.reshape(1, HID), w_second.T, dy_out.T, send.reshape(1, HALO), hub_ids.reshape(1, HUBS)))
        return dx.T, dw1, dw2.T, db1.reshape(HID), db2.reshape(OUT)

    return jax.shard_map(
        device_step,
        mesh=mesh,
        in_specs=(vertex_rows, vertex_spec, vertex_spec, vertex_spec, vertex_spec, part_spec, replicated, replicated, replicated, vertex_rows),
        out_specs=(vertex_rows, part_rows, part_rows, part_spec, part_spec),
        check_vma=False,
    )
```

```python
import functools

import jax
import jax.numpy as jnp
from jax import lax
from jax.experimental import pallas as pl
from jax.experimental.pallas import tpu as pltpu
from jax.sharding import PartitionSpec as P

F32, BF16 = jnp.float32, jnp.bfloat16
NODES, SEND, HALO, HUBS = 1024, 64, 256, 16
TABLE = NODES + HALO + HUBS
TILES = 9
COLS = TILES * 128
ROWS = TILES * TABLE
EDGES = 16384
HID, OUT, FIN = 512, 107, 200

ACCS = 4
GROUP = 4
BUILD_VMEM = 28 << 20
STEP_VMEM = 34 << 20
NT = (((1,), (1,)), ((), ()))


def split3(x):
    hi = x.astype(BF16)
    rest = x - hi.astype(F32)
    mid = rest.astype(BF16)
    return hi, mid, (rest - mid.astype(F32)).astype(BF16)


def in_hbm(a):
    return pltpu.with_memory_space_constraint(a, pltpu.HBM)


def dot(a, b):
    return jnp.dot(a, b, preferred_element_type=F32)


def dot_nt(a, b):
    return lax.dot_general(a, b, NT, preferred_element_type=F32)


def build_kernel(hub_hbm, dst_hbm, src_hbm, w_hbm, hi_ref, mid_ref, lo_ref, side_ref, hub_ref, dst_ref, src_ref, w_ref, row_ref, lane_ref, perm_ref, val_a, val_b, sem, *rest):
    row_smem, accs = rest[:8], rest[8:]
    loads = []
    for i, (a, b) in enumerate(((hub_hbm, hub_ref), (dst_hbm, dst_ref), (src_hbm, src_ref), (w_hbm, w_ref))):
        loads.append(pltpu.make_async_copy(a, b, sem.at[8 + i]))
        loads[-1].start()

    def zero(i, carry):
        for acc in accs:
            acc[pl.ds(pl.multiple_of(i * 48, 8), 48), :] = jnp.zeros((48, 128), F32)
        return carry

    lax.fori_loop(0, ROWS // 48, zero, 0)
    for load in loads:
        load.wait()
    base = lax.axis_index("graph") * NODES
    dst, src = dst_ref[...], src_ref[...]
    new_dst, new_src = dst, src
    for k in range(HUBS):
        local = hub_ref[k] - base
        local = jnp.where((local >= 0) & (local < NODES), local, -1)
        new_dst = jnp.where(dst == local, NODES + k, new_dst)
        new_src = jnp.where(src == local, NODES + HALO + k, new_src)
    row_ref[...] = (new_dst >> 7) * TABLE + new_src
    lane_ref[...] = new_dst & 127
    copies = []
    for s in range(8):
        perm_ref[s] = row_ref[pl.ds(s, 16, stride=8), :]
    for s in range(8):
        copies.append(pltpu.make_async_copy(perm_ref.at[s], row_smem[s], sem.at[s]))
        copies[-1].start()

    iota = lax.broadcasted_iota(jnp.int32, (8, 128), 1)

    def wide(block, c):
        return jnp.broadcast_to(block[:, c:c + 1], (8, 128))

    def prep(g, val_ref):
        at = pl.ds(pl.multiple_of(g * 8, 8), 8)
        lanes, weights, rows = lane_ref[at, :], w_ref[at, :], row_ref[at, :]
        place = lax.broadcasted_iota(jnp.int32, (8, 128), 1) % GROUP
        terms = [(lanes, weights)]
        for d in range(1, GROUP):
            same = (place >= d) & (rows == pltpu.roll(rows, d, 1))
            terms.append((pltpu.roll(lanes, d, 1), jnp.where(same, pltpu.roll(weights, d, 1), 0.0)))
        def one(s):
            total = None
            for lane, weight in terms:
                hit = jnp.broadcast_to(lane[s:s + 1, :], (128, 128)) == sub
                part = jnp.where(hit, jnp.broadcast_to(weight[s:s + 1, :], (128, 128)), 0.0)
                total = part if total is None else total + part
            val_ref[s * 128:(s + 1) * 128, :] = jnp.transpose(total)

        return one

    def scatter(g, val_ref, c):
        for s in range(8):
            acc = accs[s % ACCS]
            rows = [row_smem[s][g, c + i] for i in range(GROUP)]
            sums = [acc[pl.ds(rows[i], 1), :] + val_ref[s * 128 + c + i:s * 128 + c + i + 1, :] for i in range(GROUP)]
            for r, total in zip(rows, sums):
                acc[pl.ds(r, 1), :] = total

    def both(g, val_ref, next_g, next_ref):
        one = prep(next_g, next_ref)
        for c in range(0, 128, GROUP):
            if c % 16 == 0:
                one(c // 16)
            scatter(g, val_ref, c)

    sub = lax.broadcasted_iota(jnp.int32, (128, 128), 0)
    first = prep(0, val_a)
    for s in range(8):
        first(s)
    for copy in copies:
        copy.wait()

    def turn(h, carry):
        both(2 * h, val_a, 2 * h + 1, val_b)
        both(2 * h + 1, val_b, jnp.minimum(2 * h + 2, 15), val_a)
        return carry

    lax.fori_loop(0, 8, turn, 0)

    def finish(i, carry):
        at = pl.multiple_of(i * 16, 16)
        for t in range(TILES):
            part = pl.ds(pl.multiple_of(t * TABLE + i * 16, 8), 16)
            total = accs[0][part, :]
            for acc in accs[1:]:
                total = total + acc[part, :]
            parts = split3(total)
            if t < TILES - 1:
                for piece, ref in zip(parts, (hi_ref, mid_ref, lo_ref)):
                    ref[pl.ds(at, 16), t * 128:(t + 1) * 128] = piece
            else:
                side = parts[0].astype(F32)
                for i, j in enumerate((1, 2, 0, 1, 0)):
                    side = side + pltpu.roll(parts[j].astype(F32), (i + 1) * HUBS, 1)
                side_ref[pl.ds(at, 16), :] = side.astype(BF16)
        return carry

    lax.fori_loop(0, TABLE // 16, finish, 0)


def build(hub_ids, dst, src, w):
    piece = jax.ShapeDtypeStruct((TABLE, NODES), BF16)
    side = jax.ShapeDtypeStruct((TABLE, 128), BF16)
    square = lambda a: a.reshape(128, 128)
    table = pltpu.VMEM((128, 128), jnp.int32)
    return pl.pallas_call(
        build_kernel,
        out_shape=(piece, piece, piece, side),
        in_specs=[pl.BlockSpec(memory_space=pltpu.HBM)] * 4,
        out_specs=(pl.BlockSpec(memory_space=pltpu.VMEM),) * 4,
        scratch_shapes=[
            pltpu.SMEM((HUBS,), jnp.int32), table, table, pltpu.VMEM((128, 128), F32), table, table,
            pltpu.VMEM((8, 16, 128), jnp.int32), pltpu.VMEM((1024, 128), F32), pltpu.VMEM((1024, 128), F32),
            pltpu.SemaphoreType.DMA((12,)),
        ] + [pltpu.SMEM((16, 128), jnp.int32)] * 8 + [pltpu.VMEM((ROWS, 128), F32)] * ACCS,
        compiler_params=pltpu.CompilerParams(vmem_limit_bytes=BUILD_VMEM),
        name="build",
    )(*(in_hbm(a) for a in (hub_ids, square(dst), square(src), square(w))))


def step_kernel(
    hi_ref, mid_ref, lo_ref, side_ref, xt_hbm, w1_hbm, b1_hbm, w2t_hbm, dht_hbm, send_hbm, hub_hbm,
    dxt_ref, dw1_ref, dw2t_ref, db1_ref, db2_ref,
    xt_ref, w1_ref, b1_ref, w2t_ref, dht_ref, send_ref, hub_ref,
    sent_s, pt_s, xs, xr, hs, hr, z_s, yt_s, d2_s, dhub_s, g2_s, g2h_s, rb, sb, ys, yr, dy_s, dyh_s, g1_s, sd, rd, dz1_s,
    a2, half2, got2, tot2, a1, half1, got1, tot1, load_sem, send_sem, recv_sem,
):
    me = lax.axis_index("graph")
    sibling = me + 1 - 2 * lax.rem(me, 2)
    across = lax.rem(me + 2, 4)
    core = lax.rem(me, 2)
    mesh_id = pl.DeviceIdType.MESH
    peers = [lax.rem(me + d, 4) for d in (1, 2, 3)]
    loads = []
    for i, (a, b) in enumerate((
            (send_hbm, send_ref), (hub_hbm, hub_ref), (xt_hbm, xt_ref), (dht_hbm, dht_ref), (w1_hbm, w1_ref), (b1_hbm, b1_ref),
            (w2t_hbm, w2t_ref))):
        loads.append(pltpu.make_async_copy(a, b, load_sem.at[i]))
        loads[-1].start()
    barrier = pltpu.get_barrier_semaphore()
    for q in peers:
        pl.semaphore_signal(barrier, inc=1, device_id={"graph": q}, device_id_type=mesh_id)
    for load in loads:
        load.wait()
    pl.semaphore_wait(barrier, 3)
    used = [0]

    def remote(src, dst, q):
        i = used[0]
        used[0] += 1
        copy = pltpu.make_async_remote_copy(
            src_ref=src, dst_ref=dst, send_sem=send_sem.at[i], recv_sem=recv_sem.at[i],
            device_id={"graph": q}, device_id_type=mesh_id)
        copy.start()
        return copy

    def wait_all(copies):
        for copy in copies:
            copy.wait()

    pieces = (hi_ref, mid_ref, lo_ref)
    hub_local = hub_ref[...] - me * NODES
    hub_row = jnp.where((hub_local >= 0) & (hub_local < NODES), hub_local, -1).astype(F32)
    hub_block = jnp.concatenate([hub_row, jnp.full((1, SEND - HUBS), -1.0, F32)], axis=1)
    send_row = send_ref[...].astype(F32)
    row = jnp.concatenate([jnp.where(me == q, hub_block, send_row[:, q * SEND:(q + 1) * SEND]) for q in range(4)], axis=1)
    row3 = jnp.concatenate([hub_row] * 3 + [jnp.full((1, 128 - 3 * HUBS), -1.0, F32)], axis=1)
    column = jnp.transpose(jnp.broadcast_to(jnp.concatenate([row, row3], axis=1), (128, 384)))
    lane = lax.broadcasted_iota(jnp.int32, (HALO + 3 * HUBS, 128), 1).astype(F32)
    picks = jnp.concatenate(
        [jnp.where(column[:HALO + 3 * HUBS] == lane + float(j * 128), 1.0, 0.0).astype(BF16) for j in range(8)], axis=1)
    xt = xt_ref[...]
    sent_s[...] = dot_nt(picks[:HALO], xt).astype(BF16).reshape(4, SEND, FIN)
    hub_col = column[HALO:HALO + HUBS]
    alias = [jnp.where((hub_col == row[:, j * 128:(j + 1) * 128]) & (hub_col >= 0.0), 1.0, 0.0) for j in range(2)]
    own_hub_x = sent_s[me, :HUBS, :]
    for q in range(4):
        xs[q, :SEND, :] = sent_s[q]
        xs[q, SEND:SEND + HUBS, :] = own_hub_x
        part = alias[q // 2][:, (q % 2) * SEND:(q % 2 + 1) * SEND]
        xs[q, SEND + HUBS:, :SEND] = part.astype(BF16)
        xs[q, SEND + HUBS:, SEND:] = jnp.zeros((HUBS, FIN - SEND), BF16)
    xr[me] = jnp.zeros((96, FIN), BF16)
    dht = dht_ref[...]
    dh = jnp.transpose(jnp.concatenate([dht, jnp.zeros((128 - OUT, NODES), F32)], axis=0))
    for j, piece in enumerate(split3(dh)):
        d2_s[:, j * 128:(j + 1) * 128] = piece
    round_a = [remote(xs.at[q], xr.at[me], q) for q in peers]
    hub_dh = dot(picks[HALO:HALO + HUBS], d2_s[...])
    hs[...] = (hub_dh[:, :128] + hub_dh[:, 128:256]) + hub_dh[:, 256:]
    hr[me] = hs[...]
    db2 = jnp.sum(dh, axis=0, keepdims=True)
    round_a += [remote(hs, hr.at[me], q) for q in peers]
    sub = lax.broadcasted_iota(jnp.int32, (NODES, HALO), 0).astype(F32)
    pt_s[...] = jnp.where(sub == row, 1.0, 0.0).astype(BF16)

    def grad2(rows):
        a = dot(hi_ref[rows, :], d2_s[:, :256])
        b = dot(mid_ref[rows, :], d2_s[:, :256])
        c = dot(hi_ref[rows, :], d2_s[:, 256:]) + dot(lo_ref[rows, :], d2_s[:, :128])
        return ((c + b[:, 128:]) + (a[:, 128:] + b[:, :128])) + a[:, :128]

    far_rows = pl.ds(NODES, HALO + HUBS)
    g2h_s[...] = grad2(far_rows)

    def grad2_own(m, carry):
        at = pl.ds(pl.multiple_of(m * 256, 256), 256)
        g2_s[at, :] = grad2(at)
        return carry

    lax.fori_loop(0, 4, grad2_own, 0)
    w1t = jnp.transpose(jnp.concatenate([w1_ref[...], jnp.zeros((56, HID), BF16)], axis=0).astype(F32)).astype(BF16)[:, :FIN]
    z_s[:, :NODES] = dot(w1t, xt).astype(BF16)

    def forward_own(at):
        z = z_s[:, :NODES]
        acc = dot(z, hi_ref[:NODES, at])
        acc = acc + dot(z, mid_ref[:NODES, at])
        yt_s[:, at] = acc + dot(z, lo_ref[:NODES, at])

    def over_columns(body):
        def turn(n, carry):
            body(pl.ds(pl.multiple_of(n * 256, 256), 256))
            return carry

        lax.fori_loop(0, 4, turn, 0)

    y_side = dot(z_s[:, :NODES], side_ref[:NODES, :])
    wait_all(round_a)

    halo_x = jnp.concatenate([xr[q, :SEND, :] for q in range(4)], axis=0)
    hub_x = sent_s[me, :HUBS, :].astype(F32)
    for q in range(4):
        hub_x = hub_x + xr[q, SEND:SEND + HUBS, :].astype(F32)
    z_s[:, NODES:] = dot_nt(w1t, halo_x).astype(BF16)
    z_hub = dot_nt(w1t, jnp.concatenate([hub_x.astype(BF16)] * 3, axis=0)).astype(BF16)

    def forward_far(at):
        z = z_s[:, NODES:]
        acc = yt_s[:, at]
        for ref in pieces:
            acc = acc + dot(z, ref[NODES:NODES + HALO, at])
        hub_rows = jnp.concatenate([ref[NODES + HALO:, at] for ref in pieces], axis=0)
        yt_s[:, at] = acc + dot(z_hub, hub_rows)

    y_side = y_side + dot(z_s[:, NODES:], side_ref[NODES:NODES + HALO, :])
    y_side = jnp.transpose(y_side + dot(z_hub[:, :HUBS], side_ref[NODES + HALO:, :]))
    ys[...] = (y_side[:HUBS] + y_side[HUBS:2 * HUBS]) + y_side[2 * HUBS:3 * HUBS]
    yr[me] = ys[...]
    hub_dh = (hr[0] + hr[1]) + (hr[2] + hr[3])
    def side_by_side(x):
        hi, mid, lo = split3(x)
        return jnp.concatenate([hi, hi, hi, mid, mid, lo, jnp.zeros((32, x.shape[1]), BF16)], axis=0)

    dhub_s[...] = side_by_side(hub_dh)
    round_b = [remote(ys, yr.at[me], q) for q in peers]
    g2h_s[...] += dot(side_ref[far_rows, :], dhub_s[...])
    far = g2h_s[:HALO, :]
    alias_row = jnp.concatenate([xr[q, SEND + HUBS:, :SEND] for q in range(4)], axis=1)
    hub_g2 = g2h_s[HALO:, :]
    for piece in split3(far):
        hub_g2 = hub_g2 + dot(alias_row, piece)
    is_alias = dot(jnp.transpose(jnp.concatenate([alias_row.astype(F32), jnp.zeros((112, HALO), F32)], axis=0)).astype(BF16),
                   jnp.ones((128, 128), BF16))
    far = jnp.where(is_alias > 0.5, 0.0, far)
    for q in range(4):
        sb[q, :SEND, :] = far[q * SEND:(q + 1) * SEND]
        sb[q, SEND:, :] = hub_g2
    rb[me] = sb[me]
    round_b += [remote(sb.at[q], rb.at[me], q) for q in peers]

    over_columns(forward_own)
    over_columns(forward_far)

    def grad2_hub(m, carry):
        at = pl.ds(pl.multiple_of(m * 256, 256), 256)
        g2_s[at, :] += dot(side_ref[at, :], dhub_s[...])
        return carry

    lax.fori_loop(0, 4, grad2_hub, 0)
    wait_all(round_b)

    def returned(ref):
        hub_sum = (ref[0, SEND:, :] + ref[1, SEND:, :]) + (ref[2, SEND:, :] + ref[3, SEND:, :])
        ref[me, :HUBS, :] = hub_sum
        ref[me, HUBS:SEND, :] = jnp.zeros((SEND - HUBS, hub_sum.shape[1]), F32)
        return ref[:, :SEND, :].reshape(HALO, hub_sum.shape[1]), hub_sum

    back, hub_sum = returned(rb)
    hub_dz2 = hub_sum.astype(BF16)
    own = g2_s[...]
    for piece in split3(back):
        own = own + dot(pt_s[...], piece)
    dz2 = own.astype(BF16)

    y_hub = (yr[0] + yr[1]) + (yr[2] + yr[3])
    b1 = b1_ref[...]
    b1_col = jnp.transpose(jnp.broadcast_to(b1, (128, HID)))
    y_rows = jnp.concatenate([piece.astype(F32) for piece in split3(y_hub)] + [jnp.zeros((128 - 3 * HUBS, HID), F32)], axis=0)
    y_own = dot(jnp.transpose(y_rows).astype(BF16)[:, :3 * HUBS], picks[HALO:])
    pre = (yt_s[...] + y_own) + jnp.concatenate([b1_col] * 8, axis=1)
    yt_s[...] = pre
    live = jnp.transpose(jnp.where(pre > 0.0, 1.0, 0.0))
    w2t = w2t_ref[...]
    dy = jnp.where(live > 0.5, dot(dz2[:, :OUT], w2t), 0.0)
    hub_dy = jnp.where(y_hub + b1 > 0.0, dot(hub_dz2[:, :OUT], w2t), 0.0)
    db1 = jnp.sum(dy, axis=0, keepdims=True)
    for j, piece in enumerate(split3(dy)):
        dy_s[j] = piece
    dyh_s[...] = side_by_side(hub_dy)

    class GroupSum:
        def __init__(self, own, half, got, total):
            self.own, self.half, self.got, self.total = own, half, got, total
            self.copy = remote(own.at[1 - core], got.at[0], sibling)

        def across(self):
            self.copy.wait()
            self.half[...] = self.own[core] + self.got[0]
            self.copy = remote(self.half, self.got.at[1], across)

        def back(self):
            self.copy.wait()
            self.total[core] = self.half[...] + self.got[1]
            self.copy = remote(self.total.at[core], self.total.at[core], sibling)

        def done(self):
            self.copy.wait()

    def grad1(rows, cols):
        acc = dot(lo_ref[rows, :], dy_s[0, :, cols])
        acc = acc + dot(mid_ref[rows, :], dy_s[1, :, cols])
        acc = acc + dot(hi_ref[rows, :], dy_s[2, :, cols])
        acc = acc + dot(mid_ref[rows, :], dy_s[0, :, cols])
        acc = acc + dot(hi_ref[rows, :], dy_s[1, :, cols])
        acc = acc + dot(hi_ref[rows, :], dy_s[0, :, cols])
        return acc + dot(side_ref[rows, :], dyh_s[:, cols])

    halves = (pl.ds(0, 256), pl.ds(256, 256))
    round_d = []
    for h, cols in enumerate(halves):
        ret = grad1(far_rows, cols)
        for q in range(4):
            sd[h, q, :SEND, :] = ret[q * SEND:(q + 1) * SEND]
            sd[h, q, SEND:, :] = ret[HALO:]
        rd[h, me] = sd[h, me]
        round_d.append([remote(sd.at[h, q], rd.at[h, me], q) for q in peers])

    dw2t = jnp.transpose(dot(jnp.maximum(yt_s[...], 0.0).astype(BF16), dz2))
    for h in range(2):
        a2[h, :112, :] = dw2t[:112, h * 256:(h + 1) * 256]
        a2[h, 112:, :128] = jnp.broadcast_to(db2, (8, 128))
        a2[h, 112:, 128:] = jnp.zeros((8, 128), F32)

    def grad1_own(h, m):
        rows = pl.ds(m * 512, 512)
        g1_s[rows, halves[h]] = grad1(rows, halves[h])

    def finish(h):
        wait_all(round_d[h])
        cols = halves[h]
        back, _ = returned(rd.at[h])
        dz1 = g1_s[:, cols]
        for piece in split3(back):
            dz1 = dz1 + dot(pt_s[...], piece)
        dz1 = dz1.astype(BF16)
        dz1_s[:, cols] = dz1
        dw1 = dot(xt_ref[...], dz1)
        for i in range(2):
            at = slice(i * 128, (i + 1) * 128)
            a1[h, i, :FIN, :] = dw1[:, at]
            a1[h, i, FIN:, :] = jnp.broadcast_to(db1[:, h * 256 + i * 128:h * 256 + (i + 1) * 128], (8, 128))
        return GroupSum(a1.at[h], half1.at[h], got1.at[h], tot1.at[h])

    sum2 = GroupSum(a2, half2, got2, tot2)
    grad1_own(0, 0)
    sum2.across()
    grad1_own(0, 1)
    sum1 = [finish(0)]
    grad1_own(1, 0)
    sum1[0].across()
    sum2.back()
    grad1_own(1, 1)
    sum1.append(finish(1))
    sum1[0].back()
    sum2.done()
    for h in range(2):
        dw2t_ref[:, h * 256:(h + 1) * 256] = tot2[h, :OUT, :]
    db2_ref[...] = tot2[0, 112:113, :OUT]
    sum1[1].across()
    dxt_ref[...] = dot_nt(w1_ref[...], dz1_s[...])
    sum1[1].back()
    sum1[0].done()

    def put(h):
        for i in range(2):
            at = slice(h * 256 + i * 128, h * 256 + (i + 1) * 128)
            dw1_ref[:, at] = tot1[h, i, :FIN, :]
            db1_ref[:, at] = tot1[h, i, FIN:FIN + 1, :]

    put(0)
    sum1[1].done()
    put(1)


def step(hi, mid, lo, side, xt, w1, b1, w2t, dht, send, hubs):
    vmem = pl.BlockSpec(memory_space=pltpu.VMEM)
    out = lambda *shape: jax.ShapeDtypeStruct(shape, F32)
    f32 = lambda *shape: pltpu.VMEM(shape, F32)
    b16 = lambda *shape: pltpu.VMEM(shape, BF16)
    return pl.pallas_call(
        step_kernel,
        out_shape=(out(FIN, NODES), out(FIN, HID), out(OUT, HID), out(1, HID), out(1, OUT)),
        in_specs=[vmem] * 4 + [pl.BlockSpec(memory_space=pltpu.HBM)] * 7,
        out_specs=(vmem,) * 5,
        scratch_shapes=[
            b16(FIN, NODES), b16(FIN, HID), f32(1, HID), b16(OUT, HID), f32(OUT, NODES),
            pltpu.VMEM((1, HALO), jnp.int32), pltpu.VMEM((1, HUBS), jnp.int32),
            b16(4, SEND, FIN), b16(NODES, HALO), b16(4, 96, FIN), b16(4, 96, FIN), f32(HUBS, 128), f32(4, HUBS, 128),
            b16(HID, NODES + HALO), f32(HID, NODES), b16(NODES, 384), b16(128, 128), f32(NODES, 128), f32(HALO + HUBS, 128),
            f32(4, SEND + HUBS, 128), f32(4, SEND + HUBS, 128), f32(HUBS, HID), f32(4, HUBS, HID),
            b16(3, NODES, HID), b16(128, HID), f32(NODES, HID), f32(2, 4, SEND + HUBS, 256), f32(2, 4, SEND + HUBS, 256), b16(NODES, HID),
            f32(2, 120, 256), f32(120, 256), f32(2, 120, 256), f32(2, 120, 256),
            f32(2, 2, 208, 128), f32(2, 208, 128), f32(2, 2, 208, 128), f32(2, 2, 208, 128),
            pltpu.SemaphoreType.DMA((7,)), pltpu.SemaphoreType.DMA((28,)), pltpu.SemaphoreType.DMA((28,)),
        ],
        compiler_params=pltpu.CompilerParams(collective_id=0, has_side_effects=True, vmem_limit_bytes=STEP_VMEM),
        name="step",
    )(hi, mid, lo, side, *(in_hbm(a) for a in (xt, w1, b1, w2t, dht, send, hubs)))


def emit_kernel(*refs):
    ins, outs, sem = refs[:5], refs[5:10], refs[10]
    copies = [pltpu.make_async_copy(a, b, sem.at[i]) for i, (a, b) in enumerate(zip(ins, outs))]
    for copy in copies:
        copy.start()
    for copy in copies:
        copy.wait()


def emit(*arrays):
    return pl.pallas_call(
        emit_kernel,
        out_shape=tuple(jax.ShapeDtypeStruct(a.shape, a.dtype) for a in arrays),
        in_specs=[pl.BlockSpec(memory_space=pltpu.VMEM)] * 5,
        out_specs=(pl.BlockSpec(memory_space=pltpu.HBM),) * 5,
        scratch_shapes=[pltpu.SemaphoreType.DMA((5,))],
        compiler_params=pltpu.CompilerParams(vmem_limit_bytes=4 << 20),
        name="emit",
    )(*arrays)


def solution(mesh):
    vertex_spec = P(("data", "graph"))
    vertex_rows = P(("data", "graph"), None)
    part_spec = P("data")
    part_rows = P("data", None)
    replicated = P()

    def device_step(x, dst, src, w, send, hub_ids, w_first, b_first, w_second, dy_out):
        table = build(hub_ids, dst, src, w)
        dx, dw1, dw2, db1, db2 = emit(*step(
            *table, x.T, w_first, b_first.reshape(1, HID), w_second.T, dy_out.T, send.reshape(1, HALO), hub_ids.reshape(1, HUBS)))
        return dx.T, dw1, dw2.T, db1.reshape(HID), db2.reshape(OUT)

    return jax.shard_map(
        device_step,
        mesh=mesh,
        in_specs=(vertex_rows, vertex_spec, vertex_spec, vertex_spec, vertex_spec, part_spec, replicated, replicated, replicated, vertex_rows),
        out_specs=(vertex_rows, part_rows, part_rows, part_spec, part_spec),
        check_vma=False,
    )
```

```python
import functools

import jax
import jax.numpy as jnp
from jax import lax
from jax.experimental import pallas as pl
from jax.experimental.pallas import tpu as pltpu
from jax.sharding import PartitionSpec as P

F32, BF16 = jnp.float32, jnp.bfloat16
NODES, SEND, HALO, HUBS = 1024, 64, 256, 16
TABLE = NODES + HALO + HUBS
TILES = 9
COLS = TILES * 128
ROWS = TILES * TABLE
EDGES = 16384
HID, OUT, FIN = 512, 107, 200

ACCS = 4
GROUP = 4
BUILD_VMEM = 28 << 20
STEP_VMEM = 34 << 20
NT = (((1,), (1,)), ((), ()))


def split3(x):
    hi = x.astype(BF16)
    rest = x - hi.astype(F32)
    mid = rest.astype(BF16)
    return hi, mid, (rest - mid.astype(F32)).astype(BF16)


def in_hbm(a):
    return pltpu.with_memory_space_constraint(a, pltpu.HBM)


def dot(a, b):
    return jnp.dot(a, b, preferred_element_type=F32)


def dot_nt(a, b):
    return lax.dot_general(a, b, NT, preferred_element_type=F32)


def build_kernel(hub_hbm, dst_hbm, src_hbm, w_hbm, hi_ref, mid_ref, lo_ref, side_ref, hub_ref, dst_ref, src_ref, w_ref, row_ref, lane_ref, perm_ref, val_a, val_b, sem, *rest):
    row_smem, accs = rest[:8], rest[8:]
    loads = []
    for i, (a, b) in enumerate(((hub_hbm, hub_ref), (dst_hbm, dst_ref), (src_hbm, src_ref), (w_hbm, w_ref))):
        loads.append(pltpu.make_async_copy(a, b, sem.at[8 + i]))
        loads[-1].start()

    def zero(i, carry):
        for acc in accs:
            acc[pl.ds(pl.multiple_of(i * 48, 8), 48), :] = jnp.zeros((48, 128), F32)
        return carry

    lax.fori_loop(0, ROWS // 48, zero, 0)
    for load in loads:
        load.wait()
    base = lax.axis_index("graph") * NODES
    dst, src = dst_ref[...], src_ref[...]
    new_dst, new_src = dst, src
    for k in range(HUBS):
        local = hub_ref[k] - base
        local = jnp.where((local >= 0) & (local < NODES), local, -1)
        new_dst = jnp.where(dst == local, NODES + k, new_dst)
        new_src = jnp.where(src == local, NODES + HALO + k, new_src)
    row_ref[...] = (new_dst >> 7) * TABLE + new_src
    lane_ref[...] = new_dst & 127
    copies = []
    for s in range(8):
        perm_ref[s] = row_ref[pl.ds(s, 16, stride=8), :]
    for s in range(8):
        copies.append(pltpu.make_async_copy(perm_ref.at[s], row_smem[s], sem.at[s]))
        copies[-1].start()

    iota = lax.broadcasted_iota(jnp.int32, (8, 128), 1)

    def wide(block, c):
        return jnp.broadcast_to(block[:, c:c + 1], (8, 128))

    def prep(g, val_ref):
        at = pl.ds(pl.multiple_of(g * 8, 8), 8)
        lanes, weights, rows = lane_ref[at, :], w_ref[at, :], row_ref[at, :]
        place = lax.broadcasted_iota(jnp.int32, (8, 128), 1) % GROUP
        terms = [(lanes, weights)]
        for d in range(1, GROUP):
            same = (place >= d) & (rows == pltpu.roll(rows, d, 1))
            terms.append((pltpu.roll(lanes, d, 1), jnp.where(same, pltpu.roll(weights, d, 1), 0.0)))
        def one(s):
            total = None
            for lane, weight in terms:
                hit = jnp.broadcast_to(lane[s:s + 1, :], (128, 128)) == sub
                part = jnp.where(hit, jnp.broadcast_to(weight[s:s + 1, :], (128, 128)), 0.0)
                total = part if total is None else total + part
            val_ref[s * 128:(s + 1) * 128, :] = jnp.transpose(total)

        return one

    def scatter(g, val_ref, c):
        for s in range(8):
            acc = accs[s % ACCS]
            rows = [row_smem[s][g, c + i] for i in range(GROUP)]
            sums = [acc[pl.ds(rows[i], 1), :] + val_ref[s * 128 + c + i:s * 128 + c + i + 1, :] for i in range(GROUP)]
            for r, total in zip(rows, sums):
                acc[pl.ds(r, 1), :] = total

    def both(g, val_ref, next_g, next_ref):
        one = prep(next_g, next_ref)
        for c in range(0, 128, GROUP):
            if c % 16 == 0:
                one(c // 16)
            scatter(g, val_ref, c)

    sub = lax.broadcasted_iota(jnp.int32, (128, 128), 0)
    first = prep(0, val_a)
    for s in range(8):
        first(s)
    for copy in copies:
        copy.wait()

    def turn(h, carry):
        both(2 * h, val_a, 2 * h + 1, val_b)
        both(2 * h + 1, val_b, jnp.minimum(2 * h + 2, 15), val_a)
        return carry

    lax.fori_loop(0, 8, turn, 0)

    def finish(i, carry):
        at = pl.multiple_of(i * 16, 16)
        for t in range(TILES):
            part = pl.ds(pl.multiple_of(t * TABLE + i * 16, 8), 16)
            total = accs[0][part, :]
            for acc in accs[1:]:
                total = total + acc[part, :]
            parts = split3(total)
            if t < TILES - 1:
                for piece, ref in zip(parts, (hi_ref, mid_ref, lo_ref)):
                    ref[pl.ds(at, 16), t * 128:(t + 1) * 128] = piece
            else:
                side = parts[0].astype(F32)
                for i, j in enumerate((1, 2, 0, 1, 0)):
                    side = side + pltpu.roll(parts[j].astype(F32), (i + 1) * HUBS, 1)
                side_ref[pl.ds(at, 16), :] = side.astype(BF16)
        return carry

    lax.fori_loop(0, TABLE // 16, finish, 0)


def build(hub_ids, dst, src, w):
    piece = jax.ShapeDtypeStruct((TABLE, NODES), BF16)
    side = jax.ShapeDtypeStruct((TABLE, 128), BF16)
    square = lambda a: a.reshape(128, 128)
    table = pltpu.VMEM((128, 128), jnp.int32)
    return pl.pallas_call(
        build_kernel,
        out_shape=(piece, piece, piece, side),
        in_specs=[pl.BlockSpec(memory_space=pltpu.HBM)] * 4,
        out_specs=(pl.BlockSpec(memory_space=pltpu.VMEM),) * 4,
        scratch_shapes=[
            pltpu.SMEM((HUBS,), jnp.int32), table, table, pltpu.VMEM((128, 128), F32), table, table,
            pltpu.VMEM((8, 16, 128), jnp.int32), pltpu.VMEM((1024, 128), F32), pltpu.VMEM((1024, 128), F32),
            pltpu.SemaphoreType.DMA((12,)),
        ] + [pltpu.SMEM((16, 128), jnp.int32)] * 8 + [pltpu.VMEM((ROWS, 128), F32)] * ACCS,
        compiler_params=pltpu.CompilerParams(vmem_limit_bytes=BUILD_VMEM),
        name="build",
    )(*(in_hbm(a) for a in (hub_ids, square(dst), square(src), square(w))))


def step_kernel(
    hi_ref, mid_ref, lo_ref, side_ref, xt_hbm, w1_hbm, b1_hbm, w2t_hbm, dht_hbm, send_hbm, hub_hbm,
    dxt_ref, dw1_ref, dw2t_ref, db1_ref, db2_ref,
    xt_ref, w1_ref, b1_ref, w2t_ref, dht_ref, send_ref, hub_ref,
    sent_s, pt_s, xs, xr, hs, hr, z_s, yt_s, d2_s, dhub_s, g2_s, g2h_s, rb, sb, ys, yr, dy_s, dyh_s, g1_s, sd, rd, dz1_s,
    hub3_s, y_cols_s, hid_s, live_s, dz2_s,
    a2, half2, got2, tot2, a1, half1, got1, tot1, load_sem, send_sem, recv_sem,
):
    me = lax.axis_index("graph")
    sibling = me + 1 - 2 * lax.rem(me, 2)
    across = lax.rem(me + 2, 4)
    core = lax.rem(me, 2)
    mesh_id = pl.DeviceIdType.MESH
    peers = [lax.rem(me + d, 4) for d in (1, 2, 3)]
    loads = []
    for i, (a, b) in enumerate((
            (send_hbm, send_ref), (hub_hbm, hub_ref), (xt_hbm, xt_ref), (dht_hbm, dht_ref), (w1_hbm, w1_ref), (b1_hbm, b1_ref),
            (w2t_hbm, w2t_ref))):
        loads.append(pltpu.make_async_copy(a, b, load_sem.at[i]))
        loads[-1].start()
    barrier = pltpu.get_barrier_semaphore()
    for q in peers:
        pl.semaphore_signal(barrier, inc=1, device_id={"graph": q}, device_id_type=mesh_id)
    for load in loads:
        load.wait()
    pl.semaphore_wait(barrier, 3)
    used = [0]

    def remote(src, dst, q):
        i = used[0]
        used[0] += 1
        copy = pltpu.make_async_remote_copy(
            src_ref=src, dst_ref=dst, send_sem=send_sem.at[i], recv_sem=recv_sem.at[i],
            device_id={"graph": q}, device_id_type=mesh_id)
        copy.start()
        return copy

    def wait_all(copies):
        for copy in copies:
            copy.wait()

    pieces = (hi_ref, mid_ref, lo_ref)
    hub_local = hub_ref[...] - me * NODES
    hub_row = jnp.where((hub_local >= 0) & (hub_local < NODES), hub_local, -1).astype(F32)
    hub_block = jnp.concatenate([hub_row, jnp.full((1, SEND - HUBS), -1.0, F32)], axis=1)
    send_row = send_ref[...].astype(F32)
    row = jnp.concatenate([jnp.where(me == q, hub_block, send_row[:, q * SEND:(q + 1) * SEND]) for q in range(4)], axis=1)
    row3 = jnp.concatenate([hub_row] * 3 + [jnp.full((1, 128 - 3 * HUBS), -1.0, F32)], axis=1)
    column = jnp.transpose(jnp.broadcast_to(jnp.concatenate([row, row3], axis=1), (128, 384)))
    lane = lax.broadcasted_iota(jnp.int32, (HALO + 3 * HUBS, 128), 1).astype(F32)
    picks = jnp.concatenate(
        [jnp.where(column[:HALO + 3 * HUBS] == lane + float(j * 128), 1.0, 0.0).astype(BF16) for j in range(8)], axis=1)
    xt = xt_ref[...]
    sent_s[...] = dot_nt(picks[:HALO], xt).astype(BF16).reshape(4, SEND, FIN)
    hub_col = column[HALO:HALO + HUBS]
    alias = [jnp.where((hub_col == row[:, j * 128:(j + 1) * 128]) & (hub_col >= 0.0), 1.0, 0.0) for j in range(2)]
    own_hub_x = sent_s[me, :HUBS, :]
    for q in range(4):
        xs[q, :SEND, :] = sent_s[q]
        xs[q, SEND:SEND + HUBS, :] = own_hub_x
        part = alias[q // 2][:, (q % 2) * SEND:(q % 2 + 1) * SEND]
        xs[q, SEND + HUBS:, :SEND] = part.astype(BF16)
        xs[q, SEND + HUBS:, SEND:] = jnp.zeros((HUBS, FIN - SEND), BF16)
    xr[me] = jnp.zeros((96, FIN), BF16)
    dht = dht_ref[...]
    dh = jnp.transpose(jnp.concatenate([dht, jnp.zeros((128 - OUT, NODES), F32)], axis=0))
    for j, piece in enumerate(split3(dh)):
        d2_s[:, j * 128:(j + 1) * 128] = piece
    round_a = [remote(xs.at[q], xr.at[me], q) for q in peers]
    hub_dh = dot(picks[HALO:HALO + HUBS], d2_s[...])
    hs[...] = (hub_dh[:, :128] + hub_dh[:, 128:256]) + hub_dh[:, 256:]
    hr[me] = hs[...]
    db2 = jnp.sum(dh, axis=0, keepdims=True)
    round_a += [remote(hs, hr.at[me], q) for q in peers]
    sub = lax.broadcasted_iota(jnp.int32, (NODES, HALO), 0).astype(F32)
    pt_s[...] = jnp.where(sub == row, 1.0, 0.0).astype(BF16)
    hub3_s[...] = picks[HALO:]

    def grad2(rows):
        a = dot(hi_ref[rows, :], d2_s[:, :256])
        b = dot(mid_ref[rows, :], d2_s[:, :256])
        c = dot(hi_ref[rows, :], d2_s[:, 256:]) + dot(lo_ref[rows, :], d2_s[:, :128])
        return ((c + b[:, 128:]) + (a[:, 128:] + b[:, :128])) + a[:, :128]

    far_rows = pl.ds(NODES, HALO + HUBS)
    g2h_s[...] = grad2(far_rows)

    def grad2_own(m, carry):
        at = pl.ds(pl.multiple_of(m * 256, 256), 256)
        g2_s[at, :] = grad2(at)
        return carry

    lax.fori_loop(0, 4, grad2_own, 0)
    w1t = jnp.transpose(jnp.concatenate([w1_ref[...], jnp.zeros((56, HID), BF16)], axis=0).astype(F32)).astype(BF16)[:, :FIN]
    z_s[:, :NODES] = dot(w1t, xt).astype(BF16)

    def forward_own(at):
        z = z_s[:, :NODES]
        acc = dot(z, hi_ref[:NODES, at])
        acc = acc + dot(z, mid_ref[:NODES, at])
        yt_s[:, at] = acc + dot(z, lo_ref[:NODES, at])

    def over_columns(body):
        def turn(n, carry):
            body(pl.ds(pl.multiple_of(n * 256, 256), 256))
            return carry

        lax.fori_loop(0, 4, turn, 0)

    y_side = dot(z_s[:, :NODES], side_ref[:NODES, :])
    wait_all(round_a)

    halo_x = jnp.concatenate([xr[q, :SEND, :] for q in range(4)], axis=0)
    hub_x = sent_s[me, :HUBS, :].astype(F32)
    for q in range(4):
        hub_x = hub_x + xr[q, SEND:SEND + HUBS, :].astype(F32)
    z_s[:, NODES:] = dot_nt(w1t, halo_x).astype(BF16)
    z_hub = dot_nt(w1t, jnp.concatenate([hub_x.astype(BF16)] * 3, axis=0)).astype(BF16)

    def forward_far(at):
        z = z_s[:, NODES:]
        acc = yt_s[:, at]
        for ref in pieces:
            acc = acc + dot(z, ref[NODES:NODES + HALO, at])
        hub_rows = jnp.concatenate([ref[NODES + HALO:, at] for ref in pieces], axis=0)
        yt_s[:, at] = acc + dot(z_hub, hub_rows)

    y_side = y_side + dot(z_s[:, NODES:], side_ref[NODES:NODES + HALO, :])
    y_side = jnp.transpose(y_side + dot(z_hub[:, :HUBS], side_ref[NODES + HALO:, :]))
    ys[...] = (y_side[:HUBS] + y_side[HUBS:2 * HUBS]) + y_side[2 * HUBS:3 * HUBS]
    yr[me] = ys[...]
    hub_dh = (hr[0] + hr[1]) + (hr[2] + hr[3])
    def side_by_side(x):
        hi, mid, lo = split3(x)
        return jnp.concatenate([hi, hi, hi, mid, mid, lo, jnp.zeros((32, x.shape[1]), BF16)], axis=0)

    dhub_s[...] = side_by_side(hub_dh)
    round_b = [remote(ys, yr.at[me], q) for q in peers]
    g2h_s[...] += dot(side_ref[far_rows, :], dhub_s[...])
    far = g2h_s[:HALO, :]
    alias_row = jnp.concatenate([xr[q, SEND + HUBS:, :SEND] for q in range(4)], axis=1)
    hub_g2 = g2h_s[HALO:, :]
    for piece in split3(far):
        hub_g2 = hub_g2 + dot(alias_row, piece)
    is_alias = dot(jnp.transpose(jnp.concatenate([alias_row.astype(F32), jnp.zeros((112, HALO), F32)], axis=0)).astype(BF16),
                   jnp.ones((128, 128), BF16))
    far = jnp.where(is_alias > 0.5, 0.0, far)
    for q in range(4):
        sb[q, :SEND, :] = far[q * SEND:(q + 1) * SEND]
        sb[q, SEND:, :] = hub_g2
    rb[me] = sb[me]
    round_b += [remote(sb.at[q], rb.at[me], q) for q in peers]

    over_columns(forward_own)
    over_columns(forward_far)

    def grad2_hub(m, carry):
        at = pl.ds(pl.multiple_of(m * 256, 256), 256)
        g2_s[at, :] += dot(side_ref[at, :], dhub_s[...])
        return carry

    lax.fori_loop(0, 4, grad2_hub, 0)
    wait_all(round_b)

    def returned(ref):
        hub_sum = (ref[0, SEND:, :] + ref[1, SEND:, :]) + (ref[2, SEND:, :] + ref[3, SEND:, :])
        ref[me, :HUBS, :] = hub_sum
        ref[me, HUBS:SEND, :] = jnp.zeros((SEND - HUBS, hub_sum.shape[1]), F32)
        return ref[:, :SEND, :].reshape(HALO, hub_sum.shape[1]), hub_sum

    back, hub_sum = returned(rb)
    hub_dz2 = hub_sum.astype(BF16)
    back_parts = split3(back)

    def over_blocks(body, carry=0):
        def turn(n, carry):
            return body(pl.ds(pl.multiple_of(n * 256, 256), 256), carry)

        return lax.fori_loop(0, 4, turn, carry)

    def dz2_block(at, carry):
        own = g2_s[at, :]
        for piece in back_parts:
            own = own + dot(pt_s[at, :], piece)
        dz2_s[at, :] = own.astype(BF16)
        return carry

    over_blocks(dz2_block)

    y_hub = (yr[0] + yr[1]) + (yr[2] + yr[3])
    b1 = b1_ref[...]
    b1_col = jnp.transpose(jnp.broadcast_to(b1, (128, HID)))
    y_rows = jnp.concatenate([piece.astype(F32) for piece in split3(y_hub)] + [jnp.zeros((128 - 3 * HUBS, HID), F32)], axis=0)
    y_cols_s[...] = jnp.transpose(y_rows).astype(BF16)[:, :3 * HUBS]

    def pre_block(at, carry):
        pre = (yt_s[:, at] + dot(y_cols_s[...], hub3_s[:, at])) + jnp.concatenate([b1_col] * 2, axis=1)
        hid_s[:, at] = jnp.maximum(pre, 0.0).astype(BF16)
        live_s[:, at] = jnp.where(pre > 0.0, 1.0, 0.0)
        return carry

    over_blocks(pre_block)

    class GroupSum:
        def __init__(self, own, half, got, total):
            self.own, self.half, self.got, self.total = own, half, got, total
            self.copy = remote(own.at[1 - core], got.at[0], sibling)

        def across(self):
            self.copy.wait()
            self.half[...] = self.own[core] + self.got[0]
            self.copy = remote(self.half, self.got.at[1], across)

        def back(self):
            self.copy.wait()
            self.total[core] = self.half[...] + self.got[1]
            self.copy = remote(self.total.at[core], self.total.at[core], sibling)

        def done(self):
            self.copy.wait()

    dw2t = jnp.transpose(dot(hid_s[...], dz2_s[...]))
    for h in range(2):
        a2[h, :112, :] = dw2t[:112, h * 256:(h + 1) * 256]
        a2[h, 112:, :128] = jnp.broadcast_to(db2, (8, 128))
        a2[h, 112:, 128:] = jnp.zeros((8, 128), F32)
    sum2 = GroupSum(a2, half2, got2, tot2)

    def dy_block(at, db1):
        live = jnp.transpose(live_s[:, at])
        dy = jnp.where(live > 0.5, dot(dz2_s[at, :OUT], w2t_ref[...]), 0.0)
        for j, piece in enumerate(split3(dy)):
            dy_s[j, at, :] = piece
        return db1 + jnp.sum(dy, axis=0, keepdims=True)

    db1 = over_blocks(dy_block, jnp.zeros((1, HID), F32))
    hub_dy = jnp.where(y_hub + b1 > 0.0, dot(hub_dz2[:, :OUT], w2t_ref[...]), 0.0)
    dyh_s[...] = side_by_side(hub_dy)
    sum2.across()

    def grad1(rows, cols):
        acc = dot(lo_ref[rows, :], dy_s[0, :, cols])
        acc = acc + dot(mid_ref[rows, :], dy_s[1, :, cols])
        acc = acc + dot(hi_ref[rows, :], dy_s[2, :, cols])
        acc = acc + dot(mid_ref[rows, :], dy_s[0, :, cols])
        acc = acc + dot(hi_ref[rows, :], dy_s[1, :, cols])
        acc = acc + dot(hi_ref[rows, :], dy_s[0, :, cols])
        return acc + dot(side_ref[rows, :], dyh_s[:, cols])

    halves = (pl.ds(0, 256), pl.ds(256, 256))
    round_d = []
    for h, cols in enumerate(halves):
        ret = grad1(far_rows, cols)
        for q in range(4):
            sd[h, q, :SEND, :] = ret[q * SEND:(q + 1) * SEND]
            sd[h, q, SEND:, :] = ret[HALO:]
        rd[h, me] = sd[h, me]
        round_d.append([remote(sd.at[h, q], rd.at[h, me], q) for q in peers])

    def grad1_own(h, m):
        rows = pl.ds(m * 512, 512)
        g1_s[rows, halves[h]] = grad1(rows, halves[h])

    def finish(h):
        wait_all(round_d[h])
        cols = halves[h]
        back, _ = returned(rd.at[h])
        dz1 = g1_s[:, cols]
        for piece in split3(back):
            dz1 = dz1 + dot(pt_s[...], piece)
        dz1 = dz1.astype(BF16)
        dz1_s[:, cols] = dz1
        dw1 = dot(xt_ref[...], dz1)
        for i in range(2):
            at = slice(i * 128, (i + 1) * 128)
            a1[h, i, :FIN, :] = dw1[:, at]
            a1[h, i, FIN:, :] = jnp.broadcast_to(db1[:, h * 256 + i * 128:h * 256 + (i + 1) * 128], (8, 128))
        return GroupSum(a1.at[h], half1.at[h], got1.at[h], tot1.at[h])

    grad1_own(0, 0)
    grad1_own(0, 1)
    sum1 = [finish(0)]
    sum2.back()
    grad1_own(1, 0)
    sum1[0].across()
    grad1_own(1, 1)
    sum1.append(finish(1))
    sum2.done()
    for h in range(2):
        dw2t_ref[:, h * 256:(h + 1) * 256] = tot2[h, :OUT, :]
    db2_ref[...] = tot2[0, 112:113, :OUT]
    sum1[1].across()
    dxt_ref[...] = dot_nt(w1_ref[...], dz1_s[...])
    sum1[0].back()
    sum1[0].done()

    def put(h):
        for i in range(2):
            at = slice(h * 256 + i * 128, h * 256 + (i + 1) * 128)
            dw1_ref[:, at] = tot1[h, i, :FIN, :]
            db1_ref[:, at] = tot1[h, i, FIN:FIN + 1, :]

    put(0)
    sum1[1].back()
    sum1[1].done()
    put(1)


def step(hi, mid, lo, side, xt, w1, b1, w2t, dht, send, hubs):
    vmem = pl.BlockSpec(memory_space=pltpu.VMEM)
    out = lambda *shape: jax.ShapeDtypeStruct(shape, F32)
    f32 = lambda *shape: pltpu.VMEM(shape, F32)
    b16 = lambda *shape: pltpu.VMEM(shape, BF16)
    return pl.pallas_call(
        step_kernel,
        out_shape=(out(FIN, NODES), out(FIN, HID), out(OUT, HID), out(1, HID), out(1, OUT)),
        in_specs=[vmem] * 4 + [pl.BlockSpec(memory_space=pltpu.HBM)] * 7,
        out_specs=(vmem,) * 5,
        scratch_shapes=[
            b16(FIN, NODES), b16(FIN, HID), f32(1, HID), b16(OUT, HID), f32(OUT, NODES),
            pltpu.VMEM((1, HALO), jnp.int32), pltpu.VMEM((1, HUBS), jnp.int32),
            b16(4, SEND, FIN), b16(NODES, HALO), b16(4, 96, FIN), b16(4, 96, FIN), f32(HUBS, 128), f32(4, HUBS, 128),
            b16(HID, NODES + HALO), f32(HID, NODES), b16(NODES, 384), b16(128, 128), f32(NODES, 128), f32(HALO + HUBS, 128),
            f32(4, SEND + HUBS, 128), f32(4, SEND + HUBS, 128), f32(HUBS, HID), f32(4, HUBS, HID),
            b16(3, NODES, HID), b16(128, HID), f32(NODES, HID), f32(2, 4, SEND + HUBS, 256), f32(2, 4, SEND + HUBS, 256), b16(NODES, HID),
            b16(3 * HUBS, NODES), b16(HID, 3 * HUBS), b16(HID, NODES), f32(HID, NODES), b16(NODES, 128),
            f32(2, 120, 256), f32(120, 256), f32(2, 120, 256), f32(2, 120, 256),
            f32(2, 2, 208, 128), f32(2, 208, 128), f32(2, 2, 208, 128), f32(2, 2, 208, 128),
            pltpu.SemaphoreType.DMA((7,)), pltpu.SemaphoreType.DMA((28,)), pltpu.SemaphoreType.DMA((28,)),
        ],
        compiler_params=pltpu.CompilerParams(collective_id=0, has_side_effects=True, vmem_limit_bytes=STEP_VMEM),
        name="step",
    )(hi, mid, lo, side, *(in_hbm(a) for a in (xt, w1, b1, w2t, dht, send, hubs)))


def emit_kernel(*refs):
    ins, outs, sem = refs[:5], refs[5:10], refs[10]
    copies = [pltpu.make_async_copy(a, b, sem.at[i]) for i, (a, b) in enumerate(zip(ins, outs))]
    for copy in copies:
        copy.start()
    for copy in copies:
        copy.wait()


def emit(*arrays):
    return pl.pallas_call(
        emit_kernel,
        out_shape=tuple(jax.ShapeDtypeStruct(a.shape, a.dtype) for a in arrays),
        in_specs=[pl.BlockSpec(memory_space=pltpu.VMEM)] * 5,
        out_specs=(pl.BlockSpec(memory_space=pltpu.HBM),) * 5,
        scratch_shapes=[pltpu.SemaphoreType.DMA((5,))],
        compiler_params=pltpu.CompilerParams(vmem_limit_bytes=4 << 20),
        name="emit",
    )(*arrays)


def solution(mesh):
    vertex_spec = P(("data", "graph"))
    vertex_rows = P(("data", "graph"), None)
    part_spec = P("data")
    part_rows = P("data", None)
    replicated = P()

    def device_step(x, dst, src, w, send, hub_ids, w_first, b_first, w_second, dy_out):
        table = build(hub_ids, dst, src, w)
        dx, dw1, dw2, db1, db2 = emit(*step(
            *table, x.T, w_first, b_first.reshape(1, HID), w_second.T, dy_out.T, send.reshape(1, HALO), hub_ids.reshape(1, HUBS)))
        return dx.T, dw1, dw2.T, db1.reshape(HID), db2.reshape(OUT)

    return jax.shard_map(
        device_step,
        mesh=mesh,
        in_specs=(vertex_rows, vertex_spec, vertex_spec, vertex_spec, vertex_spec, part_spec, replicated, replicated, replicated, vertex_rows),
        out_specs=(vertex_rows, part_rows, part_rows, part_spec, part_spec),
        check_vma=False,
    )
```

```python
import functools

import jax
import jax.numpy as jnp
from jax import lax
from jax.experimental import pallas as pl
from jax.experimental.pallas import tpu as pltpu
from jax.sharding import PartitionSpec as P

F32, BF16 = jnp.float32, jnp.bfloat16
NODES, SEND, HALO, HUBS = 1024, 64, 256, 16
TABLE = NODES + HALO + HUBS
TILES = 9
COLS = TILES * 128
ROWS = TILES * TABLE
EDGES = 16384
HID, OUT, FIN = 512, 107, 200

ACCS = 4
GROUP = 4
BUILD_VMEM = 28 << 20
STEP_VMEM = 34 << 20
NT = (((1,), (1,)), ((), ()))


def split3(x):
    hi = x.astype(BF16)
    rest = x - hi.astype(F32)
    mid = rest.astype(BF16)
    return hi, mid, (rest - mid.astype(F32)).astype(BF16)


def in_hbm(a):
    return pltpu.with_memory_space_constraint(a, pltpu.HBM)


def dot(a, b):
    return jnp.dot(a, b, preferred_element_type=F32)


def dot_nt(a, b):
    return lax.dot_general(a, b, NT, preferred_element_type=F32)


def build_kernel(hub_hbm, dst_hbm, src_hbm, w_hbm, *refs):
    staged_in, refs = refs[:7], refs[7:]
    hi_ref, mid_ref, lo_ref, side_ref = refs[:4]
    staged_out, refs = refs[4:11], refs[11:]
    (hub_ref, dst_ref, src_ref, w_ref, row_ref, lane_ref, perm_ref, val_a, val_b, sem, stage_sem), rest = refs[:11], refs[11:]
    row_smem, accs = rest[:8], rest[8:]
    loads = []
    for i, (a, b) in enumerate(((hub_hbm, hub_ref), (dst_hbm, dst_ref), (src_hbm, src_ref), (w_hbm, w_ref))):
        loads.append(pltpu.make_async_copy(a, b, sem.at[8 + i]))
        loads[-1].start()
    stages = [pltpu.make_async_copy(a, b, stage_sem.at[i]) for i, (a, b) in enumerate(zip(staged_in, staged_out))]

    def clear(some):
        def zero(i, carry):
            for acc in some:
                acc[pl.ds(pl.multiple_of(i * 48, 8), 48), :] = jnp.zeros((48, 128), F32)
            return carry

        lax.fori_loop(0, ROWS // 48, zero, 0)

    clear(accs[:2])
    for load in loads:
        load.wait()
    base = lax.axis_index("graph") * NODES
    dst, src = dst_ref[...], src_ref[...]
    new_dst, new_src = dst, src
    for k in range(HUBS):
        local = hub_ref[k] - base
        local = jnp.where((local >= 0) & (local < NODES), local, -1)
        new_dst = jnp.where(dst == local, NODES + k, new_dst)
        new_src = jnp.where(src == local, NODES + HALO + k, new_src)
    row_ref[...] = (new_dst >> 7) * TABLE + new_src
    lane_ref[...] = new_dst & 127
    copies = []
    for s in range(8):
        perm_ref[s] = row_ref[pl.ds(s, 16, stride=8), :]
    for s in range(8):
        copies.append(pltpu.make_async_copy(perm_ref.at[s], row_smem[s], sem.at[s]))
        copies[-1].start()
    for stage in stages:
        stage.start()
    clear(accs[2:])

    iota = lax.broadcasted_iota(jnp.int32, (8, 128), 1)

    def wide(block, c):
        return jnp.broadcast_to(block[:, c:c + 1], (8, 128))

    def prep(g, val_ref):
        at = pl.ds(pl.multiple_of(g * 8, 8), 8)
        lanes, weights, rows = lane_ref[at, :], w_ref[at, :], row_ref[at, :]
        place = lax.broadcasted_iota(jnp.int32, (8, 128), 1) % GROUP
        terms = [(lanes, weights)]
        for d in range(1, GROUP):
            same = (place >= d) & (rows == pltpu.roll(rows, d, 1))
            terms.append((pltpu.roll(lanes, d, 1), jnp.where(same, pltpu.roll(weights, d, 1), 0.0)))
        def one(s):
            total = None
            for lane, weight in terms:
                hit = jnp.broadcast_to(lane[s:s + 1, :], (128, 128)) == sub
                part = jnp.where(hit, jnp.broadcast_to(weight[s:s + 1, :], (128, 128)), 0.0)
                total = part if total is None else total + part
            val_ref[s * 128:(s + 1) * 128, :] = jnp.transpose(total)

        return one

    def scatter(g, val_ref, c):
        for s in range(8):
            acc = accs[s % ACCS]
            rows = [row_smem[s][g, c + i] for i in range(GROUP)]
            sums = [acc[pl.ds(rows[i], 1), :] + val_ref[s * 128 + c + i:s * 128 + c + i + 1, :] for i in range(GROUP)]
            for r, total in zip(rows, sums):
                acc[pl.ds(r, 1), :] = total

    def both(g, val_ref, next_g, next_ref):
        one = prep(next_g, next_ref)
        for c in range(0, 128, GROUP):
            if c % 16 == 0:
                one(c // 16)
            scatter(g, val_ref, c)

    sub = lax.broadcasted_iota(jnp.int32, (128, 128), 0)
    first = prep(0, val_a)
    for s in range(8):
        first(s)
    for copy in copies:
        copy.wait()

    def turn(h, carry):
        both(2 * h, val_a, 2 * h + 1, val_b)
        both(2 * h + 1, val_b, jnp.minimum(2 * h + 2, 15), val_a)
        return carry

    lax.fori_loop(0, 8, turn, 0)

    def finish(i, carry):
        at = pl.multiple_of(i * 16, 16)
        for t in range(TILES):
            part = pl.ds(pl.multiple_of(t * TABLE + i * 16, 8), 16)
            total = accs[0][part, :]
            for acc in accs[1:]:
                total = total + acc[part, :]
            parts = split3(total)
            if t < TILES - 1:
                for piece, ref in zip(parts, (hi_ref, mid_ref, lo_ref)):
                    ref[pl.ds(at, 16), t * 128:(t + 1) * 128] = piece
            else:
                side = parts[0].astype(F32)
                for i, j in enumerate((1, 2, 0, 1, 0)):
                    side = side + pltpu.roll(parts[j].astype(F32), (i + 1) * HUBS, 1)
                side_ref[pl.ds(at, 16), :] = side.astype(BF16)
        return carry

    lax.fori_loop(0, TABLE // 16, finish, 0)
    for stage in stages:
        stage.wait()


def build(hub_ids, dst, src, w, *staged):
    piece = jax.ShapeDtypeStruct((TABLE, NODES), BF16)
    side = jax.ShapeDtypeStruct((TABLE, 128), BF16)
    square = lambda a: a.reshape(128, 128)
    table = pltpu.VMEM((128, 128), jnp.int32)
    return pl.pallas_call(
        build_kernel,
        out_shape=(piece, piece, piece, side) + tuple(jax.ShapeDtypeStruct(a.shape, a.dtype) for a in staged),
        in_specs=[pl.BlockSpec(memory_space=pltpu.HBM)] * 11,
        out_specs=(pl.BlockSpec(memory_space=pltpu.VMEM),) * 11,
        scratch_shapes=[
            pltpu.SMEM((HUBS,), jnp.int32), table, table, pltpu.VMEM((128, 128), F32), table, table,
            pltpu.VMEM((8, 16, 128), jnp.int32), pltpu.VMEM((1024, 128), F32), pltpu.VMEM((1024, 128), F32),
            pltpu.SemaphoreType.DMA((12,)), pltpu.SemaphoreType.DMA((7,)),
        ] + [pltpu.SMEM((16, 128), jnp.int32)] * 8 + [pltpu.VMEM((ROWS, 128), F32)] * ACCS,
        compiler_params=pltpu.CompilerParams(vmem_limit_bytes=BUILD_VMEM),
        name="build",
    )(*(in_hbm(a) for a in (hub_ids, square(dst), square(src), square(w)) + staged))


def step_kernel(
    hi_ref, mid_ref, lo_ref, side_ref, xt_ref, w1_ref, b1_ref, w2t_ref, dht_ref, send_ref, hub_ref,
    dxt_ref, dw1_ref, dw2t_ref, db1_ref, db2_ref,
    sent_s, pt_s, xs, xr, hs, hr, z_s, yt_s, d2_s, dhub_s, g2_s, g2h_s, rb, sb, ys, yr, dy_s, dyh_s, g1_s, sd, rd, dz1_s,
    hub3_s, y_cols_s, hid_s, live_s, dz2_s,
    a2, half2, got2, tot2, a1, half1, got1, tot1, send_sem, recv_sem,
):
    me = lax.axis_index("graph")
    sibling = me + 1 - 2 * lax.rem(me, 2)
    across = lax.rem(me + 2, 4)
    core = lax.rem(me, 2)
    mesh_id = pl.DeviceIdType.MESH
    peers = [lax.rem(me + d, 4) for d in (1, 2, 3)]
    barrier = pltpu.get_barrier_semaphore()
    for q in peers:
        pl.semaphore_signal(barrier, inc=1, device_id={"graph": q}, device_id_type=mesh_id)
    used = [0]

    def remote(src, dst, q):
        i = used[0]
        used[0] += 1
        copy = pltpu.make_async_remote_copy(
            src_ref=src, dst_ref=dst, send_sem=send_sem.at[i], recv_sem=recv_sem.at[i],
            device_id={"graph": q}, device_id_type=mesh_id)
        copy.start()
        return copy

    def wait_all(copies):
        for copy in copies:
            copy.wait()

    pieces = (hi_ref, mid_ref, lo_ref)
    hub_local = hub_ref[...] - me * NODES
    hub_row = jnp.where((hub_local >= 0) & (hub_local < NODES), hub_local, -1).astype(F32)
    hub_block = jnp.concatenate([hub_row, jnp.full((1, SEND - HUBS), -1.0, F32)], axis=1)
    send_row = send_ref[...].astype(F32)
    row = jnp.concatenate([jnp.where(me == q, hub_block, send_row[:, q * SEND:(q + 1) * SEND]) for q in range(4)], axis=1)
    row3 = jnp.concatenate([hub_row] * 3 + [jnp.full((1, 128 - 3 * HUBS), -1.0, F32)], axis=1)
    column = jnp.transpose(jnp.broadcast_to(jnp.concatenate([row, row3], axis=1), (128, 384)))
    lane = lax.broadcasted_iota(jnp.int32, (HALO + 3 * HUBS, 128), 1).astype(F32)
    picks = jnp.concatenate(
        [jnp.where(column[:HALO + 3 * HUBS] == lane + float(j * 128), 1.0, 0.0).astype(BF16) for j in range(8)], axis=1)
    xt = xt_ref[...]
    sent_s[...] = dot_nt(picks[:HALO], xt).astype(BF16).reshape(4, SEND, FIN)
    hub_col = column[HALO:HALO + HUBS]
    alias = [jnp.where((hub_col == row[:, j * 128:(j + 1) * 128]) & (hub_col >= 0.0), 1.0, 0.0) for j in range(2)]
    own_hub_x = sent_s[me, :HUBS, :]
    for q in range(4):
        xs[q, :SEND, :] = sent_s[q]
        xs[q, SEND:SEND + HUBS, :] = own_hub_x
        part = alias[q // 2][:, (q % 2) * SEND:(q % 2 + 1) * SEND]
        xs[q, SEND + HUBS:, :SEND] = part.astype(BF16)
        xs[q, SEND + HUBS:, SEND:] = jnp.zeros((HUBS, FIN - SEND), BF16)
    xr[me] = jnp.zeros((96, FIN), BF16)
    dht = dht_ref[...]
    dh = jnp.transpose(jnp.concatenate([dht, jnp.zeros((128 - OUT, NODES), F32)], axis=0))
    for j, piece in enumerate(split3(dh)):
        d2_s[:, j * 128:(j + 1) * 128] = piece
    pl.semaphore_wait(barrier, 3)
    round_a = [remote(xs.at[q], xr.at[me], q) for q in peers]
    hub_dh = dot(picks[HALO:HALO + HUBS], d2_s[...])
    hs[...] = (hub_dh[:, :128] + hub_dh[:, 128:256]) + hub_dh[:, 256:]
    hr[me] = hs[...]
    db2 = jnp.sum(dh, axis=0, keepdims=True)
    round_a += [remote(hs, hr.at[me], q) for q in peers]
    sub = lax.broadcasted_iota(jnp.int32, (NODES, HALO), 0).astype(F32)
    pt_s[...] = jnp.where(sub == row, 1.0, 0.0).astype(BF16)
    hub3_s[...] = picks[HALO:]

    def grad2(rows):
        a = dot(hi_ref[rows, :], d2_s[:, :256])
        b = dot(mid_ref[rows, :], d2_s[:, :256])
        c = dot(hi_ref[rows, :], d2_s[:, 256:]) + dot(lo_ref[rows, :], d2_s[:, :128])
        return ((c + b[:, 128:]) + (a[:, 128:] + b[:, :128])) + a[:, :128]

    far_rows = pl.ds(NODES, HALO + HUBS)
    g2h_s[...] = grad2(far_rows)

    def grad2_own(m, carry):
        at = pl.ds(pl.multiple_of(m * 256, 256), 256)
        g2_s[at, :] = grad2(at)
        return carry

    lax.fori_loop(0, 4, grad2_own, 0)
    w1t = jnp.transpose(jnp.concatenate([w1_ref[...], jnp.zeros((56, HID), BF16)], axis=0).astype(F32)).astype(BF16)[:, :FIN]
    z_s[:, :NODES] = dot(w1t, xt).astype(BF16)

    def forward_own(at):
        z = z_s[:, :NODES]
        acc = dot(z, hi_ref[:NODES, at])
        acc = acc + dot(z, mid_ref[:NODES, at])
        yt_s[:, at] = acc + dot(z, lo_ref[:NODES, at])

    def over_columns(body):
        def turn(n, carry):
            body(pl.ds(pl.multiple_of(n * 256, 256), 256))
            return carry

        lax.fori_loop(0, 4, turn, 0)

    y_side = dot(z_s[:, :NODES], side_ref[:NODES, :])
    wait_all(round_a)

    halo_x = jnp.concatenate([xr[q, :SEND, :] for q in range(4)], axis=0)
    hub_x = sent_s[me, :HUBS, :].astype(F32)
    for q in range(4):
        hub_x = hub_x + xr[q, SEND:SEND + HUBS, :].astype(F32)
    z_s[:, NODES:] = dot_nt(w1t, halo_x).astype(BF16)
    z_hub = dot_nt(w1t, jnp.concatenate([hub_x.astype(BF16)] * 3, axis=0)).astype(BF16)

    def forward_far(at):
        z = z_s[:, NODES:]
        acc = yt_s[:, at]
        for ref in pieces:
            acc = acc + dot(z, ref[NODES:NODES + HALO, at])
        hub_rows = jnp.concatenate([ref[NODES + HALO:, at] for ref in pieces], axis=0)
        yt_s[:, at] = acc + dot(z_hub, hub_rows)

    y_side = y_side + dot(z_s[:, NODES:], side_ref[NODES:NODES + HALO, :])
    y_side = jnp.transpose(y_side + dot(z_hub[:, :HUBS], side_ref[NODES + HALO:, :]))
    ys[...] = (y_side[:HUBS] + y_side[HUBS:2 * HUBS]) + y_side[2 * HUBS:3 * HUBS]
    yr[me] = ys[...]
    hub_dh = (hr[0] + hr[1]) + (hr[2] + hr[3])
    def side_by_side(x):
        hi, mid, lo = split3(x)
        return jnp.concatenate([hi, hi, hi, mid, mid, lo, jnp.zeros((32, x.shape[1]), BF16)], axis=0)

    dhub_s[...] = side_by_side(hub_dh)
    round_b = [remote(ys, yr.at[me], q) for q in peers]
    g2h_s[...] += dot(side_ref[far_rows, :], dhub_s[...])
    far = g2h_s[:HALO, :]
    alias_row = jnp.concatenate([xr[q, SEND + HUBS:, :SEND] for q in range(4)], axis=1)
    hub_g2 = g2h_s[HALO:, :]
    for piece in split3(far):
        hub_g2 = hub_g2 + dot(alias_row, piece)
    is_alias = dot(jnp.transpose(jnp.concatenate([alias_row.astype(F32), jnp.zeros((112, HALO), F32)], axis=0)).astype(BF16),
                   jnp.ones((128, 128), BF16))
    far = jnp.where(is_alias > 0.5, 0.0, far)
    for q in range(4):
        sb[q, :SEND, :] = far[q * SEND:(q + 1) * SEND]
        sb[q, SEND:, :] = hub_g2
    rb[me] = sb[me]
    round_b += [remote(sb.at[q], rb.at[me], q) for q in peers]

    over_columns(forward_own)
    over_columns(forward_far)

    def grad2_hub(m, carry):
        at = pl.ds(pl.multiple_of(m * 256, 256), 256)
        g2_s[at, :] += dot(side_ref[at, :], dhub_s[...])
        return carry

    lax.fori_loop(0, 4, grad2_hub, 0)
    wait_all(round_b)

    def returned(ref):
        hub_sum = (ref[0, SEND:, :] + ref[1, SEND:, :]) + (ref[2, SEND:, :] + ref[3, SEND:, :])
        ref[me, :HUBS, :] = hub_sum
        ref[me, HUBS:SEND, :] = jnp.zeros((SEND - HUBS, hub_sum.shape[1]), F32)
        return ref[:, :SEND, :].reshape(HALO, hub_sum.shape[1]), hub_sum

    back, hub_sum = returned(rb)
    hub_dz2 = hub_sum.astype(BF16)
    back_parts = split3(back)

    def over_blocks(body, carry=0):
        def turn(n, carry):
            return body(pl.ds(pl.multiple_of(n * 256, 256), 256), carry)

        return lax.fori_loop(0, 4, turn, carry)

    def dz2_block(at, carry):
        own = g2_s[at, :]
        for piece in back_parts:
            own = own + dot(pt_s[at, :], piece)
        dz2_s[at, :] = own.astype(BF16)
        return carry

    over_blocks(dz2_block)

    y_hub = (yr[0] + yr[1]) + (yr[2] + yr[3])
    b1 = b1_ref[...]
    b1_col = jnp.transpose(jnp.broadcast_to(b1, (128, HID)))
    y_rows = jnp.concatenate([piece.astype(F32) for piece in split3(y_hub)] + [jnp.zeros((128 - 3 * HUBS, HID), F32)], axis=0)
    y_cols_s[...] = jnp.transpose(y_rows).astype(BF16)[:, :3 * HUBS]

    def pre_block(at, carry):
        pre = (yt_s[:, at] + dot(y_cols_s[...], hub3_s[:, at])) + jnp.concatenate([b1_col] * 2, axis=1)
        hid_s[:, at] = jnp.maximum(pre, 0.0).astype(BF16)
        live_s[:, at] = jnp.where(pre > 0.0, 1.0, 0.0)
        return carry

    over_blocks(pre_block)

    class GroupSum:
        def __init__(self, own, half, got, total):
            self.own, self.half, self.got, self.total = own, half, got, total
            self.copy = remote(own.at[1 - core], got.at[0], sibling)

        def across(self):
            self.copy.wait()
            self.half[...] = self.own[core] + self.got[0]
            self.copy = remote(self.half, self.got.at[1], across)

        def back(self):
            self.copy.wait()
            self.total[core] = self.half[...] + self.got[1]
            self.copy = remote(self.total.at[core], self.total.at[core], sibling)

        def done(self):
            self.copy.wait()

    dw2t = jnp.transpose(dot(hid_s[...], dz2_s[...]))
    for h in range(2):
        a2[h, :112, :] = dw2t[:112, h * 256:(h + 1) * 256]
        a2[h, 112:, :128] = jnp.broadcast_to(db2, (8, 128))
        a2[h, 112:, 128:] = jnp.zeros((8, 128), F32)
    sum2 = GroupSum(a2, half2, got2, tot2)

    def dy_block(at, db1):
        live = jnp.transpose(live_s[:, at])
        dy = jnp.where(live > 0.5, dot(dz2_s[at, :OUT], w2t_ref[...]), 0.0)
        for j, piece in enumerate(split3(dy)):
            dy_s[j, at, :] = piece
        return db1 + jnp.sum(dy, axis=0, keepdims=True)

    db1 = over_blocks(dy_block, jnp.zeros((1, HID), F32))
    hub_dy = jnp.where(y_hub + b1 > 0.0, dot(hub_dz2[:, :OUT], w2t_ref[...]), 0.0)
    dyh_s[...] = side_by_side(hub_dy)
    sum2.across()

    def grad1(rows, cols):
        acc = dot(lo_ref[rows, :], dy_s[0, :, cols])
        acc = acc + dot(mid_ref[rows, :], dy_s[1, :, cols])
        acc = acc + dot(hi_ref[rows, :], dy_s[2, :, cols])
        acc = acc + dot(mid_ref[rows, :], dy_s[0, :, cols])
        acc = acc + dot(hi_ref[rows, :], dy_s[1, :, cols])
        acc = acc + dot(hi_ref[rows, :], dy_s[0, :, cols])
        return acc + dot(side_ref[rows, :], dyh_s[:, cols])

    halves = (pl.ds(0, 256), pl.ds(256, 256))
    round_d = []
    for h, cols in enumerate(halves):
        ret = grad1(far_rows, cols)
        for q in range(4):
            sd[h, q, :SEND, :] = ret[q * SEND:(q + 1) * SEND]
            sd[h, q, SEND:, :] = ret[HALO:]
        rd[h, me] = sd[h, me]
        round_d.append([remote(sd.at[h, q], rd.at[h, me], q) for q in peers])

    def grad1_own(h, m):
        rows = pl.ds(m * 512, 512)
        g1_s[rows, halves[h]] = grad1(rows, halves[h])

    def finish(h):
        wait_all(round_d[h])
        cols = halves[h]
        back, _ = returned(rd.at[h])
        dz1 = g1_s[:, cols]
        for piece in split3(back):
            dz1 = dz1 + dot(pt_s[...], piece)
        dz1 = dz1.astype(BF16)
        dz1_s[:, cols] = dz1
        dw1 = dot(xt_ref[...], dz1)
        for i in range(2):
            at = slice(i * 128, (i + 1) * 128)
            a1[h, i, :FIN, :] = dw1[:, at]
            a1[h, i, FIN:, :] = jnp.broadcast_to(db1[:, h * 256 + i * 128:h * 256 + (i + 1) * 128], (8, 128))
        return GroupSum(a1.at[h], half1.at[h], got1.at[h], tot1.at[h])

    grad1_own(0, 0)
    grad1_own(0, 1)
    sum1 = [finish(0)]
    sum2.back()
    grad1_own(1, 0)
    sum1[0].across()
    grad1_own(1, 1)
    sum1.append(finish(1))
    sum2.done()
    for h in range(2):
        dw2t_ref[:, h * 256:(h + 1) * 256] = tot2[h, :OUT, :]
    db2_ref[...] = tot2[0, 112:113, :OUT]
    sum1[1].across()
    dxt_ref[...] = dot_nt(w1_ref[...], dz1_s[...])
    sum1[0].back()
    sum1[0].done()

    def put(h):
        for i in range(2):
            at = slice(h * 256 + i * 128, h * 256 + (i + 1) * 128)
            dw1_ref[:, at] = tot1[h, i, :FIN, :]
            db1_ref[:, at] = tot1[h, i, FIN:FIN + 1, :]

    put(0)
    sum1[1].back()
    sum1[1].done()
    put(1)


def step(*operands):
    vmem = pl.BlockSpec(memory_space=pltpu.VMEM)
    out = lambda *shape: jax.ShapeDtypeStruct(shape, F32)
    f32 = lambda *shape: pltpu.VMEM(shape, F32)
    b16 = lambda *shape: pltpu.VMEM(shape, BF16)
    return pl.pallas_call(
        step_kernel,
        out_shape=(out(FIN, NODES), out(FIN, HID), out(OUT, HID), out(1, HID), out(1, OUT)),
        in_specs=[vmem] * 11,
        out_specs=(vmem,) * 5,
        scratch_shapes=[
            b16(4, SEND, FIN), b16(NODES, HALO), b16(4, 96, FIN), b16(4, 96, FIN), f32(HUBS, 128), f32(4, HUBS, 128),
            b16(HID, NODES + HALO), f32(HID, NODES), b16(NODES, 384), b16(128, 128), f32(NODES, 128), f32(HALO + HUBS, 128),
            f32(4, SEND + HUBS, 128), f32(4, SEND + HUBS, 128), f32(HUBS, HID), f32(4, HUBS, HID),
            b16(3, NODES, HID), b16(128, HID), f32(NODES, HID), f32(2, 4, SEND + HUBS, 256), f32(2, 4, SEND + HUBS, 256), b16(NODES, HID),
            b16(3 * HUBS, NODES), b16(HID, 3 * HUBS), b16(HID, NODES), f32(HID, NODES), b16(NODES, 128),
            f32(2, 120, 256), f32(120, 256), f32(2, 120, 256), f32(2, 120, 256),
            f32(2, 2, 208, 128), f32(2, 208, 128), f32(2, 2, 208, 128), f32(2, 2, 208, 128),
            pltpu.SemaphoreType.DMA((28,)), pltpu.SemaphoreType.DMA((28,)),
        ],
        compiler_params=pltpu.CompilerParams(collective_id=0, has_side_effects=True, vmem_limit_bytes=STEP_VMEM),
        name="step",
    )(*operands)


def emit_kernel(*refs):
    ins, outs, sem = refs[:5], refs[5:10], refs[10]
    copies = [pltpu.make_async_copy(a, b, sem.at[i]) for i, (a, b) in enumerate(zip(ins, outs))]
    for copy in copies:
        copy.start()
    for copy in copies:
        copy.wait()


def emit(*arrays):
    return pl.pallas_call(
        emit_kernel,
        out_shape=tuple(jax.ShapeDtypeStruct(a.shape, a.dtype) for a in arrays),
        in_specs=[pl.BlockSpec(memory_space=pltpu.VMEM)] * 5,
        out_specs=(pl.BlockSpec(memory_space=pltpu.HBM),) * 5,
        scratch_shapes=[pltpu.SemaphoreType.DMA((5,))],
        compiler_params=pltpu.CompilerParams(vmem_limit_bytes=4 << 20),
        name="emit",
    )(*arrays)


def solution(mesh):
    vertex_spec = P(("data", "graph"))
    vertex_rows = P(("data", "graph"), None)
    part_spec = P("data")
    part_rows = P("data", None)
    replicated = P()

    def device_step(x, dst, src, w, send, hub_ids, w_first, b_first, w_second, dy_out):
        dx, dw1, dw2, db1, db2 = emit(*step(*build(
            hub_ids, dst, src, w,
            x.T, w_first, b_first.reshape(1, HID), w_second.T, dy_out.T, send.reshape(1, HALO), hub_ids.reshape(1, HUBS))))
        return dx.T, dw1, dw2.T, db1.reshape(HID), db2.reshape(OUT)

    return jax.shard_map(
        device_step,
        mesh=mesh,
        in_specs=(vertex_rows, vertex_spec, vertex_spec, vertex_spec, vertex_spec, part_spec, replicated, replicated, replicated, vertex_rows),
        out_specs=(vertex_rows, part_rows, part_rows, part_spec, part_spec),
        check_vma=False,
    )
```

```python
import functools

import jax
import jax.numpy as jnp
from jax import lax
from jax.experimental import pallas as pl
from jax.experimental.pallas import tpu as pltpu
from jax.sharding import PartitionSpec as P

F32, BF16 = jnp.float32, jnp.bfloat16
NODES, SEND, HALO, HUBS = 1024, 64, 256, 16
TABLE = NODES + HALO + HUBS
TILES = 9
COLS = TILES * 128
ROWS = TILES * TABLE
EDGES = 16384
HID, OUT, FIN = 512, 107, 200

ACCS = 4
GROUP = 4
BUILD_VMEM = 28 << 20
STEP_VMEM = 34 << 20
NT = (((1,), (1,)), ((), ()))


def split3(x):
    hi = x.astype(BF16)
    rest = x - hi.astype(F32)
    mid = rest.astype(BF16)
    return hi, mid, (rest - mid.astype(F32)).astype(BF16)


def in_hbm(a):
    return pltpu.with_memory_space_constraint(a, pltpu.HBM)


def dot(a, b):
    return jnp.dot(a, b, preferred_element_type=F32)


def dot_nt(a, b):
    return lax.dot_general(a, b, NT, preferred_element_type=F32)


def build_kernel(hub_hbm, dst_hbm, src_hbm, w_hbm, *refs):
    staged_in, refs = refs[:7], refs[7:]
    hi_ref, mid_ref, lo_ref, side_ref = refs[:4]
    staged_out, refs = refs[4:11], refs[11:]
    (hub_ref, dst_ref, src_ref, w_ref, row_ref, lane_ref, perm_ref, val_a, val_b, sem, stage_sem), rest = refs[:11], refs[11:]
    row_smem, accs = rest[:8], rest[8:]
    loads = []
    for i, (a, b) in enumerate(((hub_hbm, hub_ref), (dst_hbm, dst_ref), (src_hbm, src_ref), (w_hbm, w_ref))):
        loads.append(pltpu.make_async_copy(a, b, sem.at[8 + i]))
        loads[-1].start()
    stages = [pltpu.make_async_copy(a, b, stage_sem.at[i]) for i, (a, b) in enumerate(zip(staged_in, staged_out))]

    def clear(some):
        def zero(i, carry):
            for acc in some:
                acc[pl.ds(pl.multiple_of(i * 48, 8), 48), :] = jnp.zeros((48, 128), F32)
            return carry

        lax.fori_loop(0, ROWS // 48, zero, 0)

    clear(accs[:2])
    for load in loads:
        load.wait()
    base = lax.axis_index("graph") * NODES
    dst, src = dst_ref[...], src_ref[...]
    new_dst, new_src = dst, src
    for k in range(HUBS):
        local = hub_ref[k] - base
        local = jnp.where((local >= 0) & (local < NODES), local, -1)
        new_dst = jnp.where(dst == local, NODES + k, new_dst)
        new_src = jnp.where(src == local, NODES + HALO + k, new_src)
    row_ref[...] = (new_dst >> 7) * TABLE + new_src
    lane_ref[...] = new_dst & 127
    copies = []
    for s in range(8):
        perm_ref[s] = row_ref[pl.ds(s, 16, stride=8), :]
    for s in range(8):
        copies.append(pltpu.make_async_copy(perm_ref.at[s], row_smem[s], sem.at[s]))
        copies[-1].start()
    for stage in stages:
        stage.start()
    clear(accs[2:])

    iota = lax.broadcasted_iota(jnp.int32, (8, 128), 1)

    def wide(block, c):
        return jnp.broadcast_to(block[:, c:c + 1], (8, 128))

    def prep(g, val_ref):
        at = pl.ds(pl.multiple_of(g * 8, 8), 8)
        lanes, weights, rows = lane_ref[at, :], w_ref[at, :], row_ref[at, :]
        place = lax.broadcasted_iota(jnp.int32, (8, 128), 1) % GROUP
        terms = [(lanes, weights)]
        for d in range(1, GROUP):
            same = (place >= d) & (rows == pltpu.roll(rows, d, 1))
            terms.append((pltpu.roll(lanes, d, 1), jnp.where(same, pltpu.roll(weights, d, 1), 0.0)))
        def one(s):
            total = None
            for lane, weight in terms:
                hit = jnp.broadcast_to(lane[s:s + 1, :], (128, 128)) == sub
                part = jnp.where(hit, jnp.broadcast_to(weight[s:s + 1, :], (128, 128)), 0.0)
                total = part if total is None else total + part
            val_ref[s * 128:(s + 1) * 128, :] = jnp.transpose(total)

        return one

    def scatter(g, val_ref, c):
        for s in range(8):
            acc = accs[s % ACCS]
            rows = [row_smem[s][g, c + i] for i in range(GROUP)]
            sums = [acc[pl.ds(rows[i], 1), :] + val_ref[s * 128 + c + i:s * 128 + c + i + 1, :] for i in range(GROUP)]
            for r, total in zip(rows, sums):
                acc[pl.ds(r, 1), :] = total

    def both(g, val_ref, next_g, next_ref):
        one = prep(next_g, next_ref)
        for c in range(0, 128, GROUP):
            if c % 16 == 0:
                one(c // 16)
            scatter(g, val_ref, c)

    sub = lax.broadcasted_iota(jnp.int32, (128, 128), 0)
    first = prep(0, val_a)
    for s in range(8):
        first(s)
    for copy in copies:
        copy.wait()

    def turn(h, carry):
        both(2 * h, val_a, 2 * h + 1, val_b)
        both(2 * h + 1, val_b, jnp.minimum(2 * h + 2, 15), val_a)
        return carry

    lax.fori_loop(0, 8, turn, 0)

    def finish(i, carry):
        at = pl.multiple_of(i * 16, 16)
        for t in range(TILES):
            part = pl.ds(pl.multiple_of(t * TABLE + i * 16, 8), 16)
            total = accs[0][part, :]
            for acc in accs[1:]:
                total = total + acc[part, :]
            parts = split3(total)
            if t < TILES - 1:
                for piece, ref in zip(parts, (hi_ref, mid_ref, lo_ref)):
                    ref[pl.ds(at, 16), t * 128:(t + 1) * 128] = piece
            else:
                side = parts[0].astype(F32)
                for i, j in enumerate((1, 2, 0, 1, 0)):
                    side = side + pltpu.roll(parts[j].astype(F32), (i + 1) * HUBS, 1)
                side_ref[pl.ds(at, 16), :] = side.astype(BF16)
        return carry

    lax.fori_loop(0, TABLE // 16, finish, 0)
    for stage in stages:
        stage.wait()


def build(hub_ids, dst, src, w, *staged):
    piece = jax.ShapeDtypeStruct((TABLE, NODES), BF16)
    side = jax.ShapeDtypeStruct((TABLE, 128), BF16)
    square = lambda a: a.reshape(128, 128)
    table = pltpu.VMEM((128, 128), jnp.int32)
    return pl.pallas_call(
        build_kernel,
        out_shape=(piece, piece, piece, side) + tuple(jax.ShapeDtypeStruct(a.shape, a.dtype) for a in staged),
        in_specs=[pl.BlockSpec(memory_space=pltpu.HBM)] * 11,
        out_specs=(pl.BlockSpec(memory_space=pltpu.VMEM),) * 11,
        scratch_shapes=[
            pltpu.SMEM((HUBS,), jnp.int32), table, table, pltpu.VMEM((128, 128), F32), table, table,
            pltpu.VMEM((8, 16, 128), jnp.int32), pltpu.VMEM((1024, 128), F32), pltpu.VMEM((1024, 128), F32),
            pltpu.SemaphoreType.DMA((12,)), pltpu.SemaphoreType.DMA((7,)),
        ] + [pltpu.SMEM((16, 128), jnp.int32)] * 8 + [pltpu.VMEM((ROWS, 128), F32)] * ACCS,
        compiler_params=pltpu.CompilerParams(vmem_limit_bytes=BUILD_VMEM),
        name="build",
    )(*(in_hbm(a) for a in (hub_ids, square(dst), square(src), square(w)) + staged))


def step_kernel(
    hi_ref, mid_ref, lo_ref, side_ref, xt_ref, w1_ref, b1_ref, w2t_ref, dht_ref, send_ref, hub_ref,
    dxt_ref, dw1_ref, dw2t_ref, db1_ref, db2_ref,
    sent_s, pt_s, xs, xr, hs, hr, z_s, yt_s, d2_s, dhub_s, g2_s, g2h_s, rb, sb, ys, yr, dy_s, dyh_s, g1_s, sd, rd, dz1_s,
    hub3_s, y_cols_s, hid_s, live_s, dz2_s,
    a2, half2, got2, tot2, a1, half1, got1, tot1, send_sem, recv_sem,
):
    me = lax.axis_index("graph")
    sibling = me + 1 - 2 * lax.rem(me, 2)
    across = lax.rem(me + 2, 4)
    core = lax.rem(me, 2)
    mesh_id = pl.DeviceIdType.MESH
    peers = [lax.rem(me + d, 4) for d in (1, 2, 3)]
    barrier = pltpu.get_barrier_semaphore()
    for q in peers:
        pl.semaphore_signal(barrier, inc=1, device_id={"graph": q}, device_id_type=mesh_id)
    used = [0]

    def remote(src, dst, q):
        i = used[0]
        used[0] += 1
        copy = pltpu.make_async_remote_copy(
            src_ref=src, dst_ref=dst, send_sem=send_sem.at[i], recv_sem=recv_sem.at[i],
            device_id={"graph": q}, device_id_type=mesh_id)
        copy.start()
        return copy

    def wait_all(copies):
        for copy in copies:
            copy.wait()

    pieces = (hi_ref, mid_ref, lo_ref)
    hub_local = hub_ref[...] - me * NODES
    hub_row = jnp.where((hub_local >= 0) & (hub_local < NODES), hub_local, -1).astype(F32)
    hub_block = jnp.concatenate([hub_row, jnp.full((1, SEND - HUBS), -1.0, F32)], axis=1)
    send_row = send_ref[...].astype(F32)
    row = jnp.concatenate([jnp.where(me == q, hub_block, send_row[:, q * SEND:(q + 1) * SEND]) for q in range(4)], axis=1)
    row3 = jnp.concatenate([hub_row] * 3 + [jnp.full((1, 128 - 3 * HUBS), -1.0, F32)], axis=1)
    column = jnp.transpose(jnp.broadcast_to(jnp.concatenate([row, row3], axis=1), (128, 384)))
    lane = lax.broadcasted_iota(jnp.int32, (HALO + 3 * HUBS, 128), 1).astype(F32)
    picks = jnp.concatenate(
        [jnp.where(column[:HALO + 3 * HUBS] == lane + float(j * 128), 1.0, 0.0).astype(BF16) for j in range(8)], axis=1)
    xt = xt_ref[...]
    sent_s[...] = dot_nt(picks[:HALO], xt).astype(BF16).reshape(4, SEND, FIN)
    hub_col = column[HALO:HALO + HUBS]
    alias = [jnp.where((hub_col == row[:, j * 128:(j + 1) * 128]) & (hub_col >= 0.0), 1.0, 0.0) for j in range(2)]
    dht = dht_ref[...]
    dh = jnp.transpose(jnp.concatenate([dht, jnp.zeros((128 - OUT, NODES), F32)], axis=0))
    for j, piece in enumerate(split3(dh)):
        d2_s[:, j * 128:(j + 1) * 128] = piece
    hub_dh = dot(picks[HALO:HALO + HUBS], d2_s[...])
    hub_dh = (hub_dh[:, :128] + hub_dh[:, 128:256]) + hub_dh[:, 256:]
    for q in range(4):
        hs[q, :HUBS, :] = hub_dh
        part = alias[q // 2][:, (q % 2) * SEND:(q % 2 + 1) * SEND]
        hs[q, HUBS:, :] = jnp.concatenate([part, jnp.zeros((HUBS, 128 - SEND), F32)], axis=1)
    hr[me, :HUBS, :] = hub_dh
    hr[me, HUBS:, :] = jnp.zeros((HUBS, 128), F32)
    own_hub_x = sent_s[me, :HUBS, :]
    xs[:, :, FIN:] = jnp.zeros((4, SEND + HUBS, 256 - FIN), BF16)
    for q in range(4):
        xs[q, :SEND, :FIN] = sent_s[q]
        xs[q, SEND:, :FIN] = own_hub_x
    xr[me] = jnp.zeros((SEND + HUBS, 256), BF16)
    pl.semaphore_wait(barrier, 3)
    round_a = [remote(hs.at[q], hr.at[me], q) for q in peers]
    round_x = [remote(xs.at[q], xr.at[me], q) for q in peers]
    db2 = jnp.sum(dh, axis=0, keepdims=True)
    sub = lax.broadcasted_iota(jnp.int32, (NODES, HALO), 0).astype(F32)
    pt_s[...] = jnp.where(sub == row, 1.0, 0.0).astype(BF16)
    hub3_s[...] = picks[HALO:]

    def grad2(rows):
        a = dot(hi_ref[rows, :], d2_s[:, :256])
        b = dot(mid_ref[rows, :], d2_s[:, :256])
        c = dot(hi_ref[rows, :], d2_s[:, 256:]) + dot(lo_ref[rows, :], d2_s[:, :128])
        return ((c + b[:, 128:]) + (a[:, 128:] + b[:, :128])) + a[:, :128]

    def over_blocks(body, carry=0, first=0, last=4):
        def turn(n, carry):
            return body(pl.ds(pl.multiple_of(n * 256, 256), 256), carry)

        return lax.fori_loop(first, last, turn, carry)

    def grad2_own(at, carry):
        g2_s[at, :] = grad2(at)
        return carry

    over_blocks(grad2_own)
    far_rows = pl.ds(NODES, HALO + HUBS)
    g2h_s[...] = grad2(far_rows)
    wait_all(round_a)

    def side_by_side(x):
        hi, mid, lo = split3(x)
        return jnp.concatenate([hi, hi, hi, mid, mid, lo, jnp.zeros((32, x.shape[1]), BF16)], axis=0)

    dhub_s[...] = side_by_side((hr[0, :HUBS] + hr[1, :HUBS]) + (hr[2, :HUBS] + hr[3, :HUBS]))
    g2h_s[...] += dot(side_ref[far_rows, :], dhub_s[...])
    far = g2h_s[:HALO, :]
    alias_row = jnp.concatenate([hr[q, HUBS:, :SEND] for q in range(4)], axis=1)
    hub_g2 = g2h_s[HALO:, :]
    for piece in split3(far):
        hub_g2 = hub_g2 + dot(alias_row.astype(BF16), piece)
    is_alias = dot(jnp.transpose(jnp.concatenate([alias_row, jnp.zeros((112, HALO), F32)], axis=0)).astype(BF16),
                   jnp.ones((128, 128), BF16))
    far = jnp.where(is_alias > 0.5, 0.0, far)
    for q in range(4):
        sb[q, :SEND, :] = far[q * SEND:(q + 1) * SEND]
        sb[q, SEND:, :] = hub_g2
    rb[me] = sb[me]
    round_b = [remote(sb.at[q], rb.at[me], q) for q in peers]

    w1t = jnp.transpose(jnp.concatenate([w1_ref[...], jnp.zeros((56, HID), BF16)], axis=0).astype(F32)).astype(BF16)[:, :FIN]
    z_s[:, :NODES] = dot(w1t, xt).astype(BF16)

    def forward_own(at, carry):
        z = z_s[:, :NODES]
        acc = dot(z, hi_ref[:NODES, at])
        acc = acc + dot(z, mid_ref[:NODES, at])
        yt_s[:, at] = acc + dot(z, lo_ref[:NODES, at])
        return carry

    over_blocks(forward_own, 0, 0, 2)
    y_side = dot(z_s[:, :NODES], side_ref[:NODES, :])
    wait_all(round_x)

    halo_x = jnp.concatenate([xr[q, :SEND, :FIN] for q in range(4)], axis=0)
    hub_x = own_hub_x.astype(F32)
    for q in range(4):
        hub_x = hub_x + xr[q, SEND:, :FIN].astype(F32)
    z_s[:, NODES:] = dot_nt(w1t, halo_x).astype(BF16)
    z_hub = dot_nt(w1t, jnp.concatenate([hub_x.astype(BF16)] * 3, axis=0)).astype(BF16)
    y_side = y_side + dot(z_s[:, NODES:], side_ref[NODES:NODES + HALO, :])
    y_side = jnp.transpose(y_side + dot(z_hub[:, :HUBS], side_ref[NODES + HALO:, :]))
    ys[...] = (y_side[:HUBS] + y_side[HUBS:2 * HUBS]) + y_side[2 * HUBS:3 * HUBS]
    yr[me] = ys[...]
    round_y = [remote(ys, yr.at[me], q) for q in peers]

    over_blocks(forward_own, 0, 2, 4)

    def forward_far(at, carry):
        z = z_s[:, NODES:]
        acc = yt_s[:, at]
        for ref in pieces:
            acc = acc + dot(z, ref[NODES:NODES + HALO, at])
        hub_rows = jnp.concatenate([ref[NODES + HALO:, at] for ref in pieces], axis=0)
        yt_s[:, at] = acc + dot(z_hub, hub_rows)
        g2_s[at, :] += dot(side_ref[at, :], dhub_s[...])
        return carry

    over_blocks(forward_far)
    wait_all(round_b)

    def returned(ref):
        hub_sum = (ref[0, SEND:, :] + ref[1, SEND:, :]) + (ref[2, SEND:, :] + ref[3, SEND:, :])
        ref[me, :HUBS, :] = hub_sum
        ref[me, HUBS:SEND, :] = jnp.zeros((SEND - HUBS, hub_sum.shape[1]), F32)
        return ref[:, :SEND, :].reshape(HALO, hub_sum.shape[1]), hub_sum

    back, hub_sum = returned(rb)
    hub_dz2 = hub_sum.astype(BF16)
    back_parts = split3(back)

    def dz2_block(at, carry):
        own = g2_s[at, :]
        for piece in back_parts:
            own = own + dot(pt_s[at, :], piece)
        dz2_s[at, :] = own.astype(BF16)
        return carry

    over_blocks(dz2_block)

    wait_all(round_y)
    y_hub = (yr[0] + yr[1]) + (yr[2] + yr[3])
    b1 = b1_ref[...]
    b1_col = jnp.transpose(jnp.broadcast_to(b1, (128, HID)))
    y_rows = jnp.concatenate([piece.astype(F32) for piece in split3(y_hub)] + [jnp.zeros((128 - 3 * HUBS, HID), F32)], axis=0)
    y_cols_s[...] = jnp.transpose(y_rows).astype(BF16)[:, :3 * HUBS]

    def pre_block(at, carry):
        pre = (yt_s[:, at] + dot(y_cols_s[...], hub3_s[:, at])) + jnp.concatenate([b1_col] * 2, axis=1)
        hid_s[:, at] = jnp.maximum(pre, 0.0).astype(BF16)
        live_s[:, at] = jnp.where(pre > 0.0, 1.0, 0.0)
        return carry

    over_blocks(pre_block)

    class GroupSum:
        def __init__(self, own, half, got, total):
            self.own, self.half, self.got, self.total = own, half, got, total
            self.copy = remote(own.at[1 - core], got.at[0], sibling)

        def across(self):
            self.copy.wait()
            self.half[...] = self.own[core] + self.got[0]
            self.copy = remote(self.half, self.got.at[1], across)

        def back(self):
            self.copy.wait()
            self.total[core] = self.half[...] + self.got[1]
            self.copy = remote(self.total.at[core], self.total.at[core], sibling)

        def done(self):
            self.copy.wait()

    dw2t = jnp.transpose(dot(hid_s[...], dz2_s[...]))
    for h in range(2):
        a2[h, :112, :] = dw2t[:112, h * 256:(h + 1) * 256]
        a2[h, 112:, :128] = jnp.broadcast_to(db2, (8, 128))
        a2[h, 112:, 128:] = jnp.zeros((8, 128), F32)
    sum2 = GroupSum(a2, half2, got2, tot2)

    def dy_block(at, db1):
        live = jnp.transpose(live_s[:, at])
        dy = jnp.where(live > 0.5, dot(dz2_s[at, :OUT], w2t_ref[...]), 0.0)
        for j, piece in enumerate(split3(dy)):
            dy_s[j, at, :] = piece
        return db1 + jnp.sum(dy, axis=0, keepdims=True)

    db1 = over_blocks(dy_block, jnp.zeros((1, HID), F32))
    hub_dy = jnp.where(y_hub + b1 > 0.0, dot(hub_dz2[:, :OUT], w2t_ref[...]), 0.0)
    dyh_s[...] = side_by_side(hub_dy)
    sum2.across()

    def grad1(rows, cols):
        acc = dot(lo_ref[rows, :], dy_s[0, :, cols])
        acc = acc + dot(mid_ref[rows, :], dy_s[1, :, cols])
        acc = acc + dot(hi_ref[rows, :], dy_s[2, :, cols])
        acc = acc + dot(mid_ref[rows, :], dy_s[0, :, cols])
        acc = acc + dot(hi_ref[rows, :], dy_s[1, :, cols])
        acc = acc + dot(hi_ref[rows, :], dy_s[0, :, cols])
        return acc + dot(side_ref[rows, :], dyh_s[:, cols])

    halves = (pl.ds(0, 256), pl.ds(256, 256))
    round_d = []
    for h, cols in enumerate(halves):
        ret = grad1(far_rows, cols)
        for q in range(4):
            sd[h, q, :SEND, :] = ret[q * SEND:(q + 1) * SEND]
            sd[h, q, SEND:, :] = ret[HALO:]
        rd[h, me] = sd[h, me]
        round_d.append([remote(sd.at[h, q], rd.at[h, me], q) for q in peers])

    def grad1_own(h, m):
        rows = pl.ds(m * 512, 512)
        g1_s[rows, halves[h]] = grad1(rows, halves[h])

    def finish(h):
        wait_all(round_d[h])
        cols = halves[h]
        back, _ = returned(rd.at[h])
        dz1 = g1_s[:, cols]
        for piece in split3(back):
            dz1 = dz1 + dot(pt_s[...], piece)
        dz1 = dz1.astype(BF16)
        dz1_s[:, cols] = dz1
        dw1 = dot(xt_ref[...], dz1)
        for i in range(2):
            at = slice(i * 128, (i + 1) * 128)
            a1[h, i, :FIN, :] = dw1[:, at]
            a1[h, i, FIN:, :] = jnp.broadcast_to(db1[:, h * 256 + i * 128:h * 256 + (i + 1) * 128], (8, 128))
        return GroupSum(a1.at[h], half1.at[h], got1.at[h], tot1.at[h])

    grad1_own(0, 0)
    grad1_own(0, 1)
    sum1 = [finish(0)]
    sum2.back()
    grad1_own(1, 0)
    sum1[0].across()
    grad1_own(1, 1)
    sum1.append(finish(1))
    sum2.done()
    for h in range(2):
        dw2t_ref[:, h * 256:(h + 1) * 256] = tot2[h, :OUT, :]
    db2_ref[...] = tot2[0, 112:113, :OUT]
    sum1[1].across()
    dxt_ref[...] = dot_nt(w1_ref[...], dz1_s[...])
    sum1[0].back()
    sum1[0].done()

    def put(h):
        for i in range(2):
            at = slice(h * 256 + i * 128, h * 256 + (i + 1) * 128)
            dw1_ref[:, at] = tot1[h, i, :FIN, :]
            db1_ref[:, at] = tot1[h, i, FIN:FIN + 1, :]

    put(0)
    sum1[1].back()
    sum1[1].done()
    put(1)


def step(*operands):
    vmem = pl.BlockSpec(memory_space=pltpu.VMEM)
    out = lambda *shape: jax.ShapeDtypeStruct(shape, F32)
    f32 = lambda *shape: pltpu.VMEM(shape, F32)
    b16 = lambda *shape: pltpu.VMEM(shape, BF16)
    return pl.pallas_call(
        step_kernel,
        out_shape=(out(FIN, NODES), out(FIN, HID), out(OUT, HID), out(1, HID), out(1, OUT)),
        in_specs=[vmem] * 11,
        out_specs=(vmem,) * 5,
        scratch_shapes=[
            b16(4, SEND, FIN), b16(NODES, HALO), b16(4, SEND + HUBS, 256), b16(4, SEND + HUBS, 256), f32(4, 32, 128), f32(4, 32, 128),
            b16(HID, NODES + HALO), f32(HID, NODES), b16(NODES, 384), b16(128, 128), f32(NODES, 128), f32(HALO + HUBS, 128),
            f32(4, SEND + HUBS, 128), f32(4, SEND + HUBS, 128), f32(HUBS, HID), f32(4, HUBS, HID),
            b16(3, NODES, HID), b16(128, HID), f32(NODES, HID), f32(2, 4, SEND + HUBS, 256), f32(2, 4, SEND + HUBS, 256), b16(NODES, HID),
            b16(3 * HUBS, NODES), b16(HID, 3 * HUBS), b16(HID, NODES), f32(HID, NODES), b16(NODES, 128),
            f32(2, 120, 256), f32(120, 256), f32(2, 120, 256), f32(2, 120, 256),
            f32(2, 2, 208, 128), f32(2, 208, 128), f32(2, 2, 208, 128), f32(2, 2, 208, 128),
            pltpu.SemaphoreType.DMA((28,)), pltpu.SemaphoreType.DMA((28,)),
        ],
        compiler_params=pltpu.CompilerParams(collective_id=0, has_side_effects=True, vmem_limit_bytes=STEP_VMEM),
        name="step",
    )(*operands)


def emit_kernel(*refs):
    ins, outs, sem = refs[:5], refs[5:10], refs[10]
    copies = [pltpu.make_async_copy(a, b, sem.at[i]) for i, (a, b) in enumerate(zip(ins, outs))]
    for copy in copies:
        copy.start()
    for copy in copies:
        copy.wait()


def emit(*arrays):
    return pl.pallas_call(
        emit_kernel,
        out_shape=tuple(jax.ShapeDtypeStruct(a.shape, a.dtype) for a in arrays),
        in_specs=[pl.BlockSpec(memory_space=pltpu.VMEM)] * 5,
        out_specs=(pl.BlockSpec(memory_space=pltpu.HBM),) * 5,
        scratch_shapes=[pltpu.SemaphoreType.DMA((5,))],
        compiler_params=pltpu.CompilerParams(vmem_limit_bytes=4 << 20),
        name="emit",
    )(*arrays)


def solution(mesh):
    vertex_spec = P(("data", "graph"))
    vertex_rows = P(("data", "graph"), None)
    part_spec = P("data")
    part_rows = P("data", None)
    replicated = P()

    def device_step(x, dst, src, w, send, hub_ids, w_first, b_first, w_second, dy_out):
        dx, dw1, dw2, db1, db2 = emit(*step(*build(
            hub_ids, dst, src, w,
            x.T, w_first, b_first.reshape(1, HID), w_second.T, dy_out.T, send.reshape(1, HALO), hub_ids.reshape(1, HUBS))))
        return dx.T, dw1, dw2.T, db1.reshape(HID), db2.reshape(OUT)

    return jax.shard_map(
        device_step,
        mesh=mesh,
        in_specs=(vertex_rows, vertex_spec, vertex_spec, vertex_spec, vertex_spec, part_spec, replicated, replicated, replicated, vertex_rows),
        out_specs=(vertex_rows, part_rows, part_rows, part_spec, part_spec),
        check_vma=False,
    )
```

```python
import functools

import jax
import jax.numpy as jnp
from jax import lax
from jax.experimental import pallas as pl
from jax.experimental.pallas import tpu as pltpu
from jax.sharding import PartitionSpec as P

F32, BF16 = jnp.float32, jnp.bfloat16
NODES, SEND, HALO, HUBS = 1024, 64, 256, 16
TABLE = NODES + HALO + HUBS
TILES = 9
COLS = TILES * 128
ROWS = TILES * TABLE
EDGES = 16384
HID, OUT, FIN = 512, 107, 200

ACCS = 4
GROUP = 4
BUILD_VMEM = 28 << 20
STEP_VMEM = 34 << 20
NT = (((1,), (1,)), ((), ()))


def split3(x):
    hi = x.astype(BF16)
    rest = x - hi.astype(F32)
    mid = rest.astype(BF16)
    return hi, mid, (rest - mid.astype(F32)).astype(BF16)


def in_hbm(a):
    return pltpu.with_memory_space_constraint(a, pltpu.HBM)


def dot(a, b):
    return jnp.dot(a, b, preferred_element_type=F32)


def dot_nt(a, b):
    return lax.dot_general(a, b, NT, preferred_element_type=F32)


def build_kernel(hub_hbm, dst_hbm, src_hbm, w_hbm, *refs):
    staged_in, refs = refs[:7], refs[7:]
    hi_ref, mid_ref, lo_ref, side_ref = refs[:4]
    staged_out, refs = refs[4:11], refs[11:]
    (hub_ref, dst_ref, src_ref, w_ref, row_ref, lane_ref, perm_ref, val_a, val_b, sem, stage_sem), rest = refs[:11], refs[11:]
    row_smem, accs = rest[:8], rest[8:]
    loads = []
    for i, (a, b) in enumerate(((hub_hbm, hub_ref), (dst_hbm, dst_ref), (src_hbm, src_ref), (w_hbm, w_ref))):
        loads.append(pltpu.make_async_copy(a, b, sem.at[8 + i]))
        loads[-1].start()
    stages = [pltpu.make_async_copy(a, b, stage_sem.at[i]) for i, (a, b) in enumerate(zip(staged_in, staged_out))]

    def clear(some):
        def zero(i, carry):
            for acc in some:
                acc[pl.ds(pl.multiple_of(i * 48, 8), 48), :] = jnp.zeros((48, 128), F32)
            return carry

        lax.fori_loop(0, ROWS // 48, zero, 0)

    clear(accs[:2])
    for load in loads:
        load.wait()
    base = lax.axis_index("graph") * NODES
    dst, src = dst_ref[...], src_ref[...]
    new_dst, new_src = dst, src
    for k in range(HUBS):
        local = hub_ref[k] - base
        local = jnp.where((local >= 0) & (local < NODES), local, -1)
        new_dst = jnp.where(dst == local, NODES + k, new_dst)
        new_src = jnp.where(src == local, NODES + HALO + k, new_src)
    row_ref[...] = (new_dst >> 7) * TABLE + new_src
    lane_ref[...] = new_dst & 127
    copies = []
    for s in range(8):
        perm_ref[s] = row_ref[pl.ds(s, 16, stride=8), :]
    for s in range(8):
        copies.append(pltpu.make_async_copy(perm_ref.at[s], row_smem[s], sem.at[s]))
        copies[-1].start()
    for stage in stages:
        stage.start()
    clear(accs[2:])

    iota = lax.broadcasted_iota(jnp.int32, (8, 128), 1)

    def wide(block, c):
        return jnp.broadcast_to(block[:, c:c + 1], (8, 128))

    def prep(g, val_ref):
        at = pl.ds(pl.multiple_of(g * 8, 8), 8)
        lanes, weights, rows = lane_ref[at, :], w_ref[at, :], row_ref[at, :]
        place = lax.broadcasted_iota(jnp.int32, (8, 128), 1) % GROUP
        terms = [(lanes, weights)]
        for d in range(1, GROUP):
            same = (place >= d) & (rows == pltpu.roll(rows, d, 1))
            terms.append((pltpu.roll(lanes, d, 1), jnp.where(same, pltpu.roll(weights, d, 1), 0.0)))
        def one(s):
            total = None
            for lane, weight in terms:
                hit = jnp.broadcast_to(lane[s:s + 1, :], (128, 128)) == sub
                part = jnp.where(hit, jnp.broadcast_to(weight[s:s + 1, :], (128, 128)), 0.0)
                total = part if total is None else total + part
            val_ref[s * 128:(s + 1) * 128, :] = jnp.transpose(total)

        return one

    def scatter(g, val_ref, c):
        for s in range(8):
            acc = accs[s % ACCS]
            rows = [row_smem[s][g, c + i] for i in range(GROUP)]
            sums = [acc[pl.ds(rows[i], 1), :] + val_ref[s * 128 + c + i:s * 128 + c + i + 1, :] for i in range(GROUP)]
            for r, total in zip(rows, sums):
                acc[pl.ds(r, 1), :] = total

    def both(g, val_ref, next_g, next_ref):
        one = prep(next_g, next_ref)
        for c in range(0, 128, GROUP):
            if c % 16 == 0:
                one(c // 16)
            scatter(g, val_ref, c)

    sub = lax.broadcasted_iota(jnp.int32, (128, 128), 0)
    first = prep(0, val_a)
    for s in range(8):
        first(s)
    for copy in copies:
        copy.wait()

    def turn(h, carry):
        both(2 * h, val_a, 2 * h + 1, val_b)
        both(2 * h + 1, val_b, jnp.minimum(2 * h + 2, 15), val_a)
        return carry

    lax.fori_loop(0, 8, turn, 0)

    def finish(i, carry):
        at = pl.multiple_of(i * 16, 16)
        for t in range(TILES):
            part = pl.ds(pl.multiple_of(t * TABLE + i * 16, 8), 16)
            total = accs[0][part, :]
            for acc in accs[1:]:
                total = total + acc[part, :]
            parts = split3(total)
            if t < TILES - 1:
                for piece, ref in zip(parts, (hi_ref, mid_ref, lo_ref)):
                    ref[pl.ds(at, 16), t * 128:(t + 1) * 128] = piece
            else:
                side = parts[0].astype(F32)
                for i, j in enumerate((1, 2, 0, 1, 0)):
                    side = side + pltpu.roll(parts[j].astype(F32), (i + 1) * HUBS, 1)
                side_ref[pl.ds(at, 16), :] = side.astype(BF16)
        return carry

    lax.fori_loop(0, TABLE // 16, finish, 0)
    for stage in stages:
        stage.wait()


def build(hub_ids, dst, src, w, *staged):
    piece = jax.ShapeDtypeStruct((TABLE, NODES), BF16)
    side = jax.ShapeDtypeStruct((TABLE, 128), BF16)
    square = lambda a: a.reshape(128, 128)
    table = pltpu.VMEM((128, 128), jnp.int32)
    return pl.pallas_call(
        build_kernel,
        out_shape=(piece, piece, piece, side) + tuple(jax.ShapeDtypeStruct(a.shape, a.dtype) for a in staged),
        in_specs=[pl.BlockSpec(memory_space=pltpu.HBM)] * 11,
        out_specs=(pl.BlockSpec(memory_space=pltpu.VMEM),) * 11,
        scratch_shapes=[
            pltpu.SMEM((HUBS,), jnp.int32), table, table, pltpu.VMEM((128, 128), F32), table, table,
            pltpu.VMEM((8, 16, 128), jnp.int32), pltpu.VMEM((1024, 128), F32), pltpu.VMEM((1024, 128), F32),
            pltpu.SemaphoreType.DMA((12,)), pltpu.SemaphoreType.DMA((7,)),
        ] + [pltpu.SMEM((16, 128), jnp.int32)] * 8 + [pltpu.VMEM((ROWS, 128), F32)] * ACCS,
        compiler_params=pltpu.CompilerParams(vmem_limit_bytes=BUILD_VMEM),
        name="build",
    )(*(in_hbm(a) for a in (hub_ids, square(dst), square(src), square(w)) + staged))


def step_kernel(
    hi_ref, mid_ref, lo_ref, side_ref, xt_ref, w1_ref, b1_ref, w2t_ref, dht_ref, send_ref, hub_ref,
    dxt_ref, dw1_ref, dw2t_ref, db1_ref, db2_ref,
    sent_s, pt_s, xs, xr, hs, hr, z_s, yt_s, d2_s, dhub_s, g2_s, g2h_s, rb, sb, ys, yr, dy_s, dyh_s, g1_s, sd, rd, dz1_s,
    hub_out, hub_in, hub_chip, hub3_s, y_cols_s, hid_s, live_s, dz2_s,
    a2, half2, got2, tot2, a1, half1, got1, tot1, send_sem, recv_sem,
):
    me = lax.axis_index("graph")
    sibling = me + 1 - 2 * lax.rem(me, 2)
    across = lax.rem(me + 2, 4)
    core = lax.rem(me, 2)
    mesh_id = pl.DeviceIdType.MESH
    peers = [lax.rem(me + d, 4) for d in (1, 2, 3)]
    barrier = pltpu.get_barrier_semaphore()
    for q in peers:
        pl.semaphore_signal(barrier, inc=1, device_id={"graph": q}, device_id_type=mesh_id)
    used = [0]

    def remote(src, dst, q):
        i = used[0]
        used[0] += 1
        copy = pltpu.make_async_remote_copy(
            src_ref=src, dst_ref=dst, send_sem=send_sem.at[i], recv_sem=recv_sem.at[i],
            device_id={"graph": q}, device_id_type=mesh_id)
        copy.start()
        return copy

    def wait_all(copies):
        for copy in copies:
            copy.wait()

    pieces = (hi_ref, mid_ref, lo_ref)
    hub_local = hub_ref[...] - me * NODES
    hub_row = jnp.where((hub_local >= 0) & (hub_local < NODES), hub_local, -1).astype(F32)
    hub_block = jnp.concatenate([hub_row, jnp.full((1, SEND - HUBS), -1.0, F32)], axis=1)
    send_row = send_ref[...].astype(F32)
    row = jnp.concatenate([jnp.where(me == q, hub_block, send_row[:, q * SEND:(q + 1) * SEND]) for q in range(4)], axis=1)
    row3 = jnp.concatenate([hub_row] * 3 + [jnp.full((1, 128 - 3 * HUBS), -1.0, F32)], axis=1)
    column = jnp.transpose(jnp.broadcast_to(jnp.concatenate([row, row3], axis=1), (128, 384)))
    lane = lax.broadcasted_iota(jnp.int32, (HALO + 3 * HUBS, 128), 1).astype(F32)
    picks = jnp.concatenate(
        [jnp.where(column[:HALO + 3 * HUBS] == lane + float(j * 128), 1.0, 0.0).astype(BF16) for j in range(8)], axis=1)
    xt = xt_ref[...]
    sent_s[...] = dot_nt(picks[:HALO], xt).astype(BF16).reshape(4, SEND, FIN)
    hub_col = column[HALO:HALO + HUBS]
    alias = [jnp.where((hub_col == row[:, j * 128:(j + 1) * 128]) & (hub_col >= 0.0), 1.0, 0.0) for j in range(2)]
    dht = dht_ref[...]
    dh = jnp.transpose(jnp.concatenate([dht, jnp.zeros((128 - OUT, NODES), F32)], axis=0))
    for j, piece in enumerate(split3(dh)):
        d2_s[:, j * 128:(j + 1) * 128] = piece
    hub_dh = dot(picks[HALO:HALO + HUBS], d2_s[...])
    hub_dh = (hub_dh[:, :128] + hub_dh[:, 128:256]) + hub_dh[:, 256:]
    for q in range(4):
        hs[q, :HUBS, :] = hub_dh
        part = alias[q // 2][:, (q % 2) * SEND:(q % 2 + 1) * SEND]
        hs[q, HUBS:, :] = jnp.concatenate([part, jnp.zeros((HUBS, 128 - SEND), F32)], axis=1)
    hr[me, :HUBS, :] = hub_dh
    hr[me, HUBS:, :] = jnp.zeros((HUBS, 128), F32)
    own_hub_x = sent_s[me, :HUBS, :]
    xs[:, :, FIN:] = jnp.zeros((4, SEND + HUBS, 256 - FIN), BF16)
    for q in range(4):
        xs[q, :SEND, :FIN] = sent_s[q]
        xs[q, SEND:, :FIN] = own_hub_x
    xr[me] = jnp.zeros((SEND + HUBS, 256), BF16)
    pl.semaphore_wait(barrier, 3)
    round_a = [remote(hs.at[q], hr.at[me], q) for q in peers]
    round_x = [remote(xs.at[q], xr.at[me], q) for q in peers]
    db2 = jnp.sum(dh, axis=0, keepdims=True)
    sub = lax.broadcasted_iota(jnp.int32, (NODES, HALO), 0).astype(F32)
    pt_s[...] = jnp.where(sub == row, 1.0, 0.0).astype(BF16)
    hub3_s[...] = picks[HALO:]

    def grad2(rows):
        a = dot(hi_ref[rows, :], d2_s[:, :256])
        b = dot(mid_ref[rows, :], d2_s[:, :256])
        c = dot(hi_ref[rows, :], d2_s[:, 256:]) + dot(lo_ref[rows, :], d2_s[:, :128])
        return ((c + b[:, 128:]) + (a[:, 128:] + b[:, :128])) + a[:, :128]

    def over_blocks(body, carry=0, first=0, last=4):
        def turn(n, carry):
            return body(pl.ds(pl.multiple_of(n * 256, 256), 256), carry)

        return lax.fori_loop(first, last, turn, carry)

    def grad2_own(at, carry):
        g2_s[at, :] = grad2(at)
        return carry

    over_blocks(grad2_own)
    far_rows = pl.ds(NODES, HALO + HUBS)
    g2h_s[...] = grad2(far_rows)
    wait_all(round_a)

    def side_by_side(x):
        hi, mid, lo = split3(x)
        return jnp.concatenate([hi, hi, hi, mid, mid, lo, jnp.zeros((32, x.shape[1]), BF16)], axis=0)

    dhub_s[...] = side_by_side((hr[0, :HUBS] + hr[1, :HUBS]) + (hr[2, :HUBS] + hr[3, :HUBS]))
    g2h_s[...] += dot(side_ref[far_rows, :], dhub_s[...])
    far = g2h_s[:HALO, :]
    alias_row = jnp.concatenate([hr[q, HUBS:, :SEND] for q in range(4)], axis=1)
    hub_g2 = g2h_s[HALO:, :]
    for piece in split3(far):
        hub_g2 = hub_g2 + dot(alias_row.astype(BF16), piece)
    is_alias = dot(jnp.transpose(jnp.concatenate([alias_row, jnp.zeros((112, HALO), F32)], axis=0)).astype(BF16),
                   jnp.ones((128, 128), BF16))
    far = jnp.where(is_alias > 0.5, 0.0, far)
    for q in range(4):
        sb[q, :SEND, :] = far[q * SEND:(q + 1) * SEND]
        sb[q, SEND:, :] = hub_g2
    rb[me] = sb[me]
    round_b = [remote(sb.at[q], rb.at[me], q) for q in peers]

    w1t = jnp.transpose(jnp.concatenate([w1_ref[...], jnp.zeros((56, HID), BF16)], axis=0).astype(F32)).astype(BF16)[:, :FIN]
    z_s[:, :NODES] = dot(w1t, xt).astype(BF16)

    def forward_own(at, carry):
        z = z_s[:, :NODES]
        acc = dot(z, hi_ref[:NODES, at])
        acc = acc + dot(z, mid_ref[:NODES, at])
        yt_s[:, at] = acc + dot(z, lo_ref[:NODES, at])
        return carry

    over_blocks(forward_own, 0, 0, 2)
    y_side = dot(z_s[:, :NODES], side_ref[:NODES, :])
    wait_all(round_x)

    halo_x = jnp.concatenate([xr[q, :SEND, :FIN] for q in range(4)], axis=0)
    hub_x = own_hub_x.astype(F32)
    for q in range(4):
        hub_x = hub_x + xr[q, SEND:, :FIN].astype(F32)
    z_s[:, NODES:] = dot_nt(w1t, halo_x).astype(BF16)
    z_hub = dot_nt(w1t, jnp.concatenate([hub_x.astype(BF16)] * 3, axis=0)).astype(BF16)
    y_side = y_side + dot(z_s[:, NODES:], side_ref[NODES:NODES + HALO, :])
    y_side = jnp.transpose(y_side + dot(z_hub[:, :HUBS], side_ref[NODES + HALO:, :]))
    ys[...] = (y_side[:HUBS] + y_side[HUBS:2 * HUBS]) + y_side[2 * HUBS:3 * HUBS]
    yr[me] = ys[...]
    round_y = [remote(ys, yr.at[me], q) for q in peers]

    over_blocks(forward_own, 0, 2, 4)

    def forward_far(at, carry):
        z = z_s[:, NODES:]
        acc = yt_s[:, at]
        for ref in pieces:
            acc = acc + dot(z, ref[NODES:NODES + HALO, at])
        hub_rows = jnp.concatenate([ref[NODES + HALO:, at] for ref in pieces], axis=0)
        yt_s[:, at] = acc + dot(z_hub, hub_rows)
        g2_s[at, :] += dot(side_ref[at, :], dhub_s[...])
        return carry

    over_blocks(forward_far)
    wait_all(round_b)

    def returned(ref, hub_sum):
        ref[me, :HUBS, :] = hub_sum
        ref[me, HUBS:SEND, :] = jnp.zeros((SEND - HUBS, hub_sum.shape[1]), F32)
        return ref[:, :SEND, :].reshape(HALO, hub_sum.shape[1])

    hub_sum = (rb[0, SEND:, :] + rb[1, SEND:, :]) + (rb[2, SEND:, :] + rb[3, SEND:, :])
    back = returned(rb, hub_sum)
    hub_dz2 = hub_sum.astype(BF16)
    back_parts = split3(back)

    def dz2_block(at, carry):
        own = g2_s[at, :]
        for piece in back_parts:
            own = own + dot(pt_s[at, :], piece)
        dz2_s[at, :] = own.astype(BF16)
        return carry

    over_blocks(dz2_block)

    wait_all(round_y)
    y_hub = (yr[0] + yr[1]) + (yr[2] + yr[3])
    b1 = b1_ref[...]
    b1_col = jnp.transpose(jnp.broadcast_to(b1, (128, HID)))
    y_rows = jnp.concatenate([piece.astype(F32) for piece in split3(y_hub)] + [jnp.zeros((128 - 3 * HUBS, HID), F32)], axis=0)
    y_cols_s[...] = jnp.transpose(y_rows).astype(BF16)[:, :3 * HUBS]

    def pre_block(at, carry):
        pre = (yt_s[:, at] + dot(y_cols_s[...], hub3_s[:, at])) + jnp.concatenate([b1_col] * 2, axis=1)
        hid_s[:, at] = jnp.maximum(pre, 0.0).astype(BF16)
        live_s[:, at] = jnp.where(pre > 0.0, 1.0, 0.0)
        return carry

    over_blocks(pre_block)

    class GroupSum:
        def __init__(self, own, half, got, total):
            self.own, self.half, self.got, self.total = own, half, got, total
            self.copy = remote(own.at[1 - core], got.at[0], sibling)

        def across(self):
            self.copy.wait()
            self.half[...] = self.own[core] + self.got[0]
            self.copy = remote(self.half, self.got.at[1], across)

        def back(self):
            self.copy.wait()
            self.total[core] = self.half[...] + self.got[1]
            self.copy = remote(self.total.at[core], self.total.at[core], sibling)

        def done(self):
            self.copy.wait()

    dw2t = jnp.transpose(dot(hid_s[...], dz2_s[...]))
    for h in range(2):
        a2[h] = dw2t[:112, h * 256:(h + 1) * 256]
        a2[h, OUT:OUT + 1, :128] = db2
    sum2 = GroupSum(a2, half2, got2, tot2)

    def dy_block(at, db1):
        live = jnp.transpose(live_s[:, at])
        dy = jnp.where(live > 0.5, dot(dz2_s[at, :OUT], w2t_ref[...]), 0.0)
        for j, piece in enumerate(split3(dy)):
            dy_s[j, at, :] = piece
        return db1 + jnp.sum(dy, axis=0, keepdims=True)

    db1 = over_blocks(dy_block, jnp.zeros((1, HID), F32))
    hub_dy = jnp.where(y_hub + b1 > 0.0, dot(hub_dz2[:, :OUT], w2t_ref[...]), 0.0)
    dyh_s[...] = side_by_side(hub_dy)
    sum2.across()

    def grad1(rows, cols):
        acc = dot(lo_ref[rows, :], dy_s[0, :, cols])
        acc = acc + dot(mid_ref[rows, :], dy_s[1, :, cols])
        acc = acc + dot(hi_ref[rows, :], dy_s[2, :, cols])
        acc = acc + dot(mid_ref[rows, :], dy_s[0, :, cols])
        acc = acc + dot(hi_ref[rows, :], dy_s[1, :, cols])
        acc = acc + dot(hi_ref[rows, :], dy_s[0, :, cols])
        return acc + dot(side_ref[rows, :], dyh_s[:, cols])

    halves = (pl.ds(0, 256), pl.ds(256, 256))
    round_d, hub_copy = [], []
    for h, cols in enumerate(halves):
        ret = grad1(far_rows, cols)
        for q in range(4):
            sd[h, q] = ret[q * SEND:(q + 1) * SEND]
        hub_out[h] = ret[HALO:]
        hub_copy.append(remote(hub_out.at[h], hub_in.at[h, 0], sibling))
        round_d.append([remote(sd.at[h, q], rd.at[h, me], q) for q in peers])

    def hub_across(h):
        hub_copy[h].wait()
        hub_chip[h] = hub_out[h] + hub_in[h, 0]
        hub_copy[h] = remote(hub_chip.at[h], hub_in.at[h, 1], across)

    hub_across(0)

    def grad1_own(h, m):
        rows = pl.ds(m * 512, 512)
        g1_s[rows, halves[h]] = grad1(rows, halves[h])

    def finish(h):
        wait_all(round_d[h])
        cols = halves[h]
        hub_copy[h].wait()
        back = returned(rd.at[h], hub_chip[h] + hub_in[h, 1])
        dz1 = g1_s[:, cols]
        for piece in split3(back):
            dz1 = dz1 + dot(pt_s[...], piece)
        dz1 = dz1.astype(BF16)
        dz1_s[:, cols] = dz1
        dw1 = dot(xt_ref[...], dz1)
        for i in range(2):
            at = slice(i * 128, (i + 1) * 128)
            a1[h, i, :FIN, :] = dw1[:, at]
            a1[h, i, FIN:, :] = jnp.broadcast_to(db1[:, h * 256 + i * 128:h * 256 + (i + 1) * 128], (8, 128))
        return GroupSum(a1.at[h], half1.at[h], got1.at[h], tot1.at[h])

    grad1_own(0, 0)
    hub_across(1)
    grad1_own(0, 1)
    sum1 = [finish(0)]
    sum2.back()
    grad1_own(1, 0)
    sum1[0].across()
    grad1_own(1, 1)
    sum1.append(finish(1))
    sum2.done()
    for h in range(2):
        dw2t_ref[:, h * 256:(h + 1) * 256] = tot2[h, :OUT, :]
    db2_ref[...] = tot2[0, OUT:OUT + 1, :OUT]
    sum1[1].across()
    dxt_ref[...] = dot_nt(w1_ref[...], dz1_s[...])
    sum1[0].back()
    sum1[0].done()

    def put(h):
        for i in range(2):
            at = slice(h * 256 + i * 128, h * 256 + (i + 1) * 128)
            dw1_ref[:, at] = tot1[h, i, :FIN, :]
            db1_ref[:, at] = tot1[h, i, FIN:FIN + 1, :]

    put(0)
    sum1[1].back()
    sum1[1].done()
    put(1)


def step(*operands):
    vmem = pl.BlockSpec(memory_space=pltpu.VMEM)
    out = lambda *shape: jax.ShapeDtypeStruct(shape, F32)
    f32 = lambda *shape: pltpu.VMEM(shape, F32)
    b16 = lambda *shape: pltpu.VMEM(shape, BF16)
    return pl.pallas_call(
        step_kernel,
        out_shape=(out(FIN, NODES), out(FIN, HID), out(OUT, HID), out(1, HID), out(1, OUT)),
        in_specs=[vmem] * 11,
        out_specs=(vmem,) * 5,
        scratch_shapes=[
            b16(4, SEND, FIN), b16(NODES, HALO), b16(4, SEND + HUBS, 256), b16(4, SEND + HUBS, 256), f32(4, 32, 128), f32(4, 32, 128),
            b16(HID, NODES + HALO), f32(HID, NODES), b16(NODES, 384), b16(128, 128), f32(NODES, 128), f32(HALO + HUBS, 128),
            f32(4, SEND + HUBS, 128), f32(4, SEND + HUBS, 128), f32(HUBS, HID), f32(4, HUBS, HID),
            b16(3, NODES, HID), b16(128, HID), f32(NODES, HID), f32(2, 4, SEND, 256), f32(2, 4, SEND, 256), b16(NODES, HID),
            f32(2, HUBS, 256), f32(2, 2, HUBS, 256), f32(2, HUBS, 256),
            b16(3 * HUBS, NODES), b16(HID, 3 * HUBS), b16(HID, NODES), f32(HID, NODES), b16(NODES, 128),
            f32(2, 112, 256), f32(112, 256), f32(2, 112, 256), f32(2, 112, 256),
            f32(2, 2, 208, 128), f32(2, 208, 128), f32(2, 2, 208, 128), f32(2, 2, 208, 128),
            pltpu.SemaphoreType.DMA((32,)), pltpu.SemaphoreType.DMA((32,)),
        ],
        compiler_params=pltpu.CompilerParams(collective_id=0, has_side_effects=True, vmem_limit_bytes=STEP_VMEM),
        name="step",
    )(*operands)


def emit_kernel(*refs):
    ins, outs, sem = refs[:5], refs[5:10], refs[10]
    copies = [pltpu.make_async_copy(a, b, sem.at[i]) for i, (a, b) in enumerate(zip(ins, outs))]
    for copy in copies:
        copy.start()
    for copy in copies:
        copy.wait()


def emit(*arrays):
    return pl.pallas_call(
        emit_kernel,
        out_shape=tuple(jax.ShapeDtypeStruct(a.shape, a.dtype) for a in arrays),
        in_specs=[pl.BlockSpec(memory_space=pltpu.VMEM)] * 5,
        out_specs=(pl.BlockSpec(memory_space=pltpu.HBM),) * 5,
        scratch_shapes=[pltpu.SemaphoreType.DMA((5,))],
        compiler_params=pltpu.CompilerParams(vmem_limit_bytes=4 << 20),
        name="emit",
    )(*arrays)


def solution(mesh):
    vertex_spec = P(("data", "graph"))
    vertex_rows = P(("data", "graph"), None)
    part_spec = P("data")
    part_rows = P("data", None)
    replicated = P()

    def device_step(x, dst, src, w, send, hub_ids, w_first, b_first, w_second, dy_out):
        dx, dw1, dw2, db1, db2 = emit(*step(*build(
            hub_ids, dst, src, w,
            x.T, w_first, b_first.reshape(1, HID), w_second.T, dy_out.T, send.reshape(1, HALO), hub_ids.reshape(1, HUBS))))
        return dx.T, dw1, dw2.T, db1.reshape(HID), db2.reshape(OUT)

    return jax.shard_map(
        device_step,
        mesh=mesh,
        in_specs=(vertex_rows, vertex_spec, vertex_spec, vertex_spec, vertex_spec, part_spec, replicated, replicated, replicated, vertex_rows),
        out_specs=(vertex_rows, part_rows, part_rows, part_spec, part_spec),
        check_vma=False,
    )
```

```python
import functools

import jax
import jax.numpy as jnp
from jax import lax
from jax.experimental import pallas as pl
from jax.experimental.pallas import tpu as pltpu
from jax.sharding import PartitionSpec as P

F32, BF16 = jnp.float32, jnp.bfloat16
NODES, SEND, HALO, HUBS = 1024, 64, 256, 16
TABLE = NODES + HALO + HUBS
TILES = 9
COLS = TILES * 128
ROWS = TILES * TABLE
EDGES = 16384
HID, OUT, FIN = 512, 107, 200

ACCS = 4
GROUP = 4
BUILD_VMEM = 28 << 20
STEP_VMEM = 34 << 20
NT = (((1,), (1,)), ((), ()))


def split3(x):
    hi = x.astype(BF16)
    rest = x - hi.astype(F32)
    mid = rest.astype(BF16)
    return hi, mid, (rest - mid.astype(F32)).astype(BF16)


def in_hbm(a):
    return pltpu.with_memory_space_constraint(a, pltpu.HBM)


def dot(a, b):
    return jnp.dot(a, b, preferred_element_type=F32)


def dot_nt(a, b):
    return lax.dot_general(a, b, NT, preferred_element_type=F32)


def build_kernel(hub_hbm, dst_hbm, src_hbm, w_hbm, *refs):
    staged_in, refs = refs[:7], refs[7:]
    hi_ref, mid_ref, lo_ref, side_ref = refs[:4]
    staged_out, refs = refs[4:11], refs[11:]
    (hub_ref, dst_ref, src_ref, w_ref, row_ref, lane_ref, perm_ref, val_a, val_b, sem, stage_sem), rest = refs[:11], refs[11:]
    row_smem, accs = rest[:8], rest[8:]
    loads = []
    for i, (a, b) in enumerate(((hub_hbm, hub_ref), (dst_hbm, dst_ref), (src_hbm, src_ref), (w_hbm, w_ref))):
        loads.append(pltpu.make_async_copy(a, b, sem.at[8 + i]))
        loads[-1].start()
    stages = [pltpu.make_async_copy(a, b, stage_sem.at[i]) for i, (a, b) in enumerate(zip(staged_in, staged_out))]

    def clear(some):
        def zero(i, carry):
            for acc in some:
                acc[pl.ds(pl.multiple_of(i * 48, 8), 48), :] = jnp.zeros((48, 128), F32)
            return carry

        lax.fori_loop(0, ROWS // 48, zero, 0)

    clear(accs[:2])
    for load in loads:
        load.wait()
    base = lax.axis_index("graph") * NODES
    dst, src = dst_ref[...], src_ref[...]
    new_dst, new_src = dst, src
    for k in range(HUBS):
        local = hub_ref[k] - base
        local = jnp.where((local >= 0) & (local < NODES), local, -1)
        new_dst = jnp.where(dst == local, NODES + k, new_dst)
        new_src = jnp.where(src == local, NODES + HALO + k, new_src)
    row_ref[...] = (new_dst >> 7) * TABLE + new_src
    lane_ref[...] = new_dst & 127
    copies = []
    for s in range(8):
        perm_ref[s] = row_ref[pl.ds(s, 16, stride=8), :]
    for s in range(8):
        copies.append(pltpu.make_async_copy(perm_ref.at[s], row_smem[s], sem.at[s]))
        copies[-1].start()
    for stage in stages:
        stage.start()
    clear(accs[2:])

    iota = lax.broadcasted_iota(jnp.int32, (8, 128), 1)

    def wide(block, c):
        return jnp.broadcast_to(block[:, c:c + 1], (8, 128))

    def prep(g, val_ref):
        at = pl.ds(pl.multiple_of(g * 8, 8), 8)
        lanes, weights, rows = lane_ref[at, :], w_ref[at, :], row_ref[at, :]
        place = lax.broadcasted_iota(jnp.int32, (8, 128), 1) % GROUP
        terms = [(lanes, weights)]
        for d in range(1, GROUP):
            same = (place >= d) & (rows == pltpu.roll(rows, d, 1))
            terms.append((pltpu.roll(lanes, d, 1), jnp.where(same, pltpu.roll(weights, d, 1), 0.0)))
        def one(s):
            total = None
            for lane, weight in terms:
                hit = jnp.broadcast_to(lane[s:s + 1, :], (128, 128)) == sub
                part = jnp.where(hit, jnp.broadcast_to(weight[s:s + 1, :], (128, 128)), 0.0)
                total = part if total is None else total + part
            val_ref[s * 128:(s + 1) * 128, :] = jnp.transpose(total)

        return one

    def scatter(g, val_ref, c):
        for s in range(8):
            acc = accs[s % ACCS]
            rows = [row_smem[s][g, c + i] for i in range(GROUP)]
            sums = [acc[pl.ds(rows[i], 1), :] + val_ref[s * 128 + c + i:s * 128 + c + i + 1, :] for i in range(GROUP)]
            for r, total in zip(rows, sums):
                acc[pl.ds(r, 1), :] = total

    def both(g, val_ref, next_g, next_ref):
        one = prep(next_g, next_ref)
        for c in range(0, 128, GROUP):
            if c % 16 == 0:
                one(c // 16)
            scatter(g, val_ref, c)

    sub = lax.broadcasted_iota(jnp.int32, (128, 128), 0)
    first = prep(0, val_a)
    for s in range(8):
        first(s)
    for copy in copies:
        copy.wait()

    def turn(h, carry):
        both(2 * h, val_a, 2 * h + 1, val_b)
        both(2 * h + 1, val_b, jnp.minimum(2 * h + 2, 15), val_a)
        return carry

    lax.fori_loop(0, 8, turn, 0)

    def finish(i, carry):
        at = pl.multiple_of(i * 16, 16)
        for t in range(TILES):
            part = pl.ds(pl.multiple_of(t * TABLE + i * 16, 8), 16)
            total = accs[0][part, :]
            for acc in accs[1:]:
                total = total + acc[part, :]
            parts = split3(total)
            if t < TILES - 1:
                for piece, ref in zip(parts, (hi_ref, mid_ref, lo_ref)):
                    ref[pl.ds(at, 16), t * 128:(t + 1) * 128] = piece
            else:
                side = parts[0].astype(F32)
                for i, j in enumerate((1, 2, 0, 1, 0)):
                    side = side + pltpu.roll(parts[j].astype(F32), (i + 1) * HUBS, 1)
                side_ref[pl.ds(at, 16), :] = side.astype(BF16)
        return carry

    lax.fori_loop(0, TABLE // 16, finish, 0)
    for stage in stages:
        stage.wait()


def build(hub_ids, dst, src, w, *staged):
    piece = jax.ShapeDtypeStruct((TABLE, NODES), BF16)
    side = jax.ShapeDtypeStruct((TABLE, 128), BF16)
    square = lambda a: a.reshape(128, 128)
    table = pltpu.VMEM((128, 128), jnp.int32)
    return pl.pallas_call(
        build_kernel,
        out_shape=(piece, piece, piece, side) + tuple(jax.ShapeDtypeStruct(a.shape, a.dtype) for a in staged),
        in_specs=[pl.BlockSpec(memory_space=pltpu.HBM)] * 11,
        out_specs=(pl.BlockSpec(memory_space=pltpu.VMEM),) * 11,
        scratch_shapes=[
            pltpu.SMEM((HUBS,), jnp.int32), table, table, pltpu.VMEM((128, 128), F32), table, table,
            pltpu.VMEM((8, 16, 128), jnp.int32), pltpu.VMEM((1024, 128), F32), pltpu.VMEM((1024, 128), F32),
            pltpu.SemaphoreType.DMA((12,)), pltpu.SemaphoreType.DMA((7,)),
        ] + [pltpu.SMEM((16, 128), jnp.int32)] * 8 + [pltpu.VMEM((ROWS, 128), F32)] * ACCS,
        compiler_params=pltpu.CompilerParams(vmem_limit_bytes=BUILD_VMEM),
        name="build",
    )(*(in_hbm(a) for a in (hub_ids, square(dst), square(src), square(w)) + staged))


def step_kernel(
    hi_ref, mid_ref, lo_ref, side_ref, xt_ref, w1_ref, b1_ref, w2t_ref, dht_ref, send_ref, hub_ref,
    dxt_ref, dw1_ref, dw2t_ref, db1_ref, db2_ref,
    sent_s, pt_s, xs, xr, hs, hr, z_s, yt_s, d2_s, dhub_s, g2_s, g2h_s, rb, sb, ys, yr, dy_s, dyh_s, g1_s, sd, rd, dz1_s,
    hub3_s, y_cols_s, hid_s, live_s, dz2_s,
    a2, half2, got2, tot2, a1, half1, got1, tot1, send_sem, recv_sem,
):
    me = lax.axis_index("graph")
    sibling = me + 1 - 2 * lax.rem(me, 2)
    across = lax.rem(me + 2, 4)
    core = lax.rem(me, 2)
    mesh_id = pl.DeviceIdType.MESH
    peers = [lax.rem(me + d, 4) for d in (1, 2, 3)]
    barrier = pltpu.get_barrier_semaphore()
    for q in peers:
        pl.semaphore_signal(barrier, inc=1, device_id={"graph": q}, device_id_type=mesh_id)
    used = [0]

    def remote(src, dst, q):
        i = used[0]
        used[0] += 1
        copy = pltpu.make_async_remote_copy(
            src_ref=src, dst_ref=dst, send_sem=send_sem.at[i], recv_sem=recv_sem.at[i],
            device_id={"graph": q}, device_id_type=mesh_id)
        copy.start()
        return copy

    def wait_all(copies):
        for copy in copies:
            copy.wait()

    pieces = (hi_ref, mid_ref, lo_ref)
    hub_local = hub_ref[...] - me * NODES
    hub_row = jnp.where((hub_local >= 0) & (hub_local < NODES), hub_local, -1).astype(F32)
    hub_block = jnp.concatenate([hub_row, jnp.full((1, SEND - HUBS), -1.0, F32)], axis=1)
    send_row = send_ref[...].astype(F32)
    row = jnp.concatenate([jnp.where(me == q, hub_block, send_row[:, q * SEND:(q + 1) * SEND]) for q in range(4)], axis=1)
    row3 = jnp.concatenate([hub_row] * 3 + [jnp.full((1, 128 - 3 * HUBS), -1.0, F32)], axis=1)
    column = jnp.transpose(jnp.broadcast_to(jnp.concatenate([row, row3], axis=1), (128, 384)))
    lane = lax.broadcasted_iota(jnp.int32, (HALO + 3 * HUBS, 128), 1).astype(F32)
    picks = jnp.concatenate(
        [jnp.where(column[:HALO + 3 * HUBS] == lane + float(j * 128), 1.0, 0.0).astype(BF16) for j in range(8)], axis=1)
    xt = xt_ref[...]
    sent_s[...] = dot_nt(picks[:HALO], xt).astype(BF16).reshape(4, SEND, FIN)
    hub_col = column[HALO:HALO + HUBS]
    alias = [jnp.where((hub_col == row[:, j * 128:(j + 1) * 128]) & (hub_col >= 0.0), 1.0, 0.0) for j in range(2)]
    dht = dht_ref[...]
    dh = jnp.transpose(jnp.concatenate([dht, jnp.zeros((128 - OUT, NODES), F32)], axis=0))
    for j, piece in enumerate(split3(dh)):
        d2_s[:, j * 128:(j + 1) * 128] = piece
    hub_dh = dot(picks[HALO:HALO + HUBS], d2_s[...])
    hub_dh = (hub_dh[:, :128] + hub_dh[:, 128:256]) + hub_dh[:, 256:]
    for q in range(4):
        hs[q, :HUBS, :] = hub_dh
        part = alias[q // 2][:, (q % 2) * SEND:(q % 2 + 1) * SEND]
        hs[q, HUBS:, :] = jnp.concatenate([part, jnp.zeros((HUBS, 128 - SEND), F32)], axis=1)
    hr[me, :HUBS, :] = hub_dh
    hr[me, HUBS:, :] = jnp.zeros((HUBS, 128), F32)
    own_hub_x = sent_s[me, :HUBS, :]
    xs[:, :, FIN:] = jnp.zeros((4, SEND + HUBS, 256 - FIN), BF16)
    for q in range(4):
        xs[q, :SEND, :FIN] = sent_s[q]
        xs[q, SEND:, :FIN] = own_hub_x
    xr[me] = jnp.zeros((SEND + HUBS, 256), BF16)
    pl.semaphore_wait(barrier, 3)
    round_a = [remote(hs.at[q], hr.at[me], q) for q in peers]
    round_x = [remote(xs.at[q], xr.at[me], q) for q in peers]
    db2 = jnp.sum(dh, axis=0, keepdims=True)
    sub = lax.broadcasted_iota(jnp.int32, (NODES, HALO), 0).astype(F32)
    pt_s[...] = jnp.where(sub == row, 1.0, 0.0).astype(BF16)
    hub3_s[...] = picks[HALO:]

    def grad2(rows):
        a = dot(hi_ref[rows, :], d2_s[:, :256])
        b = dot(mid_ref[rows, :], d2_s[:, :256])
        c = dot(hi_ref[rows, :], d2_s[:, 256:]) + dot(lo_ref[rows, :], d2_s[:, :128])
        return ((c + b[:, 128:]) + (a[:, 128:] + b[:, :128])) + a[:, :128]

    def over_blocks(body, carry=0, first=0, last=4):
        def turn(n, carry):
            return body(pl.ds(pl.multiple_of(n * 256, 256), 256), carry)

        return lax.fori_loop(first, last, turn, carry)

    def grad2_own(at, carry):
        g2_s[at, :] = grad2(at)
        return carry

    over_blocks(grad2_own)
    far_rows = pl.ds(NODES, HALO + HUBS)
    g2h_s[...] = grad2(far_rows)
    wait_all(round_a)

    def side_by_side(x):
        hi, mid, lo = split3(x)
        return jnp.concatenate([hi, hi, hi, mid, mid, lo, jnp.zeros((32, x.shape[1]), BF16)], axis=0)

    dhub_s[...] = side_by_side((hr[0, :HUBS] + hr[1, :HUBS]) + (hr[2, :HUBS] + hr[3, :HUBS]))
    g2h_s[...] += dot(side_ref[far_rows, :], dhub_s[...])
    far = g2h_s[:HALO, :]
    alias_row = jnp.concatenate([hr[q, HUBS:, :SEND] for q in range(4)], axis=1)
    hub_g2 = g2h_s[HALO:, :]
    for piece in split3(far):
        hub_g2 = hub_g2 + dot(alias_row.astype(BF16), piece)
    is_alias = dot(jnp.transpose(jnp.concatenate([alias_row, jnp.zeros((112, HALO), F32)], axis=0)).astype(BF16),
                   jnp.ones((128, 128), BF16))
    far = jnp.where(is_alias > 0.5, 0.0, far)
    for q in range(4):
        sb[q, :SEND, :] = far[q * SEND:(q + 1) * SEND]
        sb[q, SEND:, :] = hub_g2
    rb[me] = sb[me]
    round_b = [remote(sb.at[q], rb.at[me], q) for q in peers]

    w1t = jnp.transpose(jnp.concatenate([w1_ref[...], jnp.zeros((56, HID), BF16)], axis=0).astype(F32)).astype(BF16)[:, :FIN]
    z_s[:, :NODES] = dot(w1t, xt).astype(BF16)

    def forward_own(at, carry):
        z = z_s[:, :NODES]
        acc = dot(z, hi_ref[:NODES, at])
        acc = acc + dot(z, mid_ref[:NODES, at])
        yt_s[:, at] = acc + dot(z, lo_ref[:NODES, at])
        return carry

    over_blocks(forward_own, 0, 0, 2)
    y_side = dot(z_s[:, :NODES], side_ref[:NODES, :])
    wait_all(round_x)

    halo_x = jnp.concatenate([xr[q, :SEND, :FIN] for q in range(4)], axis=0)
    hub_x = own_hub_x.astype(F32)
    for q in range(4):
        hub_x = hub_x + xr[q, SEND:, :FIN].astype(F32)
    z_s[:, NODES:] = dot_nt(w1t, halo_x).astype(BF16)
    z_hub = dot_nt(w1t, jnp.concatenate([hub_x.astype(BF16)] * 3, axis=0)).astype(BF16)
    y_side = y_side + dot(z_s[:, NODES:], side_ref[NODES:NODES + HALO, :])
    y_side = jnp.transpose(y_side + dot(z_hub[:, :HUBS], side_ref[NODES + HALO:, :]))
    ys[...] = (y_side[:HUBS] + y_side[HUBS:2 * HUBS]) + y_side[2 * HUBS:3 * HUBS]
    yr[me] = ys[...]
    round_y = [remote(ys, yr.at[me], q) for q in peers]

    over_blocks(forward_own, 0, 2, 4)

    def forward_far(at, carry):
        z = z_s[:, NODES:]
        acc = yt_s[:, at]
        for ref in pieces:
            acc = acc + dot(z, ref[NODES:NODES + HALO, at])
        hub_rows = jnp.concatenate([ref[NODES + HALO:, at] for ref in pieces], axis=0)
        yt_s[:, at] = acc + dot(z_hub, hub_rows)
        g2_s[at, :] += dot(side_ref[at, :], dhub_s[...])
        return carry

    over_blocks(forward_far)
    wait_all(round_b)

    def returned(ref):
        hub_sum = (ref[0, SEND:, :] + ref[1, SEND:, :]) + (ref[2, SEND:, :] + ref[3, SEND:, :])
        ref[me, :HUBS, :] = hub_sum
        ref[me, HUBS:SEND, :] = jnp.zeros((SEND - HUBS, hub_sum.shape[1]), F32)
        return ref[:, :SEND, :].reshape(HALO, hub_sum.shape[1]), hub_sum

    back, hub_sum = returned(rb)
    hub_dz2 = hub_sum.astype(BF16)
    back_parts = split3(back)

    def dz2_block(at, carry):
        own = g2_s[at, :]
        for piece in back_parts:
            own = own + dot(pt_s[at, :], piece)
        dz2_s[at, :] = own.astype(BF16)
        return carry

    over_blocks(dz2_block)

    wait_all(round_y)
    y_hub = (yr[0] + yr[1]) + (yr[2] + yr[3])
    b1 = b1_ref[...]
    b1_col = jnp.transpose(jnp.broadcast_to(b1, (128, HID)))
    y_rows = jnp.concatenate([piece.astype(F32) for piece in split3(y_hub)] + [jnp.zeros((128 - 3 * HUBS, HID), F32)], axis=0)
    y_cols_s[...] = jnp.transpose(y_rows).astype(BF16)[:, :3 * HUBS]

    def pre_block(at, carry):
        pre = (yt_s[:, at] + dot(y_cols_s[...], hub3_s[:, at])) + jnp.concatenate([b1_col] * 2, axis=1)
        hid_s[:, at] = jnp.maximum(pre, 0.0).astype(BF16)
        live_s[:, at] = jnp.where(pre > 0.0, 1.0, 0.0)
        return carry

    over_blocks(pre_block)

    class GroupSum:
        def __init__(self, own, half, got, total):
            self.own, self.half, self.got, self.total = own, half, got, total
            self.copy = remote(own.at[1 - core], got.at[0], sibling)

        def across(self):
            self.copy.wait()
            self.half[...] = self.own[core] + self.got[0]
            self.copy = remote(self.half, self.got.at[1], across)

        def back(self):
            self.copy.wait()
            self.total[core] = self.half[...] + self.got[1]
            self.copy = remote(self.total.at[core], self.total.at[core], sibling)

        def done(self):
            self.copy.wait()

    dw2t = jnp.transpose(dot(hid_s[...], dz2_s[...]))
    for h in range(2):
        a2[h] = dw2t[:112, h * 256:(h + 1) * 256]
        a2[h, OUT:OUT + 1, :128] = db2
    sum2 = GroupSum(a2, half2, got2, tot2)

    def dy_block(at, db1):
        live = jnp.transpose(live_s[:, at])
        dy = jnp.where(live > 0.5, dot(dz2_s[at, :OUT], w2t_ref[...]), 0.0)
        for j, piece in enumerate(split3(dy)):
            dy_s[j, at, :] = piece
        return db1 + jnp.sum(dy, axis=0, keepdims=True)

    db1 = over_blocks(dy_block, jnp.zeros((1, HID), F32))
    hub_dy = jnp.where(y_hub + b1 > 0.0, dot(hub_dz2[:, :OUT], w2t_ref[...]), 0.0)
    dyh_s[...] = side_by_side(hub_dy)
    sum2.across()

    def grad1(rows, cols):
        acc = dot(lo_ref[rows, :], dy_s[0, :, cols])
        acc = acc + dot(mid_ref[rows, :], dy_s[1, :, cols])
        acc = acc + dot(hi_ref[rows, :], dy_s[2, :, cols])
        acc = acc + dot(mid_ref[rows, :], dy_s[0, :, cols])
        acc = acc + dot(hi_ref[rows, :], dy_s[1, :, cols])
        acc = acc + dot(hi_ref[rows, :], dy_s[0, :, cols])
        return acc + dot(side_ref[rows, :], dyh_s[:, cols])

    halves = (pl.ds(0, 256), pl.ds(256, 256))
    round_d = []
    for h, cols in enumerate(halves):
        ret = grad1(far_rows, cols)
        for q in range(4):
            sd[h, q, :SEND, :] = ret[q * SEND:(q + 1) * SEND]
            sd[h, q, SEND:, :] = ret[HALO:]
        rd[h, me] = sd[h, me]
        round_d.append([remote(sd.at[h, q], rd.at[h, me], q) for q in peers])

    def grad1_own(h, m):
        rows = pl.ds(m * 512, 512)
        g1_s[rows, halves[h]] = grad1(rows, halves[h])

    def finish(h):
        wait_all(round_d[h])
        cols = halves[h]
        back, _ = returned(rd.at[h])
        dz1 = g1_s[:, cols]
        for piece in split3(back):
            dz1 = dz1 + dot(pt_s[...], piece)
        dz1 = dz1.astype(BF16)
        dz1_s[:, cols] = dz1
        dw1 = dot(xt_ref[...], dz1)
        for i in range(2):
            at = slice(i * 128, (i + 1) * 128)
            a1[h, i, :FIN, :] = dw1[:, at]
            a1[h, i, FIN:, :] = jnp.broadcast_to(db1[:, h * 256 + i * 128:h * 256 + (i + 1) * 128], (8, 128))
        return GroupSum(a1.at[h], half1.at[h], got1.at[h], tot1.at[h])

    grad1_own(0, 0)
    grad1_own(0, 1)
    grad1_own(1, 0)
    sum1 = [finish(0)]
    sum2.back()
    grad1_own(1, 1)
    sum1[0].across()
    sum1.append(finish(1))
    sum2.done()
    for h in range(2):
        dw2t_ref[:, h * 256:(h + 1) * 256] = tot2[h, :OUT, :]
    db2_ref[...] = tot2[0, OUT:OUT + 1, :OUT]
    sum1[1].across()
    dxt_ref[...] = dot_nt(w1_ref[...], dz1_s[...])
    sum1[0].back()
    sum1[0].done()

    def put(h):
        for i in range(2):
            at = slice(h * 256 + i * 128, h * 256 + (i + 1) * 128)
            dw1_ref[:, at] = tot1[h, i, :FIN, :]
            db1_ref[:, at] = tot1[h, i, FIN:FIN + 1, :]

    put(0)
    sum1[1].back()
    sum1[1].done()
    put(1)


def step(*operands):
    vmem = pl.BlockSpec(memory_space=pltpu.VMEM)
    out = lambda *shape: jax.ShapeDtypeStruct(shape, F32)
    f32 = lambda *shape: pltpu.VMEM(shape, F32)
    b16 = lambda *shape: pltpu.VMEM(shape, BF16)
    return pl.pallas_call(
        step_kernel,
        out_shape=(out(FIN, NODES), out(FIN, HID), out(OUT, HID), out(1, HID), out(1, OUT)),
        in_specs=[vmem] * 11,
        out_specs=(vmem,) * 5,
        scratch_shapes=[
            b16(4, SEND, FIN), b16(NODES, HALO), b16(4, SEND + HUBS, 256), b16(4, SEND + HUBS, 256), f32(4, 32, 128), f32(4, 32, 128),
            b16(HID, NODES + HALO), f32(HID, NODES), b16(NODES, 384), b16(128, 128), f32(NODES, 128), f32(HALO + HUBS, 128),
            f32(4, SEND + HUBS, 128), f32(4, SEND + HUBS, 128), f32(HUBS, HID), f32(4, HUBS, HID),
            b16(3, NODES, HID), b16(128, HID), f32(NODES, HID), f32(2, 4, SEND + HUBS, 256), f32(2, 4, SEND + HUBS, 256), b16(NODES, HID),
            b16(3 * HUBS, NODES), b16(HID, 3 * HUBS), b16(HID, NODES), f32(HID, NODES), b16(NODES, 128),
            f32(2, 112, 256), f32(112, 256), f32(2, 112, 256), f32(2, 112, 256),
            f32(2, 2, 208, 128), f32(2, 208, 128), f32(2, 2, 208, 128), f32(2, 2, 208, 128),
            pltpu.SemaphoreType.DMA((28,)), pltpu.SemaphoreType.DMA((28,)),
        ],
        compiler_params=pltpu.CompilerParams(collective_id=0, has_side_effects=True, vmem_limit_bytes=STEP_VMEM),
        name="step",
    )(*operands)


def emit_kernel(*refs):
    ins, outs, sem = refs[:5], refs[5:10], refs[10]
    copies = [pltpu.make_async_copy(a, b, sem.at[i]) for i, (a, b) in enumerate(zip(ins, outs))]
    for copy in copies:
        copy.start()
    for copy in copies:
        copy.wait()


def emit(*arrays):
    return pl.pallas_call(
        emit_kernel,
        out_shape=tuple(jax.ShapeDtypeStruct(a.shape, a.dtype) for a in arrays),
        in_specs=[pl.BlockSpec(memory_space=pltpu.VMEM)] * 5,
        out_specs=(pl.BlockSpec(memory_space=pltpu.HBM),) * 5,
        scratch_shapes=[pltpu.SemaphoreType.DMA((5,))],
        compiler_params=pltpu.CompilerParams(vmem_limit_bytes=4 << 20),
        name="emit",
    )(*arrays)


def solution(mesh):
    vertex_spec = P(("data", "graph"))
    vertex_rows = P(("data", "graph"), None)
    part_spec = P("data")
    part_rows = P("data", None)
    replicated = P()

    def device_step(x, dst, src, w, send, hub_ids, w_first, b_first, w_second, dy_out):
        dx, dw1, dw2, db1, db2 = emit(*step(*build(
            hub_ids, dst, src, w,
            x.T, w_first, b_first.reshape(1, HID), w_second.T, dy_out.T, send.reshape(1, HALO), hub_ids.reshape(1, HUBS))))
        return dx.T, dw1, dw2.T, db1.reshape(HID), db2.reshape(OUT)

    return jax.shard_map(
        device_step,
        mesh=mesh,
        in_specs=(vertex_rows, vertex_spec, vertex_spec, vertex_spec, vertex_spec, part_spec, replicated, replicated, replicated, vertex_rows),
        out_specs=(vertex_rows, part_rows, part_rows, part_spec, part_spec),
        check_vma=False,
    )
```
